32 devices in a mesh: context: 4 (over z), fsdp: 4 (over x, core), heads: 2 (over y).
Axes of the slice: x: 2, y: 2, z: 4, core: 2. Of those that a mesh axis runs over, the one named last changes fastest.
Arguments:
- layer_input: bfloat16 [2048, 2048], P(('context', 'fsdp')), may hold values from -6 to 6
- block_pair: int32 [4], replicated, may hold values from 0 to 3, each once
- attn_gain: bfloat16 [2048], P(('context', 'fsdp')), may hold values from 0.099609375 to 1.8984375
- q_weight: bfloat16 [2048, 2048], P(('context', 'fsdp'), 'heads'), may hold values from -0.125 to 0.125
- key_projection: bfloat16 [2048, 1024], P(('context', 'fsdp'), 'heads'), may hold values from -0.125 to 0.125
- value_projection: bfloat16 [2048, 1024], P(('context', 'fsdp'), 'heads'), may hold values from -0.125 to 0.125
- q_gain: bfloat16 [128], P(('context', 'fsdp')), may hold values from 0.8 to 5
- k_gain: bfloat16 [128], P(('context', 'fsdp')), may hold values from 0.8 to 5
- o_weight: bfloat16 [2048, 2048], P('heads', ('context', 'fsdp')), may hold values from -0.75 to 0.75
- mlp_gain: bfloat16 [2048], P(('context', 'fsdp')), may hold values from 0.099609375 to 1.8984375
- gate_weight: bfloat16 [2048, 6144], P(('context', 'fsdp'), 'heads'), may hold values from -0.125 to 0.125
- up_weight: bfloat16 [2048, 6144], P(('context', 'fsdp'), 'heads'), may hold values from -0.125 to 0.125
- down_weight: bfloat16 [6144, 2048], P('heads', ('context', 'fsdp')), may hold values from -0.078125 to 0.078125
- cotangent: bfloat16 [2048, 2048], P(('context', 'fsdp')), may hold values from -6 to 6
Outputs:
- block_out: bfloat16 [2048, 2048], P(('context', 'fsdp'))
- input_grad: float32 [2048, 2048], P(('context', 'fsdp'))
- attn_gain_grad: float32 [2048], P(('context', 'fsdp'))
- q_weight_grad: float32 [2048, 2048], P(('context', 'fsdp'), 'heads')
- k_weight_grad: float32 [2048, 1024], P(('context', 'fsdp'), 'heads')
- v_weight_grad: float32 [2048, 1024], P(('context', 'fsdp'), 'heads')
- q_gain_grad: float32 [128], P(('context', 'fsdp'))
- k_gain_grad: float32 [128], P(('context', 'fsdp'))
- o_weight_grad: float32 [2048, 2048], P('heads', ('context', 'fsdp'))
- mlp_gain_grad: float32 [2048], P(('context', 'fsdp'))
- gate_weight_grad: float32 [2048, 6144], P(('context', 'fsdp'), 'heads')
- up_weight_grad: float32 [2048, 6144], P(('context', 'fsdp'), 'heads')
- down_weight_grad: float32 [6144, 2048], P('heads', ('context', 'fsdp'))
The draws below stay inside these ranges and needn't reach their ends.
Inputs may be any that keep to these rules, and one draw needn't show every extreme that they name: `block_pair`: each of 0 to 3 appears once.
All inputs are finite; a program needn't handle non-finite values.
Results may differ from the reference program's by a relative error of at most 0.025.
The reference program's roundings to bfloat16 on the way count: a program that leaves them out, or rounds other values in their place, can miss the bound.
Values may be sent and summed in bfloat16 or wider, within the bound.
A program may use at most 256 MiB of HBM per device.

```python
import math
import jax
import jax.numpy as jnp
from jax import lax

MODEL_WIDTH = 2048
QUERY_HEADS = 16
KEY_VALUE_HEADS = 8
HEAD_SIZE = 128
FF = 6144
SEQUENCE_TOKENS = 2048
BLOCK = 256
N_CONTEXT = 4


def gain_values(key):
    values = jnp.exp(jax.random.uniform(key, (HEAD_SIZE,), jnp.float32, math.log(0.8), math.log(2.5)))
    return values.astype(jnp.bfloat16)


def draw_q_gain(key, part):
    return gain_values(jax.random.fold_in(key, 11))


def draw_k_gain(key, part):
    return gain_values(jax.random.fold_in(key, 23))


def strengthened(array, own_key, source, target, shards_of, factor):
    owner, partner = [(jnp.arange(array.shape[position]) // (array.shape[position] // shards_of)).reshape([-1 if axis == position else 1 for axis in range(array.ndim)]) for position in (source, target)]
    chosen = jax.random.permutation(own_key, shards_of)[partner]
    strong = (owner == chosen) | (owner == (partner + shards_of // 2) % shards_of)
    return jnp.where(strong, factor * array, array)


def levels(key, shape, split, low, high):
    factor_of = 1.0
    for dim, shards_of in split:
        steps = jax.random.uniform(jax.random.fold_in(jax.random.fold_in(key, 6), dim), (shards_of,), jnp.float32, low / len(split), high / len(split))
        factor_of = factor_of * jnp.repeat(jnp.exp(steps), shape[dim] // shards_of).reshape((-1,) + (1,) * (len(shape) - 1 - dim))
    return factor_of


def bell_draw(rng, dims, width, limit, split=(), kind=jnp.bfloat16):
    array = jax.random.normal(rng, dims, jnp.float32) * width
    if len(split) > 0:
        array = levels(rng, dims, split, -0.22, 0.18) * array
    return jnp.clip(array, min=-limit, max=limit).astype(kind)


def bell_draw_with(own_key, extent, width, most, pieces, heavy, held_as=jnp.bfloat16):
    entries = width * jax.random.normal(own_key, extent, jnp.float32)
    if pieces:
        entries = entries * levels(own_key, extent, pieces, -0.22, 0.18)
    return jnp.clip(strengthened(entries, jax.random.fold_in(own_key, 3), *heavy), -most, most).astype(held_as)


def setup_inputs(seed: int = 0) -> dict:
    splits = jax.random.split(jax.random.key(seed), 15)
    layer_input = bell_draw_with(splits[0], (SEQUENCE_TOKENS, MODEL_WIDTH), 1.0, 6.0, ((0, 16),), (0, 1, 16, 2.0))
    block_pair = jax.random.permutation(splits[1], N_CONTEXT).astype(jnp.int32)
    attn_gain = jnp.clip(1.0 + 0.18 * jax.random.normal(splits[2], (MODEL_WIDTH,), jnp.float32), 0.099609375, 1.8984375).astype(jnp.bfloat16)
    q_weight = bell_draw(splits[3], (MODEL_WIDTH, QUERY_HEADS * HEAD_SIZE), MODEL_WIDTH ** -0.5, 0.125, ((0, 16), (1, 2)))
    key_projection = bell_draw(splits[4], (MODEL_WIDTH, KEY_VALUE_HEADS * HEAD_SIZE), MODEL_WIDTH ** -0.5, 0.125, ((0, 16), (1, 2)))
    value_projection = bell_draw(splits[5], (MODEL_WIDTH, KEY_VALUE_HEADS * HEAD_SIZE), MODEL_WIDTH ** -0.5, 0.125, ((0, 16), (1, 2)))
    q_gain = draw_q_gain(jax.random.fold_in(splits[14], 71), 0)
    k_gain = draw_k_gain(jax.random.fold_in(splits[14], 71), 0)
    o_weight = bell_draw(splits[8], (QUERY_HEADS * HEAD_SIZE, MODEL_WIDTH), (QUERY_HEADS * HEAD_SIZE // 32) ** -0.5, 0.75, ((0, 2), (1, 16)))
    mlp_gain = jnp.clip(1.0 + 0.18 * jax.random.normal(splits[9], (MODEL_WIDTH,), jnp.float32), 0.099609375, 1.8984375).astype(jnp.bfloat16)
    gate_weight = bell_draw(splits[10], (MODEL_WIDTH, FF), MODEL_WIDTH ** -0.5, 0.125, ((0, 16), (1, 2)))
    up_weight = bell_draw(splits[11], (MODEL_WIDTH, FF), MODEL_WIDTH ** -0.5, 0.125, ((0, 16), (1, 2)))
    down_weight = bell_draw(splits[12], (FF, MODEL_WIDTH), FF ** -0.5, 0.078125, ((0, 2), (1, 16)))
    cotangent = bell_draw_with(splits[13], (SEQUENCE_TOKENS, MODEL_WIDTH), 1.0, 6.0, ((0, 16),), (0, 1, 16, 2.0))
    return {"layer_input": layer_input, "block_pair": block_pair, "attn_gain": attn_gain, "q_weight": q_weight, "key_projection": key_projection, "value_projection": value_projection, "q_gain": q_gain, "k_gain": k_gain, "o_weight": o_weight, "mlp_gain": mlp_gain, "gate_weight": gate_weight, "up_weight": up_weight, "down_weight": down_weight, "cotangent": cotangent}


EPS = 1e-06
THETA = 1000000.0
NEG = -1e+30

def row_places(block_pair, row_ids, block_len):
    owners = block_pair.shape[0]
    holder = row_ids // (2 * block_len)
    within = row_ids % (2 * block_len)
    match = holder[:, None] == jnp.arange(owners, dtype=jnp.int32)[None, :]
    paired = lax.optimization_barrier(jnp.sum(jnp.where(match, block_pair[None, :], 0), axis=1)).astype(jnp.int32)
    which = jnp.where(within >= block_len, 2 * owners - 1 - paired, paired)
    return (which * block_len + within % block_len).astype(jnp.int32)

def rope_tables(places, head_dim):
    half = head_dim // 2
    freq = jnp.exp(jnp.arange(half, dtype=jnp.float32) * (-2.0 * math.log(THETA) / head_dim))
    angle = places.astype(jnp.float32)[:, None] * freq[None, :]
    return (jnp.cos(angle)[:, None, :], jnp.sin(angle)[:, None, :])

def apply_rotary(field, cosine_table, sine_table):
    half = field.shape[-1] // 2
    first = field[..., :half]
    second = field[..., half:]
    return jnp.concatenate([first * cosine_table - second * sine_table, second * cosine_table + first * sine_table], axis=-1)

def unrotate(grad, cosine_table, sine_table):
    half = grad.shape[-1] // 2
    first = grad[..., :half]
    second = grad[..., half:]
    return jnp.concatenate([first * cosine_table + second * sine_table, second * cosine_table - first * sine_table], axis=-1)

def row_norm(field):
    factor = lax.rsqrt(lax.optimization_barrier(jnp.mean(field * field, axis=-1, keepdims=True)) + EPS)
    return (field * factor, factor)

def norm_backward(grad_hat, normed, factor):
    return factor * (grad_hat - normed * lax.optimization_barrier(jnp.mean(grad_hat * normed, axis=-1, keepdims=True)))

def rounded_values(value):
    return lax.optimization_barrier(value.astype(jnp.bfloat16)).astype(jnp.float32)

def masked_scores(query_matrix, key_rows, query_places, key_places, softmax_scale):
    score_matrix = jnp.einsum('oblh,wbh->blow', query_matrix, key_rows) * softmax_scale
    allowed = key_places[None, :] <= query_places[:, None]
    return (jnp.where(allowed, score_matrix, NEG), allowed)

def reference(layer_input, block_pair, attn_gain, q_weight, key_projection, value_projection, q_gain, k_gain, o_weight, mlp_gain, gate_weight, up_weight, down_weight, cotangent):
    wide_float_type = jnp.float32
    narrow_float_type = jnp.bfloat16
    softmax_scale = 1.0 / math.sqrt(HEAD_SIZE)
    group_size = QUERY_HEADS // KEY_VALUE_HEADS
    places = row_places(block_pair, jnp.arange(SEQUENCE_TOKENS, dtype=jnp.int32), BLOCK)
    cosine_table, sine_table = rope_tables(places, HEAD_SIZE)
    x_full = layer_input.astype(wide_float_type)
    x_hat, x_scale = row_norm(x_full)
    attn_scale = attn_gain.astype(wide_float_type)
    normalized_input = (x_hat * attn_scale).astype(narrow_float_type)
    q_raw = jnp.dot(normalized_input, q_weight, preferred_element_type=wide_float_type).reshape(SEQUENCE_TOKENS, QUERY_HEADS, HEAD_SIZE)
    unnormalized_keys = jnp.dot(normalized_input, key_projection, preferred_element_type=wide_float_type).reshape(SEQUENCE_TOKENS, KEY_VALUE_HEADS, HEAD_SIZE)
    value_rows_backward = jnp.dot(normalized_input, value_projection, preferred_element_type=wide_float_type).astype(narrow_float_type)
    value_rows_forward = lax.optimization_barrier(value_rows_backward).astype(wide_float_type).reshape(SEQUENCE_TOKENS, KEY_VALUE_HEADS, HEAD_SIZE)
    normalized_queries, q_scale = row_norm(q_raw)
    normalized_keys, key_norm_scale = row_norm(unnormalized_keys)
    query_gain_vector = q_gain.astype(wide_float_type)
    key_gain_vector = k_gain.astype(wide_float_type)
    rotated_queries = rounded_values(apply_rotary(normalized_queries * query_gain_vector, cosine_table, sine_table)).reshape(SEQUENCE_TOKENS, KEY_VALUE_HEADS, group_size, HEAD_SIZE)
    rotated_keys = rounded_values(apply_rotary(normalized_keys * key_gain_vector, cosine_table, sine_table))
    query_rows = math.gcd(SEQUENCE_TOKENS, 256)
    block_list = SEQUENCE_TOKENS // query_rows
    query_block_list = rotated_queries.reshape(block_list, query_rows, KEY_VALUE_HEADS, group_size, HEAD_SIZE)
    block_placement = places.reshape(block_list, query_rows)

    def forward_block(blockset):
        query_matrix, query_places = blockset
        score_matrix, allowed = masked_scores(query_matrix, rotated_keys, query_places, places, softmax_scale)
        top = lax.optimization_barrier(jnp.max(score_matrix, axis=-1))
        weight_set = jnp.where(allowed, jnp.exp(score_matrix - top[..., None]), 0.0)
        total = lax.optimization_barrier(jnp.sum(weight_set, axis=-1))
        softmax_numerator = jnp.einsum('nwqf,fny->nwqy', rounded_values(weight_set), value_rows_forward)
        return (softmax_numerator / total[..., None], top + jnp.log(total))
    outputs, logsumexp_per_block = lax.map(forward_block, (query_block_list, block_placement))
    attention_backward = jnp.transpose(outputs, (0, 3, 1, 2, 4)).reshape(SEQUENCE_TOKENS, QUERY_HEADS * HEAD_SIZE).astype(narrow_float_type)
    hidden = x_full + jnp.dot(attention_backward, o_weight, preferred_element_type=wide_float_type)
    mrows = math.gcd(SEQUENCE_TOKENS, 4096)
    mblocks = SEQUENCE_TOKENS // mrows
    mlp_scale = mlp_gain.astype(wide_float_type)

    def mlp_block(carry, blockset):
        grad_gatew, grad_upw, grad_downw, grad_gain = carry
        hid, cot = blockset
        h_hat, h_scale = row_norm(hid)
        h_normed = (h_hat * mlp_scale).astype(narrow_float_type)
        gate = jnp.dot(h_normed, gate_weight, preferred_element_type=wide_float_type)
        up_val = jnp.dot(h_normed, up_weight, preferred_element_type=wide_float_type)
        sigma = jax.nn.sigmoid(gate)
        silu = gate * sigma
        act = (silu * up_val).astype(narrow_float_type)
        out = (hid + jnp.dot(act, down_weight, preferred_element_type=wide_float_type)).astype(narrow_float_type)
        grad_act = jnp.dot(cot, down_weight.T, preferred_element_type=wide_float_type)
        grad_g = (grad_act * up_val * (sigma * (1.0 + gate * (1.0 - sigma)))).astype(narrow_float_type)
        grad_u = (grad_act * silu).astype(narrow_float_type)
        grad_downw = grad_downw + jnp.dot(act.T, cot, preferred_element_type=wide_float_type)
        grad_gatew = grad_gatew + jnp.dot(h_normed.T, grad_g, preferred_element_type=wide_float_type)
        grad_upw = grad_upw + jnp.dot(h_normed.T, grad_u, preferred_element_type=wide_float_type)
        grad_normed = jnp.dot(grad_g, gate_weight.T, preferred_element_type=wide_float_type) + jnp.dot(grad_u, up_weight.T, preferred_element_type=wide_float_type)
        grad_gain = grad_gain + lax.optimization_barrier(jnp.sum(grad_normed * h_hat, axis=0))
        grad_hid = cot.astype(wide_float_type) + norm_backward(grad_normed * mlp_scale, h_hat, h_scale)
        return ((grad_gatew, grad_upw, grad_downw, grad_gain), (out, grad_hid))
    start = (jnp.zeros((MODEL_WIDTH, FF), wide_float_type), jnp.zeros((MODEL_WIDTH, FF), wide_float_type), jnp.zeros((FF, MODEL_WIDTH), wide_float_type), jnp.zeros((MODEL_WIDTH,), wide_float_type))
    carried, produced = lax.scan(mlp_block, start, (hidden.reshape(mblocks, mrows, MODEL_WIDTH), cotangent.reshape(mblocks, mrows, MODEL_WIDTH)))
    gate_weight_grad, up_weight_grad, down_weight_grad, mlp_gain_grad = carried
    block_out = produced[0].reshape(SEQUENCE_TOKENS, MODEL_WIDTH)
    grad_h = produced[1].reshape(SEQUENCE_TOKENS, MODEL_WIDTH)
    grad_hb = grad_h.astype(narrow_float_type)
    o_weight_grad = jnp.dot(attention_backward.T, grad_hb, preferred_element_type=wide_float_type)
    output_gradient_backward = jnp.dot(grad_hb, o_weight.T, preferred_element_type=wide_float_type).astype(narrow_float_type)
    output_gradient_forward = lax.optimization_barrier(output_gradient_backward).astype(wide_float_type).reshape(SEQUENCE_TOKENS, KEY_VALUE_HEADS, group_size, HEAD_SIZE)
    attention_forward = lax.optimization_barrier(attention_backward).astype(wide_float_type).reshape(SEQUENCE_TOKENS, KEY_VALUE_HEADS, group_size, HEAD_SIZE)
    delta_rows = lax.optimization_barrier(jnp.sum(output_gradient_forward * attention_forward, axis=-1))
    delta_per_block = jnp.transpose(delta_rows.reshape(block_list, query_rows, KEY_VALUE_HEADS, group_size), (0, 2, 3, 1))

    def backward_block_step(carry, blockset):
        key_gradient, value_gradient = carry
        query_matrix, output_gradient, log_total, delta_part, query_places = blockset
        score_matrix, allowed = masked_scores(query_matrix, rotated_keys, query_places, places, softmax_scale)
        probability_rows = jnp.where(allowed, jnp.exp(score_matrix - log_total[..., None]), 0.0)
        value_gradient = value_gradient + jnp.einsum('mojp,jmof->pmf', rounded_values(probability_rows), output_gradient)
        probability_gradient = jnp.einsum('oblh,wbh->blow', output_gradient, value_rows_forward)
        score_gradient = rounded_values(probability_rows * (probability_gradient - delta_part[..., None]))
        query_gradient = jnp.einsum('xwzq,qxp->zxwp', score_gradient, rotated_keys) * softmax_scale
        key_gradient = key_gradient + jnp.einsum('mojp,jmof->pmf', score_gradient, query_matrix) * softmax_scale
        return ((key_gradient, value_gradient), query_gradient)
    zero_key_value = jnp.zeros((SEQUENCE_TOKENS, KEY_VALUE_HEADS, HEAD_SIZE), wide_float_type)
    (rotated_key_gradient, value_gradient), rotated_query_gradient = lax.scan(backward_block_step, (zero_key_value, zero_key_value), (query_block_list, output_gradient_forward.reshape(block_list, query_rows, KEY_VALUE_HEADS, group_size, HEAD_SIZE), logsumexp_per_block, delta_per_block, block_placement))
    rotated_query_gradient = rotated_query_gradient.reshape(SEQUENCE_TOKENS, QUERY_HEADS, HEAD_SIZE)
    grad_qg = unrotate(rotated_query_gradient, cosine_table, sine_table)
    q_gain_grad = lax.optimization_barrier(jnp.sum(grad_qg * normalized_queries, axis=(0, 1)))
    query_gradient = norm_backward(grad_qg * query_gain_vector, normalized_queries, q_scale).reshape(SEQUENCE_TOKENS, QUERY_HEADS * HEAD_SIZE).astype(narrow_float_type)
    key_gain_gradient = unrotate(rotated_key_gradient, cosine_table, sine_table)
    k_gain_grad = lax.optimization_barrier(jnp.sum(key_gain_gradient * normalized_keys, axis=(0, 1)))
    key_gradient = norm_backward(key_gain_gradient * key_gain_vector, normalized_keys, key_norm_scale).reshape(SEQUENCE_TOKENS, KEY_VALUE_HEADS * HEAD_SIZE).astype(narrow_float_type)
    value_gradient_backward = value_gradient.reshape(SEQUENCE_TOKENS, KEY_VALUE_HEADS * HEAD_SIZE).astype(narrow_float_type)
    q_weight_grad = jnp.dot(normalized_input.T, query_gradient, preferred_element_type=wide_float_type)
    k_weight_grad = jnp.dot(normalized_input.T, key_gradient, preferred_element_type=wide_float_type)
    v_weight_grad = jnp.dot(normalized_input.T, value_gradient_backward, preferred_element_type=wide_float_type)
    grad_xn = jnp.dot(query_gradient, q_weight.T, preferred_element_type=wide_float_type) + jnp.dot(key_gradient, key_projection.T, preferred_element_type=wide_float_type) + jnp.dot(value_gradient_backward, value_projection.T, preferred_element_type=wide_float_type)
    attn_gain_grad = lax.optimization_barrier(jnp.sum(grad_xn * x_hat, axis=0))
    input_grad = grad_h + norm_backward(grad_xn * attn_scale, x_hat, x_scale)
    return (block_out, input_grad, attn_gain_grad, q_weight_grad, k_weight_grad, v_weight_grad, q_gain_grad, k_gain_grad, o_weight_grad, mlp_gain_grad, gate_weight_grad, up_weight_grad, down_weight_grad)
```

```python
import functools
import math

import jax
import jax.numpy as jnp
from jax import lax
from jax.experimental import pallas as pl
from jax.experimental.pallas import tpu as pltpu
from jax.sharding import PartitionSpec as P

HEAD_SIZE = 128
CONTEXT, FSDP, HEADS = "context", "fsdp", "heads"
ROWS = (CONTEXT, FSDP)


EPS = 1e-06
THETA = 1000000.0
NEG = -1e30


def row_places(block_pair, row_ids, block_len):
    owners = block_pair.shape[0]
    holder = row_ids // (2 * block_len)
    within = row_ids % (2 * block_len)
    match = holder[:, None] == jnp.arange(owners, dtype=jnp.int32)[None, :]
    paired = jnp.sum(jnp.where(match, block_pair[None, :], 0), axis=1)
    which = jnp.where(within >= block_len, 2 * owners - 1 - paired, paired)
    return which * block_len + within % block_len


def rope_tables(places, head_dim):
    half = head_dim // 2
    freq = jnp.exp(jnp.arange(half, dtype=jnp.float32) * (-2.0 * math.log(THETA) / head_dim))
    angle = places.astype(jnp.float32)[:, None] * freq[None, :]
    return (jnp.cos(angle)[:, None, :], jnp.sin(angle)[:, None, :])


def apply_rotary(field, cosine_table, sine_table):
    half = field.shape[-1] // 2
    first = field[..., :half]
    second = field[..., half:]
    return jnp.concatenate(
        [first * cosine_table - second * sine_table, second * cosine_table + first * sine_table],
        axis=-1,
    )


def unrotate(grad, cosine_table, sine_table):
    half = grad.shape[-1] // 2
    first = grad[..., :half]
    second = grad[..., half:]
    return jnp.concatenate(
        [first * cosine_table + second * sine_table, second * cosine_table - first * sine_table],
        axis=-1,
    )


def row_norm(field):
    factor = lax.rsqrt(jnp.mean(field * field, axis=-1, keepdims=True) + EPS)
    return (field * factor, factor)


def norm_backward(grad_hat, normed, factor):
    return factor * (grad_hat - normed * jnp.mean(grad_hat * normed, axis=-1, keepdims=True))


def masked_scores(query_matrix, key_rows, query_places, key_places, softmax_scale):
    score_matrix = (
        jnp.einsum("oblh,wbh->blow", query_matrix, key_rows, preferred_element_type=jnp.float32)
        * softmax_scale
    )
    allowed = key_places[None, :] <= query_places[:, None]
    return (jnp.where(allowed, score_matrix, NEG), allowed)


def per_device(
    layer_input,
    block_pair,
    attn_gain,
    q_weight,
    key_projection,
    value_projection,
    q_gain,
    k_gain,
    o_weight,
    mlp_gain,
    gate_weight,
    up_weight,
    down_weight,
    cotangent,
):
    wide_float_type = jnp.float32
    narrow_float_type = jnp.bfloat16
    tokens = layer_input.shape[0]
    members = lax.axis_size(ROWS)
    seq_len = tokens * members
    block_len = tokens * lax.axis_size(FSDP) // 2
    kv_local = key_projection.shape[1] // HEAD_SIZE
    q_local = q_weight.shape[1] // HEAD_SIZE
    group_size = q_local // kv_local
    softmax_scale = 1.0 / math.sqrt(HEAD_SIZE)
    (
        full_attn_gain,
        full_q,
        full_k,
        full_v,
        full_q_gain,
        full_k_gain,
        full_o,
        full_mlp_gain,
        full_gate,
        full_up,
        full_down,
    ) = (
        lax.all_gather(attn_gain, ROWS, axis=0, tiled=True),
        lax.all_gather(q_weight, ROWS, axis=0, tiled=True),
        lax.all_gather(key_projection, ROWS, axis=0, tiled=True),
        lax.all_gather(value_projection, ROWS, axis=0, tiled=True),
        lax.all_gather(q_gain, ROWS, axis=0, tiled=True),
        lax.all_gather(k_gain, ROWS, axis=0, tiled=True),
        lax.all_gather(o_weight, ROWS, axis=1, tiled=True),
        lax.all_gather(mlp_gain, ROWS, axis=0, tiled=True),
        lax.all_gather(gate_weight, ROWS, axis=0, tiled=True),
        lax.all_gather(up_weight, ROWS, axis=0, tiled=True),
        lax.all_gather(down_weight, ROWS, axis=1, tiled=True),
    )
    own_rows = lax.axis_index(ROWS) * tokens + jnp.arange(tokens, dtype=jnp.int32)
    own_places = row_places(block_pair, own_rows, block_len)
    cosine_table, sine_table = rope_tables(own_places, HEAD_SIZE)
    x_full = layer_input.astype(wide_float_type)
    x_hat, x_scale = row_norm(x_full)
    attn_scale = full_attn_gain.astype(wide_float_type)
    normalized_input = (x_hat * attn_scale).astype(narrow_float_type)
    q_raw = jnp.dot(normalized_input, full_q, preferred_element_type=wide_float_type).reshape(
        tokens, q_local, HEAD_SIZE
    )
    unnormalized_keys = jnp.dot(
        normalized_input, full_k, preferred_element_type=wide_float_type
    ).reshape(tokens, kv_local, HEAD_SIZE)
    value_rows_backward = jnp.dot(
        normalized_input, full_v, preferred_element_type=wide_float_type
    ).astype(narrow_float_type)
    normalized_queries, q_scale = row_norm(q_raw)
    normalized_keys, key_norm_scale = row_norm(unnormalized_keys)
    query_gain_vector = full_q_gain.astype(wide_float_type)
    key_gain_vector = full_k_gain.astype(wide_float_type)
    rotated_queries = apply_rotary(
        normalized_queries * query_gain_vector, cosine_table, sine_table
    ).astype(narrow_float_type)
    grouped_queries = rotated_queries.reshape(tokens, kv_local, group_size, HEAD_SIZE)
    k_flat = (
        apply_rotary(normalized_keys * key_gain_vector, cosine_table, sine_table)
        .astype(narrow_float_type)
        .reshape(tokens, kv_local * HEAD_SIZE)
    )
    start_state = (
        jnp.full((kv_local, group_size, tokens), NEG, wide_float_type),
        jnp.zeros((kv_local, group_size, tokens), wide_float_type),
        jnp.zeros((kv_local, group_size, tokens, HEAD_SIZE), wide_float_type),
    )
    key_piece = lax.all_gather(k_flat, ROWS, axis=0, tiled=True)
    value_piece = lax.all_gather(value_rows_backward, ROWS, axis=0, tiled=True)
    count = key_piece.shape[0]
    width = math.gcd(count, 512)
    steps_here = count // width
    key_blocks = key_piece.reshape(steps_here, width, kv_local, HEAD_SIZE)
    value_blocks = value_piece.reshape(steps_here, width, kv_local, HEAD_SIZE)
    key_places = row_places(block_pair, jnp.arange(count, dtype=jnp.int32), block_len).reshape(
        steps_here, width
    )

    def online(state, blockset):
        top, total, softmax_numerator = state
        key_tile, value_tile, place_blk = blockset
        score_matrix, allowed = masked_scores(
            grouped_queries, key_tile, own_places, place_blk, softmax_scale
        )
        new_top = jnp.maximum(top, jnp.max(score_matrix, axis=-1))
        shrink = jnp.exp(top - new_top)
        weight_set = jnp.where(allowed, jnp.exp(score_matrix - new_top[..., None]), 0.0)
        total = total * shrink + jnp.sum(weight_set, axis=-1)
        softmax_numerator = softmax_numerator * shrink[..., None] + jnp.einsum(
            "nwqf,fny->nwqy",
            weight_set.astype(narrow_float_type),
            value_tile,
            preferred_element_type=wide_float_type,
        )
        return ((new_top, total, softmax_numerator), None)

    result, _ = lax.scan(online, start_state, (key_blocks, value_blocks, key_places))
    top, total, softmax_numerator = result
    log_total = top + jnp.log(total)
    attention_backward = (
        jnp.transpose(softmax_numerator / total[..., None], (2, 0, 1, 3))
        .reshape(tokens, q_local * HEAD_SIZE)
        .astype(narrow_float_type)
    )
    attn_part = jnp.dot(attention_backward, full_o, preferred_element_type=wide_float_type)
    hidden = x_full + lax.psum(attn_part, HEADS)
    mlp_scale = full_mlp_gain.astype(wide_float_type)
    h_hat, h_scale = row_norm(hidden)
    h_normed = (h_hat * mlp_scale).astype(narrow_float_type)
    gate = jnp.dot(h_normed, full_gate, preferred_element_type=wide_float_type)
    up_val = jnp.dot(h_normed, full_up, preferred_element_type=wide_float_type)
    sigma = jax.nn.sigmoid(gate)
    silu = gate * sigma
    act = (silu * up_val).astype(narrow_float_type)
    mlp_part = jnp.dot(act, full_down, preferred_element_type=wide_float_type)
    block_out = (hidden + lax.psum(mlp_part, HEADS)).astype(narrow_float_type)
    (
        full_attn_gain,
        full_q,
        full_k,
        full_v,
        full_q_gain,
        full_k_gain,
        full_o,
        full_mlp_gain,
        full_gate,
        full_up,
        full_down,
    ) = (
        lax.all_gather(attn_gain, ROWS, axis=0, tiled=True),
        lax.all_gather(q_weight, ROWS, axis=0, tiled=True),
        lax.all_gather(key_projection, ROWS, axis=0, tiled=True),
        lax.all_gather(value_projection, ROWS, axis=0, tiled=True),
        lax.all_gather(q_gain, ROWS, axis=0, tiled=True),
        lax.all_gather(k_gain, ROWS, axis=0, tiled=True),
        lax.all_gather(o_weight, ROWS, axis=1, tiled=True),
        lax.all_gather(mlp_gain, ROWS, axis=0, tiled=True),
        lax.all_gather(gate_weight, ROWS, axis=0, tiled=True),
        lax.all_gather(up_weight, ROWS, axis=0, tiled=True),
        lax.all_gather(down_weight, ROWS, axis=1, tiled=True),
    )
    grad_downw = jnp.einsum("tf,td->fd", act, cotangent, preferred_element_type=wide_float_type)
    grad_act = jnp.einsum("td,fd->tf", cotangent, full_down, preferred_element_type=wide_float_type)
    grad_g = (grad_act * up_val * (sigma * (1.0 + gate * (1.0 - sigma)))).astype(narrow_float_type)
    grad_u = (grad_act * silu).astype(narrow_float_type)
    grad_gatew = jnp.einsum("tc,tf->cf", h_normed, grad_g, preferred_element_type=wide_float_type)
    grad_upw = jnp.einsum("tc,tf->cf", h_normed, grad_u, preferred_element_type=wide_float_type)
    normed_part = jnp.einsum(
        "tf,cf->tc", grad_g, full_gate, preferred_element_type=wide_float_type
    ) + jnp.einsum("tf,cf->tc", grad_u, full_up, preferred_element_type=wide_float_type)
    grad_normed = lax.psum(normed_part, HEADS)
    grad_mlp_gain = jnp.sum(grad_normed * h_hat, axis=0)
    grad_h = cotangent.astype(wide_float_type) + norm_backward(
        grad_normed * mlp_scale, h_hat, h_scale
    )
    grad_hb = grad_h.astype(narrow_float_type)
    grad_ow = jnp.einsum(
        "tq,td->qd", attention_backward, grad_hb, preferred_element_type=wide_float_type
    )
    output_gradient_backward = jnp.einsum(
        "td,qd->tq", grad_hb, full_o, preferred_element_type=wide_float_type
    ).astype(narrow_float_type)
    grouped_output_gradient = output_gradient_backward.reshape(
        tokens, kv_local, group_size, HEAD_SIZE
    )
    delta_rows = jnp.sum(
        grouped_output_gradient.astype(wide_float_type)
        * attention_backward.reshape(tokens, kv_local, group_size, HEAD_SIZE).astype(
            wide_float_type
        ),
        axis=-1,
    )
    delta_rows = jnp.transpose(delta_rows, (1, 2, 0))
    keys_all, values_all = (
        lax.all_gather(k_flat, ROWS, axis=0, tiled=True),
        lax.all_gather(value_rows_backward, ROWS, axis=0, tiled=True),
    )
    width = math.gcd(seq_len, 512)
    steps_all = seq_len // width
    all_places = row_places(block_pair, jnp.arange(seq_len, dtype=jnp.int32), block_len).reshape(
        steps_all, width
    )

    def backward_step(grad_q_acc, blockset):
        key_tile, value_tile, place_blk = blockset
        score_matrix, allowed = masked_scores(
            grouped_queries, key_tile, own_places, place_blk, softmax_scale
        )
        probability_rows = jnp.where(allowed, jnp.exp(score_matrix - log_total[..., None]), 0.0)
        grad_v_blk = jnp.einsum(
            "mojp,jmof->pmf",
            probability_rows.astype(narrow_float_type),
            grouped_output_gradient,
            preferred_element_type=wide_float_type,
        )
        probability_gradient = jnp.einsum(
            "oblh,wbh->blow",
            grouped_output_gradient,
            value_tile,
            preferred_element_type=wide_float_type,
        )
        score_gradient = (probability_rows * (probability_gradient - delta_rows[..., None])).astype(
            narrow_float_type
        )
        grad_q_acc = (
            grad_q_acc
            + jnp.einsum(
                "xwzq,qxp->zxwp", score_gradient, key_tile, preferred_element_type=wide_float_type
            )
            * softmax_scale
        )
        grad_k_blk = (
            jnp.einsum(
                "mojp,jmof->pmf",
                score_gradient,
                grouped_queries,
                preferred_element_type=wide_float_type,
            )
            * softmax_scale
        )
        return (grad_q_acc, (grad_k_blk, grad_v_blk))

    rotated_query_gradient, stacked = lax.scan(
        backward_step,
        jnp.zeros((tokens, kv_local, group_size, HEAD_SIZE), wide_float_type),
        (
            keys_all.reshape(steps_all, width, kv_local, HEAD_SIZE),
            values_all.reshape(steps_all, width, kv_local, HEAD_SIZE),
            all_places,
        ),
    )
    grad_k_all = stacked[0].reshape(seq_len, kv_local * HEAD_SIZE)
    grad_v_all = stacked[1].reshape(seq_len, kv_local * HEAD_SIZE)
    grad_k_own, grad_v_own = (
        lax.psum_scatter(grad_k_all, ROWS, scatter_dimension=0, tiled=True),
        lax.psum_scatter(grad_v_all, ROWS, scatter_dimension=0, tiled=True),
    )
    grad_qg = unrotate(
        rotated_query_gradient.reshape(tokens, q_local, HEAD_SIZE), cosine_table, sine_table
    )
    q_gain_part = jnp.sum(grad_qg * normalized_queries, axis=(0, 1))
    query_gradient = (
        norm_backward(grad_qg * query_gain_vector, normalized_queries, q_scale)
        .reshape(tokens, q_local * HEAD_SIZE)
        .astype(narrow_float_type)
    )
    key_gain_gradient = unrotate(
        grad_k_own.reshape(tokens, kv_local, HEAD_SIZE), cosine_table, sine_table
    )
    k_gain_part = jnp.sum(key_gain_gradient * normalized_keys, axis=(0, 1))
    key_gradient = (
        norm_backward(key_gain_gradient * key_gain_vector, normalized_keys, key_norm_scale)
        .reshape(tokens, kv_local * HEAD_SIZE)
        .astype(narrow_float_type)
    )
    value_gradient_backward = grad_v_own.astype(narrow_float_type)
    grad_qw = jnp.einsum(
        "tc,tq->cq", normalized_input, query_gradient, preferred_element_type=wide_float_type
    )
    grad_kw = jnp.einsum(
        "tc,tq->cq", normalized_input, key_gradient, preferred_element_type=wide_float_type
    )
    grad_vw = jnp.einsum(
        "tc,tq->cq",
        normalized_input,
        value_gradient_backward,
        preferred_element_type=wide_float_type,
    )
    xn_part = (
        jnp.einsum("tq,cq->tc", query_gradient, full_q, preferred_element_type=wide_float_type)
        + jnp.einsum("tq,cq->tc", key_gradient, full_k, preferred_element_type=wide_float_type)
        + jnp.einsum(
            "tq,cq->tc", value_gradient_backward, full_v, preferred_element_type=wide_float_type
        )
    )
    grad_xn, grad_q_gain, grad_k_gain = lax.psum((xn_part, q_gain_part, k_gain_part), HEADS)
    grad_attn_gain = jnp.sum(grad_xn * x_hat, axis=0)
    input_grad = grad_h + norm_backward(grad_xn * attn_scale, x_hat, x_scale)
    owned = (
        lax.psum_scatter(grad_attn_gain, ROWS, scatter_dimension=0, tiled=True),
        lax.psum_scatter(grad_qw, ROWS, scatter_dimension=0, tiled=True),
        lax.psum_scatter(grad_kw, ROWS, scatter_dimension=0, tiled=True),
        lax.psum_scatter(grad_vw, ROWS, scatter_dimension=0, tiled=True),
        lax.psum_scatter(grad_q_gain, ROWS, scatter_dimension=0, tiled=True),
        lax.psum_scatter(grad_k_gain, ROWS, scatter_dimension=0, tiled=True),
        lax.psum_scatter(grad_ow, ROWS, scatter_dimension=1, tiled=True),
        lax.psum_scatter(grad_mlp_gain, ROWS, scatter_dimension=0, tiled=True),
        lax.psum_scatter(grad_gatew, ROWS, scatter_dimension=0, tiled=True),
        lax.psum_scatter(grad_upw, ROWS, scatter_dimension=0, tiled=True),
        lax.psum_scatter(grad_downw, ROWS, scatter_dimension=1, tiled=True),
    )
    return (
        block_out,
        input_grad,
        owned[0],
        owned[1],
        owned[2],
        owned[3],
        owned[4],
        owned[5],
        owned[6],
        owned[7],
        owned[8],
        owned[9],
        owned[10],
    )


MESH = pl.DeviceIdType.MESH
HBM = pl.BlockSpec(memory_space=pltpu.HBM)
VM = pl.BlockSpec(memory_space=pltpu.VMEM)
SLOTS = 160
NT = (((1,), (1,)), ((), ()))
TN = (((0,), (0,)), ((), ()))
BF = jnp.bfloat16
F32 = jnp.float32


class Net:
    def __init__(self, shards, send, recv, loc):
        self.C = shards
        self.send, self.recv, self.loc = send, recv, loc
        self.used = self.used_local = 0
        self.c, f, self.y = (lax.axis_index(a) for a in (CONTEXT, FSDP, HEADS))
        self.x, self.k = f // 2, f % 2

    def at(self, c=None, x=None, k=None, y=None):
        c, x, k, y = (own if v is None else v for v, own in ((c, self.c), (x, self.x), (k, self.k), (y, self.y)))
        return (c, 2 * x + k, y)

    def core(self):
        return self.at(k=1 - self.k)

    def over_x(self):
        return self.at(x=1 - self.x)

    def over_y(self):
        return self.at(y=1 - self.y)

    def shard(self, step):
        return lax.rem(self.c + step + self.C, self.C)

    def slot(self):
        self.used += 1
        return self.used - 1

    def remote(self, src, dst, slot, to):
        return pltpu.make_async_remote_copy(
            src_ref=src, dst_ref=dst, send_sem=self.send.at[slot], recv_sem=self.recv.at[slot],
            device_id=to, device_id_type=MESH,
        )

    def local(self, src, dst):
        self.used_local += 1
        return pltpu.make_async_copy(src, dst, self.loc.at[self.used_local - 1])

    def meet(self, devices):
        barrier = pltpu.get_barrier_semaphore()
        for to in devices:
            pl.semaphore_signal(barrier, inc=1, device_id=to, device_id_type=MESH)
        pl.semaphore_wait(barrier, len(devices))

    def group(self):
        return [
            self.at(c=self.shard(dc), k=(self.k + dk) % 2)
            for dc in range(self.C) for dk in range(2) if (dc, dk) != (0, 0)
        ]


def run(*parts):
    live = list(parts)
    while live:
        live = [p for p in live if next(p, 0) != 0]


def gather_rows(net, src, dst, half):
    C, c, k, y = net.C, net.c, net.k, net.y
    H = dst.shape[-1] // 2
    mine = pl.ds(pl.multiple_of(y * H, 128), H)
    other = pl.ds(pl.multiple_of((1 - y) * H, 128), H)
    own_cols = mine if half else pl.ds(0, 2 * H)
    own_half = src if half else src.at[:, mine]
    right, left = net.at(c=c + 1), net.at(c=c - 1)
    core, over_y = net.core(), net.over_y()
    keep = net.local(src, dst.at[k, c, :, own_cols])
    keep.start()
    hops = [(d, s) for s in range(1, C) for d in (0, 1)]
    zslot = {h: net.slot() for h in hops}
    yslot = {h: net.slot() for h in hops}
    aslot = {h: net.slot() for h in hops}
    bslot = {h: net.slot() for h in hops}
    own_core, own_y, own_core2 = net.slot(), net.slot(), net.slot()
    no_right, no_left = c < C - 1, c > 0

    def chunk(d, s):
        return (c - s, c - s >= 0) if d == 0 else (c + s, c + s < C)

    def z_send(d, s, source, q):
        to = right if d == 0 else left
        return net.remote(source, dst.at[k, q, :, mine], zslot[d, s], to)

    @pl.when(no_right)
    def _():
        z_send(0, 1, own_half, c).start()

    @pl.when(no_left)
    def _():
        z_send(1, 1, own_half, c).start()

    to_core = net.remote(src, dst.at[k, c, :, own_cols], own_core, core)
    to_core.start()
    if half:
        to_y = net.remote(src, dst.at[k, c, :, mine], own_y, over_y)
        to_y.start()
    yield 1
    for d, s in hops:
        q, valid = chunk(d, s)

        @pl.when(valid)
        def _(d=d, s=s, q=q):
            piece = dst.at[k, q, :, mine]
            z_send(d, s, piece, q).wait_recv()
            if s < C - 1:
                @pl.when(no_right if d == 0 else no_left)
                def _():
                    z_send(d, s + 1, piece, q).start()
            net.remote(piece, piece, yslot[d, s], over_y).start()
            net.remote(piece, piece, aslot[d, s], core).start()
        yield 1
    if half:
        piece = dst.at[k, c, :, other]
        net.remote(piece, piece, own_y, over_y).wait_recv()
        net.remote(piece, piece, own_core2, core).start()
    for d, s in hops:
        q, valid = chunk(d, s)

        @pl.when(valid)
        def _(d=d, s=s, q=q):
            piece = dst.at[k, q, :, other]
            net.remote(piece, piece, yslot[d, s], over_y).wait_recv()
            net.remote(piece, piece, bslot[d, s], core).start()
        yield 1
    to_core_in = net.remote(src, dst.at[1 - k, c, :, own_cols], own_core, core)
    to_core_in.wait_recv()
    to_core_in.wait_send()
    if half:
        piece = dst.at[1 - k, c, :, other]
        net.remote(piece, piece, own_core2, core).wait()
        to_y.wait_send()
    for d, s in hops:
        q, valid = chunk(d, s)

        @pl.when(valid)
        def _(d=d, s=s, q=q):
            a, b = dst.at[1 - k, q, :, mine], dst.at[1 - k, q, :, other]
            net.remote(a, a, aslot[d, s], core).wait()
            net.remote(b, b, bslot[d, s], core).wait()
            net.remote(a, a, yslot[d, s], over_y).wait_send()

        sent = jnp.logical_and(no_right if d == 0 else no_left, chunk(d, s - 1)[1])

        @pl.when(sent)
        def _(d=d, s=s):
            piece = dst.at[k, c, :, mine]
            z_send(d, s, piece, c).wait_send()
    keep.wait()
    yield 1


def deal_weights(net, groups):
    C, c, x, k = net.C, net.c, net.x, net.k
    steps = [(dc, dk) for dc in range(C) for dk in range(2)]
    zs = {(g, s): net.slot() for s in steps for g in range(len(groups))}
    xs = {(g, s): net.slot() for s in steps for g in range(len(groups))}
    mine = c * 4 + 2 * x + k
    keeps = []
    for s in steps[1:] + steps[:1]:
        dc, dk = s
        tc, tk = net.shard(dc), (k + dk) % 2
        for g, (pieces, whole) in enumerate(groups):
            for src, pick, put in pieces:
                if s == (0, 0):
                    net.remote(src.at[pick(tc, tk)], put(mine), xs[g, s], net.over_x()).start()
                    keep = net.local(src.at[pick(tc, tk)], put(mine))
                    keep.start()
                    keeps.append(keep)
                else:
                    net.remote(src.at[pick(tc, tk)], put(mine), zs[g, s], net.at(c=tc, k=tk)).start()
        if dk:
            yield 1
    for s in steps[1:]:
        dc, dk = s
        fc, fk = net.shard(-dc), (k + dk) % 2
        for g, (pieces, whole) in enumerate(groups):
            block = whole(fc * 4 + 2 * x + fk)
            net.remote(block, block, zs[g, s], net.over_x()).wait_recv()
            net.remote(block, block, xs[g, s], net.over_x()).start()
        yield 1
    for s in steps:
        dc, dk = s
        fc, fk = net.shard(-dc), (k + dk) % 2
        for g, (pieces, whole) in enumerate(groups):
            block = whole(fc * 4 + 2 * (1 - x) + fk)
            net.remote(block, block, xs[g, s], net.over_x()).wait()
            if s != (0, 0):
                net.remote(block, block, zs[g, s], net.over_x()).wait_send()
        yield 1
    for keep in keeps:
        keep.wait()
    yield 1


def reduce_scratch(C, rows, width, tiles):
    w = width // tiles
    return [
        pltpu.VMEM((tiles, C, rows, w), BF),
        pltpu.VMEM((tiles, C, rows, w), BF),
        pltpu.VMEM((tiles // 2, C, rows, w), BF),
        pltpu.VMEM((tiles // 2, C, rows, w), BF),
        pltpu.VMEM((tiles // 2, C, rows, w), F32),
        pltpu.VMEM((tiles // 2, C - 1, rows, w), BF),
        pltpu.VMEM((tiles // 2, C - 1, rows, w), BF),
    ]


def reduce_rows(net, product, scratch, out):
    osend, orecv, ysend, yrecv, sums, zsend, zrecv = scratch
    tiles, C, rows, w = osend.shape
    n = tiles // 2
    k, y = net.k, net.y
    core, over_y = net.core(), net.over_y()
    column = [(1 - y) * n + j for j in range(n)] + [y * n + j for j in range(n)]
    copies = []
    for j in range(tiles):
        osend[j] = product(1 - k, column[j]).astype(BF).reshape(C, rows, w)
        cp = net.remote(osend.at[j], orecv.at[j], net.slot(), core)
        cp.start()
        copies.append(cp)
        yield 1
    ycopies = []
    for j in range(n):
        own = product(k, column[j]).reshape(C, rows, w)
        copies[j].wait_recv()
        ysend[j] = (own + orecv[j].astype(F32)).astype(BF)
        cp = net.remote(ysend.at[j], yrecv.at[j], net.slot(), over_y)
        cp.start()
        ycopies.append(cp)
        yield 1
    zcopies = []
    for j in range(n):
        own = product(k, column[n + j]).reshape(C, rows, w)
        copies[n + j].wait_recv()
        own = own + orecv[n + j].astype(F32)
        sums[j] = own
        ycopies[j].wait_recv()
        sums[j] = sums[j] + yrecv[j].astype(F32)
        for dc in range(1, C):
            to = net.shard(dc)
            zsend[j, dc - 1] = sums[j, to].astype(BF)
            cp = net.remote(zsend.at[j, dc - 1], zrecv.at[j, dc - 1], net.slot(), net.at(c=to))
            cp.start()
            zcopies.append(cp)
        yield 1
    for j in range(n):
        total = sums[j, net.c]
        for dc in range(1, C):
            zcopies[j * (C - 1) + dc - 1].wait_recv()
            total = total + zrecv[j, dc - 1].astype(F32)
        out[j] = total
        yield 1
    for cp in copies + ycopies + zcopies:
        cp.wait_send()
    yield 1


def deal_grads(net, groups):
    C, c, x, k = net.C, net.c, net.x, net.k
    steps = [(dc, dk) for dc in range(C) for dk in range(2)]
    order = steps[1:] + steps[:1]
    over_x = net.over_x()
    xs = {}
    for s in order:
        for g, (grad, pick, xbuf, stage, puts, own_put) in enumerate(groups):
            b = net.shard(s[0]) * 4 + 2 * (1 - x) + (k + s[1]) % 2
            cp = net.remote(grad.at[pick(b)], xbuf.at[2 * s[0] + s[1]], net.slot(), over_x)
            cp.start()
            xs[g, s] = cp
    yield 1
    zs = []
    for s in order:
        tc, tk = net.shard(s[0]), (k + s[1]) % 2
        i = 2 * s[0] + s[1]
        for g, (grad, pick, xbuf, stage, puts, own_put) in enumerate(groups):
            b = tc * 4 + 2 * x + tk
            xs[g, s].wait_recv()
            total = grad[pick(b)].astype(F32) + xbuf[i].astype(F32)
            if s == (0, 0):
                own_put(total)
            else:
                stage[i] = total.astype(BF)
                slot = net.slot()
                for take, put in puts:
                    net.remote(stage.at[(i,) + take], put(c, k), slot, net.at(c=tc, k=tk)).start()
                zs.append((g, s, slot))
        yield 1
    for g, s, slot in zs:
        grad, pick, xbuf, stage, puts, own_put = groups[g]
        i = 2 * s[0] + s[1]
        net.remote(stage.at[i], stage.at[i], slot, over_x).wait()
        yield 1
    for cp in xs.values():
        cp.wait_send()
    yield 1


def half_of(ref, y, width):
    return ref[:, pl.ds(pl.multiple_of(y * width, 128), width)]


def gain_half(gains, y, row, blocks):
    return [gains[y * blocks + i].astype(F32)[row:row + 1] for i in range(blocks)]


def times_gain(value, rows):
    w = value.shape[1] // len(rows)
    return jnp.concatenate([value[:, i * w:(i + 1) * w] * r for i, r in enumerate(rows)], axis=1)


def swap_sums(net, part, out_buf, in_buf):
    out_buf[...] = jnp.broadcast_to(part, out_buf.shape)
    cp = net.remote(out_buf, in_buf, net.slot(), net.over_y())
    cp.start()
    cp.wait()
    return part + in_buf[:, 0:1]


def open_kernel(C, unit, x_ref, g_ref, wq, wk, wv, wo, xg, gains, wqkv, wod, xn, send, recv, loc):
    net = Net(C, send, recv, loc)
    c, x, k = net.c, net.x, net.k
    head = unit
    B = wq.shape[0]
    plane = [(dc, dx, dk) for dc in range(C) for dx in range(2) for dk in range(2)][1:]
    mates = [net.at(c=net.shard(dc), x=(x + dx) % 2, k=(k + dk) % 2) for dc, dx, dk in plane]
    net.meet(mates + [net.over_y()])
    me = c * 4 + 2 * x + k
    own = net.local(g_ref, gains.at[me])
    own.start()
    sent = []
    for (dc, dx, dk), to in zip(plane, mates):
        cp = net.remote(g_ref, gains.at[me], net.slot(), to)
        cp.start()
        sent.append(cp)
    full = slice(None)
    lanes = lambda n, w: pl.ds(pl.multiple_of(n * w, 128), w)
    rows = lambda b: pl.ds(pl.multiple_of(b * B, B), B)
    groups = [
        ([(wq, lambda tc, tk: (full, lanes(2 * tc + tk, head)), lambda b: wqkv.at[rows(b), pl.ds(0, head)]),
          (wk, lambda tc, tk: (full, lanes(tc, head)), lambda b: wqkv.at[rows(b), pl.ds(head, head)]),
          (wv, lambda tc, tk: (full, lanes(tc, head)), lambda b: wqkv.at[rows(b), pl.ds(2 * head, head)])],
         lambda b: wqkv.at[rows(b), :]),
        ([(wo, lambda tc, tk: (pl.ds(pl.multiple_of((2 * tc + tk) * head, head), head), full),
           lambda b: wod.at[:, lanes(b, B)])],
         lambda b: wod.at[:, lanes(b, B)]),
    ]
    weights = deal_weights(net, groups)
    next(weights)
    own.wait()
    for cp in sent:
        cp.wait()
    value = x_ref[...].astype(F32)
    hat = value * lax.rsqrt(jnp.mean(value * value, axis=-1, keepdims=True) + EPS)
    blocks = gains.shape[0]
    xn[...] = times_gain(hat, [gains[b].astype(F32)[0:1] for b in range(blocks)]).astype(BF)
    run(gather_rows(net, xn, xg, False), weights)


def middle_kernel(C, tiles, a_ref, wo_ref, x_ref, gains, cot, wg, wu, wd, hg, cotg, wgu, wdd, h_out, scale_out,
                  red, hn, s_out, s_in, rs, send, recv, loc):
    net = Net(C, send, recv, loc)
    y = net.y
    H = h_out.shape[1]
    B, unit = wg.shape[0], wdd.shape[0]
    w = H * 2 // tiles
    net.meet(net.group() + [net.over_x(), net.over_y()])
    full = slice(None)
    lanes = lambda n, m: pl.ds(pl.multiple_of(n * m, 128), m)
    rows = lambda b: pl.ds(pl.multiple_of(b * B, B), B)
    groups = [
        ([(wg, lambda tc, tk: (full, lanes(2 * tc + tk, unit)), lambda b: wgu.at[rows(b), pl.ds(0, unit)]),
          (wu, lambda tc, tk: (full, lanes(2 * tc + tk, unit)), lambda b: wgu.at[rows(b), pl.ds(unit, unit)])],
         lambda b: wgu.at[rows(b), :]),
        ([(wd, lambda tc, tk: (pl.ds(pl.multiple_of((2 * tc + tk) * unit, 128), unit), full),
           lambda b: wdd.at[:, lanes(b, B)])],
         lambda b: wdd.at[:, lanes(b, B)]),
    ]
    weights = deal_weights(net, groups)
    cots = gather_rows(net, cot, cotg, False)

    def product(kk, tile):
        return jnp.dot(a_ref[kk], wo_ref[:, lanes(tile, w)], preferred_element_type=F32)

    next(cots)
    next(weights)
    run(reduce_rows(net, product, red, rs), weights, cots)
    half = half_of(x_ref, y, H).astype(F32) + jnp.concatenate([rs[j] for j in range(tiles // 2)], axis=1)
    total = swap_sums(net, jnp.sum(half * half, axis=-1, keepdims=True), s_out, s_in)
    scale = lax.rsqrt(total / (2 * H) + EPS)
    h_out[...] = half
    scale_out[...] = jnp.broadcast_to(scale, scale_out.shape)
    hn[...] = times_gain(half * scale, gain_half(gains, y, 1, gains.shape[0] // 2)).astype(BF)
    run(gather_rows(net, hn, hg, True))


def turn_kernel(C, tiles, act, wdd, ggu, wgu, h_ref, scale_ref, gains, cot, ghg, blk, gh_out, part_out,
                red, red2, gb, s_out, s_in, rs, rs2, send, recv, loc):
    net = Net(C, send, recv, loc)
    y = net.y
    H = h_ref.shape[1]
    w = H * 2 // tiles
    net.meet([net.at(c=net.shard(dc)) for dc in range(1, C)] + [net.core(), net.over_y()])
    lanes = lambda n, m: pl.ds(pl.multiple_of(n * m, 128), m)

    def down(kk, tile):
        return jnp.dot(act[kk], wdd[:, lanes(tile, w)], preferred_element_type=F32)

    def normed(kk, tile):
        return lax.dot_general(ggu[kk], wgu[lanes(tile, w), :], NT, preferred_element_type=F32)

    run(reduce_rows(net, normed, red2, rs2), reduce_rows(net, down, red, rs))
    h = h_ref[...]
    blk[y] = (h + jnp.concatenate([rs[j] for j in range(tiles // 2)], axis=1)).astype(BF)
    swap = net.remote(blk.at[y], blk.at[y], net.slot(), net.over_y())
    swap.start()
    g = jnp.concatenate([rs2[j] for j in range(tiles // 2)], axis=1)
    scale = scale_ref[:, 0:1]
    hat = h * scale
    col = jnp.sum(g * hat, axis=0, keepdims=True)
    for i in range(part_out.shape[0]):
        n = part_out.shape[1]
        part_out[i:i + 1] = col[:, i * n:(i + 1) * n]
    m = times_gain(g, gain_half(gains, y, 1, gains.shape[0] // 2))
    mean = swap_sums(net, jnp.sum(m * hat, axis=-1, keepdims=True), s_out, s_in) / (2 * H)
    gh = half_of(cot, y, H).astype(F32) + scale * (m - hat * mean)
    gh_out[...] = gh
    gb[...] = gh.astype(BF)
    run(gather_rows(net, gb, ghg, True))
    swap.wait()


def close_kernel(C, tiles, a_ref, w_ref, x_ref, gains, gh_ref, parts, dgu, dd, dq, do,
                 ig, sums_out, g_out, u_out, d_out, q_out, kv_out, o_out,
                 red, s_out, s_in, rs, xgu, zgu, xd, zd, xq, zq, xo, zo, vec, vin, vx, vz, send, recv, loc):
    net = Net(C, send, recv, loc)
    c, y, k = net.c, net.y, net.k
    H = gh_ref.shape[1]
    w = H * 2 // tiles
    B = g_out.shape[0]
    unit, head = dd.shape[0], do.shape[0]
    net.meet(net.group() + [net.over_x(), net.over_y()])
    full = slice(None)
    lanes = lambda n, m: pl.ds(pl.multiple_of(n * m, 128), m)
    rows = lambda b: (pl.ds(pl.multiple_of(b * B, B), B), full)
    cols = lambda b: (full, lanes(b, B))
    me = 2 * c + k

    def put_gu(v):
        g_out[:, lanes(me, unit)] = v[:, :unit].astype(BF)
        u_out[:, lanes(me, unit)] = v[:, unit:].astype(BF)

    def put_d(v):
        d_out[pl.ds(pl.multiple_of(me * unit, 128), unit), :] = v.astype(BF)

    def put_q(v):
        q_out[:, lanes(me, head)] = v[:, :head].astype(BF)
        kv_out[k, :, lanes(c, head)] = v[:, head:].astype(BF)

    def put_o(v):
        o_out[pl.ds(pl.multiple_of(me * head, 128), head), :] = v.astype(BF)

    groups = [
        (dgu, rows, xgu, zgu,
         [((full, pl.ds(0, unit)), lambda a, b: g_out.at[:, lanes(2 * a + b, unit)]),
          ((full, pl.ds(unit, unit)), lambda a, b: u_out.at[:, lanes(2 * a + b, unit)])], put_gu),
        (dd, cols, xd, zd,
         [((full, full), lambda a, b: d_out.at[pl.ds(pl.multiple_of((2 * a + b) * unit, 128), unit), :])], put_d),
        (dq, rows, xq, zq,
         [((full, pl.ds(0, head)), lambda a, b: q_out.at[:, lanes(2 * a + b, head)]),
          ((full, pl.ds(head, head)), lambda a, b: kv_out.at[b, :, lanes(a, head)])], put_q),
        (do, cols, xo, zo,
         [((full, full), lambda a, b: o_out.at[pl.ds(pl.multiple_of((2 * a + b) * head, 128), head), :])], put_o),
    ]

    def product(kk, tile):
        return lax.dot_general(a_ref[kk], w_ref[lanes(tile, w), :], NT, preferred_element_type=F32)

    grads = deal_grads(net, groups)
    next(grads)
    run(reduce_rows(net, product, red, rs))
    value = x_ref[...].astype(F32)
    scale = lax.rsqrt(jnp.mean(value * value, axis=-1, keepdims=True) + EPS)
    hat = half_of(x_ref, y, H).astype(F32) * scale
    g = jnp.concatenate([rs[j] for j in range(tiles // 2)], axis=1)
    col = jnp.sum(g * hat, axis=0, keepdims=True)
    n = vec.shape[2]
    count = H // n
    vec[0] = parts[...]
    for i in range(count):
        vec[0, i:i + 1] = col[:, i * n:(i + 1) * n]
    first = net.remote(vec.at[0], vin, net.slot(), net.core())
    first.start()
    m = times_gain(g, gain_half(gains, y, 0, gains.shape[0] // 2))
    mean = swap_sums(net, jnp.sum(m * hat, axis=-1, keepdims=True), s_out, s_in) / (2 * H)
    ig[y] = (gh_ref[...] + scale * (m - hat * mean)).astype(BF)
    swap = net.remote(ig.at[y], ig.at[y], net.slot(), net.over_y())
    swap.start()
    first.wait()
    vec[1] = vec[0] + vin[...]
    second = net.remote(vec.at[1], vx, net.slot(), net.over_x())
    second.start()
    second.wait()
    vz[c] = vec[1] + vx[...]
    third = []
    for dc in range(1, C):
        cp = net.remote(vz.at[c], vz.at[c], net.slot(), net.at(c=net.shard(dc)))
        cp.start()
        third.append(cp)
    run(grads)
    for cp in third:
        cp.wait()
    total = vz[0]
    for i in range(1, C):
        total = total + vz[i]
    sums_out[y] = total
    last = net.remote(sums_out.at[y], sums_out.at[y], net.slot(), net.over_y())
    last.start()
    last.wait()
    swap.wait()


def attend_kernel(C, scale, tile, q_ref, kv, qp, kp, o_ref, lse_ref, kvp, m_s, l_s, acc, send, recv, loc):
    net = Net(C, send, recv, loc)
    head = q_ref.shape[1]
    net.meet([net.over_x()])
    swap = net.remote(kv, kvp, 0, net.over_x())
    swap.start()
    steps = q_ref.shape[0] // tile

    def own(i, _):
        r = pl.ds(pl.multiple_of(i * tile, tile), tile)
        s = lax.dot_general(q_ref[r], kv[:, :head], NT, preferred_element_type=F32) * scale
        s = jnp.where(kp[0:1] <= qp[r, 0:1], s, NEG)
        top = jnp.max(s, axis=-1, keepdims=True)
        e = jnp.exp(s - top)
        m_s[r] = jnp.broadcast_to(top, (tile, 128))
        l_s[r] = jnp.broadcast_to(jnp.sum(e, axis=-1, keepdims=True), (tile, 128))
        acc[r] = jnp.dot(e.astype(BF), kv[:, head:], preferred_element_type=F32)
        return 0

    lax.fori_loop(0, steps, own, 0)
    swap.wait()

    @pl.when(net.x == 1)
    def _():
        def more(i, _):
            r = pl.ds(pl.multiple_of(i * tile, tile), tile)
            s = lax.dot_general(q_ref[r], kvp[:, :head], NT, preferred_element_type=F32) * scale
            old = m_s[r, 0:1]
            top = jnp.maximum(old, jnp.max(s, axis=-1, keepdims=True))
            e = jnp.exp(s - top)
            shrink = jnp.exp(old - top)
            m_s[r] = jnp.broadcast_to(top, (tile, 128))
            l_s[r] = jnp.broadcast_to(l_s[r, 0:1] * shrink + jnp.sum(e, axis=-1, keepdims=True), (tile, 128))
            acc[r] = acc[r] * shrink + jnp.dot(e.astype(BF), kvp[:, head:], preferred_element_type=F32)
            return 0

        lax.fori_loop(0, steps, more, 0)

    o_ref[...] = (acc[...] / l_s[...]).astype(BF)
    lse_ref[...] = m_s[...] + jnp.log(l_s[...])


def attend_back_kernel(C, scale, tile, q_ref, kv, kvp, do, lse, delta, qp, kp, dq, kvg, own, peer, cin, xs, xin,
                       send, recv, loc):
    net = Net(C, send, recv, loc)
    head = q_ref.shape[1]
    k = net.k
    net.meet([net.over_x(), net.core()])
    steps = q_ref.shape[0] // tile
    dq[...] = jnp.zeros_like(dq)
    own[...] = jnp.zeros_like(own)

    def sweep(keys, grads, masked):
        def step(i, _):
            r = pl.ds(pl.multiple_of(i * tile, tile), tile)
            q, g = q_ref[r], do[r]
            s = lax.dot_general(keys[:, :head], q, NT, preferred_element_type=F32) * scale
            p = jnp.exp(s - lse[0:1, r])
            if masked:
                p = jnp.where(kp[:, 0:1] <= qp[0:1, r], p, 0.0)
            grads[1] += jnp.dot(p.astype(BF), g, preferred_element_type=F32)
            dp = lax.dot_general(keys[:, head:], g, NT, preferred_element_type=F32)
            ds = (p * (dp - delta[0:1, r])).astype(BF)
            grads[0] += jnp.dot(ds, q, preferred_element_type=F32)
            dq[r] += lax.dot_general(ds, keys[:, :head], TN, preferred_element_type=F32)
            return 0

        lax.fori_loop(0, steps, step, 0)

    one = net.remote(peer.at[1 - k], cin.at[0], net.slot(), net.core())
    two = net.remote(xs, xin, net.slot(), net.over_x())
    three = net.remote(own.at[1 - k], cin.at[1], net.slot(), net.core())

    @pl.when(net.x == 1)
    def _():
        peer[...] = jnp.zeros_like(peer)
        sweep(kvp, peer, False)
        one.start()
        one.wait()
        xs[...] = peer[k] + cin[0]
        two.start()

    sweep(kv, own, True)
    three.start()
    three.wait()
    dq[...] = dq[...] * scale
    kvg[...] = own[k] + cin[1]

    @pl.when(net.x == 1)
    def _():
        two.wait_send()

    @pl.when(net.x == 0)
    def _():
        two.wait_recv()
        kvg[...] = kvg[...] + xin[...]

    @pl.when(k == 0)
    def _():
        kvg[...] = kvg[...] * scale


def call(kernel, name, cid, out_shape, in_specs, out_specs, scratch, *args):
    return pl.pallas_call(
        kernel, name=name, out_shape=out_shape, in_specs=in_specs, out_specs=out_specs,
        scratch_shapes=scratch + [
            pltpu.SemaphoreType.DMA((SLOTS,)), pltpu.SemaphoreType.DMA((SLOTS,)), pltpu.SemaphoreType.DMA((32,)),
        ],
        compiler_params=pltpu.CompilerParams(
            collective_id=cid, has_side_effects=True, vmem_limit_bytes=60 * 1024 * 1024
        ),
    )(*args)


def tensor_parallel(layer_input, block_pair, attn_gain, q_weight, key_projection, value_projection, q_gain, k_gain,
                    o_weight, mlp_gain, gate_weight, up_weight, down_weight, cotangent):
    C = lax.axis_size(CONTEXT)
    R, D = layer_input.shape
    B = q_weight.shape[0]
    NB = 4 * C
    T = 2 * C * R
    H = D // 2
    head = HEAD_SIZE
    unit = gate_weight.shape[1] // (2 * C)
    scale = 1.0 / math.sqrt(head)
    S = jax.ShapeDtypeStruct
    k = lax.axis_index(FSDP) % 2
    x = lax.axis_index(FSDP) // 2
    TILES = 8

    pad = lambda v: jnp.pad(v, (0, B - v.shape[0]))
    packed = jnp.pad(jnp.stack([attn_gain, mlp_gain, pad(q_gain), pad(k_gain)]), ((0, 12), (0, 0)))
    xg, gains, wqkv, wo = call(
        functools.partial(open_kernel, C, head), "open", 1,
        (S((2, C, R, D), BF), S((NB, 16, B), BF), S((D, 3 * head), BF), S((head, D), BF)),
        [VM, VM, HBM, HBM, HBM, HBM], (HBM, VM, HBM, HBM),
        [pltpu.VMEM((R, D), BF)],
        layer_input, packed, q_weight, key_projection, value_projection, o_weight,
    )
    xt = xg.reshape(T, D)
    qgain = gains[:, 2, :q_gain.shape[0]].reshape(head).astype(F32)
    kgain = gains[:, 3, :k_gain.shape[0]].reshape(head).astype(F32)
    order = jnp.arange(T, dtype=jnp.int32)
    ids = (order // R % C) * (4 * R) + x * (2 * R) + (order // (C * R)) * R + order % R
    places = row_places(block_pair, ids, 2 * R)
    cosine, sine = (t[:, 0, :] for t in rope_tables(places, head))
    raw = jnp.dot(xt, wqkv, preferred_element_type=F32)
    q_hat, q_scale = row_norm(raw[:, :head])
    k_hat, k_scale = row_norm(raw[:, head:2 * head])
    q_rot = apply_rotary(q_hat * qgain, cosine, sine).astype(BF)
    k_rot = apply_rotary(k_hat * kgain, cosine, sine).astype(BF)
    kv = jnp.concatenate([k_rot, raw[:, 2 * head:].astype(BF)], axis=1)
    p_col = jnp.broadcast_to(places[:, None], (T, 128))
    p_row = jnp.broadcast_to(places[None, :], (8, T))
    attn_o, lse, kvp = call(
        functools.partial(attend_kernel, C, scale, 256), "attend", 2,
        (S((T, head), BF), S((T, 128), F32), S((T, 2 * head), BF)),
        [VM] * 4, (VM,) * 3,
        [pltpu.VMEM((T, 128), F32), pltpu.VMEM((T, 128), F32), pltpu.VMEM((T, head), F32)],
        q_rot, kv, p_col, p_row,
    )
    red = lambda: reduce_scratch(C, R, D, TILES)
    rs = lambda: pltpu.VMEM((TILES // 2, R, D // TILES), F32)
    stat = lambda: pltpu.VMEM((R, 128), F32)
    hg, cotg, wgu, wd, h_half, h_scale = call(
        lambda *r: middle_kernel(C, TILES, *r[:14], r[14:21], *r[21:]), "middle", 3,
        (S((2, C, R, D), BF), S((2, C, R, D), BF), S((D, 2 * unit), BF), S((unit, D), BF), S((R, H), F32),
         S((R, 128), F32)),
        [VM] * 5 + [HBM] * 3, (HBM, HBM, HBM, HBM, VM, VM),
        red() + [pltpu.VMEM((R, H), BF), stat(), stat(), rs()],
        attn_o.reshape(2, C * R, head), wo, layer_input, gains, cotangent, gate_weight, up_weight, down_weight,
    )
    ht, ct = hg.reshape(T, D), cotg.reshape(T, D)
    gu = jnp.dot(ht, wgu, preferred_element_type=F32)
    gate, up = gu[:, :unit], gu[:, unit:]
    sigma = jax.nn.sigmoid(gate)
    silu = gate * sigma
    act = (silu * up).astype(BF)
    grad_act = jnp.einsum("td,fd->tf", ct, wd, preferred_element_type=F32)
    grad_g = (grad_act * up * (sigma * (1.0 + gate * (1.0 - sigma)))).astype(BF)
    grad_u = (grad_act * silu).astype(BF)
    ggu = jnp.concatenate([grad_g, grad_u], axis=1)
    dd = jnp.einsum("tf,td->fd", act, ct, preferred_element_type=F32).astype(BF)
    dgu = jnp.einsum("tc,tf->cf", ht, ggu, preferred_element_type=F32).astype(BF)
    ghg, blk, gh_half, mlp_part = call(
        lambda *r: turn_kernel(C, TILES, *r[:12], r[12:19], r[19:26], *r[26:]), "turn", 4,
        (S((2, C, R, D), BF), S((2, R, H), BF), S((R, H), F32), S((H // 128, 128), F32)),
        [VM] * 8, (HBM, VM, VM, VM),
        red() + red() + [pltpu.VMEM((R, H), BF), stat(), stat(), rs(), rs()],
        act.reshape(2, C * R, unit), wd, ggu.reshape(2, C * R, 2 * unit), wgu, h_half, h_scale, gains, cotangent,
    )
    gt = ghg.reshape(T, D)
    grad_o = jnp.einsum("td,qd->tq", gt, wo, preferred_element_type=F32).astype(BF)
    do_w = jnp.einsum("tq,td->qd", attn_o, gt, preferred_element_type=F32).astype(BF)
    delta = jnp.sum(grad_o.astype(F32) * attn_o.astype(F32), axis=-1)
    row = lambda v: jnp.broadcast_to(v[None, :], (8, T))
    dq, kvg = call(
        functools.partial(attend_back_kernel, C, scale, 256), "attend_back", 5,
        (S((T, head), F32), S((T, head), F32)),
        [VM] * 8, (VM, VM),
        [pltpu.VMEM((2, T, head), F32), pltpu.VMEM((2, T, head), F32), pltpu.VMEM((2, T, head), F32),
         pltpu.VMEM((T, head), F32), pltpu.VMEM((T, head), F32)],
        q_rot, kv, kvp, grad_o, row(lse[:, 0]), row(delta), p_row, p_col,
    )
    grad_qg = unrotate(dq, cosine, sine)
    q_part = jnp.sum(grad_qg * q_hat, axis=0)
    grad_q = norm_backward(grad_qg * qgain, q_hat, q_scale).astype(BF)
    grad_kg = unrotate(kvg, cosine, sine)
    k_part = jnp.where(k == 0, jnp.sum(grad_kg * k_hat, axis=0), 0.0)
    grad_k = norm_backward(grad_kg * kgain, k_hat, k_scale).astype(BF)
    kv_grad = jnp.where(k == 0, grad_k, kvg.astype(BF))
    gqk = jnp.concatenate([grad_q, kv_grad], axis=1)
    w_kv = jnp.where(k == 0, wqkv[:, head:2 * head], wqkv[:, 2 * head:])
    wqk = jnp.concatenate([wqkv[:, :head], w_kv], axis=1)
    dqk = jnp.einsum("tc,tq->cq", xt, gqk, preferred_element_type=F32).astype(BF)
    n_rows = H // 128
    parts = jnp.concatenate(
        [jnp.zeros_like(mlp_part), mlp_part, q_part[None], k_part[None], jnp.zeros((6, 128), F32)], axis=0
    )
    V = parts.shape
    ig, sums, g_w, u_w, d_w, q_w, kv_w, o_w = call(
        lambda *r: close_kernel(C, TILES, *r[:18], r[18:25], *r[25:]), "close", 6,
        (S((2, R, H), BF), S((2,) + V, F32), S((B, 2 * C * unit), BF), S((B, 2 * C * unit), BF),
         S((2 * C * unit, B), BF), S((B, 2 * C * head), BF), S((2, B, C * head), BF), S((2 * C * head, B), BF)),
        [VM] * 10, (VM,) * 8,
        red() + [stat(), stat(), rs()]
        + [pltpu.VMEM((2 * C, B, 2 * unit), BF)] * 2 + [pltpu.VMEM((2 * C, unit, B), BF)] * 2
        + [pltpu.VMEM((2 * C, B, 2 * head), BF)] * 2 + [pltpu.VMEM((2 * C, head, B), BF)] * 2
        + [pltpu.VMEM((2,) + V, F32), pltpu.VMEM(V, F32), pltpu.VMEM(V, F32), pltpu.VMEM((C,) + V, F32)],
        gqk.reshape(2, C * R, 2 * head), wqk, layer_input, gains, gh_half, parts, dgu, dd, dqk, do_w,
    )
    join = lambda v: jnp.concatenate([v[0], v[1]], axis=1)
    mine = lax.axis_index(CONTEXT) * 4 + lax.axis_index(FSDP)
    both = sums[:, :n_rows].reshape(2 * n_rows, 128)
    both_mlp = sums[:, n_rows:2 * n_rows].reshape(2 * n_rows, 128)
    pick = lambda v: lax.dynamic_slice_in_dim(v.reshape(-1), mine * B, B)
    few = q_gain.shape[0]
    pick_few = lambda v: lax.dynamic_slice_in_dim(v, mine * few, few)
    head_sums = sums[0, 2 * n_rows:] + sums[1, 2 * n_rows:]
    return (
        join(blk), join(ig).astype(F32), pick(both), q_w.astype(F32), kv_w[0].astype(F32), kv_w[1].astype(F32),
        pick_few(head_sums[0]), pick_few(head_sums[1]), o_w.astype(F32), pick(both_mlp), g_w.astype(F32),
        u_w.astype(F32), d_w.astype(F32),
    )


def fits(mesh_shape, layer_input, q_weight, key_projection, gate_weight):
    C = mesh_shape[CONTEXT]
    return (
        mesh_shape[FSDP] == 4 and mesh_shape[HEADS] == 2
        and key_projection.shape[1] == C * HEAD_SIZE and q_weight.shape[1] == 2 * C * HEAD_SIZE
        and gate_weight.shape[1] % (2 * C * 128) == 0 and q_weight.shape[0] == 128
        and layer_input.shape[0] % 128 == 0 and layer_input.shape[1] % (8 * 128) == 0
    )


def solution(mesh):
    def program(*args):
        layer_input, q_weight, key_projection, gate_weight = args[0], args[3], args[4], args[10]
        if fits(dict(mesh.shape), layer_input, q_weight, key_projection, gate_weight):
            return tensor_parallel(*args)
        return per_device(*args)

    return jax.shard_map(
        program,
        mesh=mesh,
        in_specs=(
            P(ROWS, None),
            P(),
            P(ROWS),
            P(ROWS, HEADS),
            P(ROWS, HEADS),
            P(ROWS, HEADS),
            P(ROWS),
            P(ROWS),
            P(HEADS, ROWS),
            P(ROWS),
            P(ROWS, HEADS),
            P(ROWS, HEADS),
            P(HEADS, ROWS),
            P(ROWS, None),
        ),
        out_specs=(
            P(ROWS, None),
            P(ROWS, None),
            P(ROWS),
            P(ROWS, HEADS),
            P(ROWS, HEADS),
            P(ROWS, HEADS),
            P(ROWS),
            P(ROWS),
            P(HEADS, ROWS),
            P(ROWS),
            P(ROWS, HEADS),
            P(ROWS, HEADS),
            P(HEADS, ROWS),
        ),
        check_vma=False,
    )
```

```python
import functools
import math

import jax
import jax.numpy as jnp
from jax import lax
from jax.experimental import pallas as pl
from jax.experimental.pallas import tpu as pltpu
from jax.sharding import PartitionSpec as P

HEAD_SIZE = 128
CONTEXT, FSDP, HEADS = "context", "fsdp", "heads"
ROWS = (CONTEXT, FSDP)


EPS = 1e-06
THETA = 1000000.0
NEG = -1e30


def row_places(block_pair, row_ids, block_len):
    owners = block_pair.shape[0]
    holder = row_ids // (2 * block_len)
    within = row_ids % (2 * block_len)
    match = holder[:, None] == jnp.arange(owners, dtype=jnp.int32)[None, :]
    paired = jnp.sum(jnp.where(match, block_pair[None, :], 0), axis=1)
    which = jnp.where(within >= block_len, 2 * owners - 1 - paired, paired)
    return which * block_len + within % block_len


def rope_tables(places, head_dim):
    half = head_dim // 2
    freq = jnp.exp(jnp.arange(half, dtype=jnp.float32) * (-2.0 * math.log(THETA) / head_dim))
    angle = places.astype(jnp.float32)[:, None] * freq[None, :]
    return (jnp.cos(angle)[:, None, :], jnp.sin(angle)[:, None, :])


def apply_rotary(field, cosine_table, sine_table):
    half = field.shape[-1] // 2
    first = field[..., :half]
    second = field[..., half:]
    return jnp.concatenate(
        [first * cosine_table - second * sine_table, second * cosine_table + first * sine_table],
        axis=-1,
    )


def unrotate(grad, cosine_table, sine_table):
    half = grad.shape[-1] // 2
    first = grad[..., :half]
    second = grad[..., half:]
    return jnp.concatenate(
        [first * cosine_table + second * sine_table, second * cosine_table - first * sine_table],
        axis=-1,
    )


def row_norm(field):
    factor = lax.rsqrt(jnp.mean(field * field, axis=-1, keepdims=True) + EPS)
    return (field * factor, factor)


def norm_backward(grad_hat, normed, factor):
    return factor * (grad_hat - normed * jnp.mean(grad_hat * normed, axis=-1, keepdims=True))


def masked_scores(query_matrix, key_rows, query_places, key_places, softmax_scale):
    score_matrix = (
        jnp.einsum("oblh,wbh->blow", query_matrix, key_rows, preferred_element_type=jnp.float32)
        * softmax_scale
    )
    allowed = key_places[None, :] <= query_places[:, None]
    return (jnp.where(allowed, score_matrix, NEG), allowed)


def per_device(
    layer_input,
    block_pair,
    attn_gain,
    q_weight,
    key_projection,
    value_projection,
    q_gain,
    k_gain,
    o_weight,
    mlp_gain,
    gate_weight,
    up_weight,
    down_weight,
    cotangent,
):
    wide_float_type = jnp.float32
    narrow_float_type = jnp.bfloat16
    tokens = layer_input.shape[0]
    members = lax.axis_size(ROWS)
    seq_len = tokens * members
    block_len = tokens * lax.axis_size(FSDP) // 2
    kv_local = key_projection.shape[1] // HEAD_SIZE
    q_local = q_weight.shape[1] // HEAD_SIZE
    group_size = q_local // kv_local
    softmax_scale = 1.0 / math.sqrt(HEAD_SIZE)
    (
        full_attn_gain,
        full_q,
        full_k,
        full_v,
        full_q_gain,
        full_k_gain,
        full_o,
        full_mlp_gain,
        full_gate,
        full_up,
        full_down,
    ) = (
        lax.all_gather(attn_gain, ROWS, axis=0, tiled=True),
        lax.all_gather(q_weight, ROWS, axis=0, tiled=True),
        lax.all_gather(key_projection, ROWS, axis=0, tiled=True),
        lax.all_gather(value_projection, ROWS, axis=0, tiled=True),
        lax.all_gather(q_gain, ROWS, axis=0, tiled=True),
        lax.all_gather(k_gain, ROWS, axis=0, tiled=True),
        lax.all_gather(o_weight, ROWS, axis=1, tiled=True),
        lax.all_gather(mlp_gain, ROWS, axis=0, tiled=True),
        lax.all_gather(gate_weight, ROWS, axis=0, tiled=True),
        lax.all_gather(up_weight, ROWS, axis=0, tiled=True),
        lax.all_gather(down_weight, ROWS, axis=1, tiled=True),
    )
    own_rows = lax.axis_index(ROWS) * tokens + jnp.arange(tokens, dtype=jnp.int32)
    own_places = row_places(block_pair, own_rows, block_len)
    cosine_table, sine_table = rope_tables(own_places, HEAD_SIZE)
    x_full = layer_input.astype(wide_float_type)
    x_hat, x_scale = row_norm(x_full)
    attn_scale = full_attn_gain.astype(wide_float_type)
    normalized_input = (x_hat * attn_scale).astype(narrow_float_type)
    q_raw = jnp.dot(normalized_input, full_q, preferred_element_type=wide_float_type).reshape(
        tokens, q_local, HEAD_SIZE
    )
    unnormalized_keys = jnp.dot(
        normalized_input, full_k, preferred_element_type=wide_float_type
    ).reshape(tokens, kv_local, HEAD_SIZE)
    value_rows_backward = jnp.dot(
        normalized_input, full_v, preferred_element_type=wide_float_type
    ).astype(narrow_float_type)
    normalized_queries, q_scale = row_norm(q_raw)
    normalized_keys, key_norm_scale = row_norm(unnormalized_keys)
    query_gain_vector = full_q_gain.astype(wide_float_type)
    key_gain_vector = full_k_gain.astype(wide_float_type)
    rotated_queries = apply_rotary(
        normalized_queries * query_gain_vector, cosine_table, sine_table
    ).astype(narrow_float_type)
    grouped_queries = rotated_queries.reshape(tokens, kv_local, group_size, HEAD_SIZE)
    k_flat = (
        apply_rotary(normalized_keys * key_gain_vector, cosine_table, sine_table)
        .astype(narrow_float_type)
        .reshape(tokens, kv_local * HEAD_SIZE)
    )
    start_state = (
        jnp.full((kv_local, group_size, tokens), NEG, wide_float_type),
        jnp.zeros((kv_local, group_size, tokens), wide_float_type),
        jnp.zeros((kv_local, group_size, tokens, HEAD_SIZE), wide_float_type),
    )
    key_piece = lax.all_gather(k_flat, ROWS, axis=0, tiled=True)
    value_piece = lax.all_gather(value_rows_backward, ROWS, axis=0, tiled=True)
    count = key_piece.shape[0]
    width = math.gcd(count, 512)
    steps_here = count // width
    key_blocks = key_piece.reshape(steps_here, width, kv_local, HEAD_SIZE)
    value_blocks = value_piece.reshape(steps_here, width, kv_local, HEAD_SIZE)
    key_places = row_places(block_pair, jnp.arange(count, dtype=jnp.int32), block_len).reshape(
        steps_here, width
    )

    def online(state, blockset):
        top, total, softmax_numerator = state
        key_tile, value_tile, place_blk = blockset
        score_matrix, allowed = masked_scores(
            grouped_queries, key_tile, own_places, place_blk, softmax_scale
        )
        new_top = jnp.maximum(top, jnp.max(score_matrix, axis=-1))
        shrink = jnp.exp(top - new_top)
        weight_set = jnp.where(allowed, jnp.exp(score_matrix - new_top[..., None]), 0.0)
        total = total * shrink + jnp.sum(weight_set, axis=-1)
        softmax_numerator = softmax_numerator * shrink[..., None] + jnp.einsum(
            "nwqf,fny->nwqy",
            weight_set.astype(narrow_float_type),
            value_tile,
            preferred_element_type=wide_float_type,
        )
        return ((new_top, total, softmax_numerator), None)

    result, _ = lax.scan(online, start_state, (key_blocks, value_blocks, key_places))
    top, total, softmax_numerator = result
    log_total = top + jnp.log(total)
    attention_backward = (
        jnp.transpose(softmax_numerator / total[..., None], (2, 0, 1, 3))
        .reshape(tokens, q_local * HEAD_SIZE)
        .astype(narrow_float_type)
    )
    attn_part = jnp.dot(attention_backward, full_o, preferred_element_type=wide_float_type)
    hidden = x_full + lax.psum(attn_part, HEADS)
    mlp_scale = full_mlp_gain.astype(wide_float_type)
    h_hat, h_scale = row_norm(hidden)
    h_normed = (h_hat * mlp_scale).astype(narrow_float_type)
    gate = jnp.dot(h_normed, full_gate, preferred_element_type=wide_float_type)
    up_val = jnp.dot(h_normed, full_up, preferred_element_type=wide_float_type)
    sigma = jax.nn.sigmoid(gate)
    silu = gate * sigma
    act = (silu * up_val).astype(narrow_float_type)
    mlp_part = jnp.dot(act, full_down, preferred_element_type=wide_float_type)
    block_out = (hidden + lax.psum(mlp_part, HEADS)).astype(narrow_float_type)
    (
        full_attn_gain,
        full_q,
        full_k,
        full_v,
        full_q_gain,
        full_k_gain,
        full_o,
        full_mlp_gain,
        full_gate,
        full_up,
        full_down,
    ) = (
        lax.all_gather(attn_gain, ROWS, axis=0, tiled=True),
        lax.all_gather(q_weight, ROWS, axis=0, tiled=True),
        lax.all_gather(key_projection, ROWS, axis=0, tiled=True),
        lax.all_gather(value_projection, ROWS, axis=0, tiled=True),
        lax.all_gather(q_gain, ROWS, axis=0, tiled=True),
        lax.all_gather(k_gain, ROWS, axis=0, tiled=True),
        lax.all_gather(o_weight, ROWS, axis=1, tiled=True),
        lax.all_gather(mlp_gain, ROWS, axis=0, tiled=True),
        lax.all_gather(gate_weight, ROWS, axis=0, tiled=True),
        lax.all_gather(up_weight, ROWS, axis=0, tiled=True),
        lax.all_gather(down_weight, ROWS, axis=1, tiled=True),
    )
    grad_downw = jnp.einsum("tf,td->fd", act, cotangent, preferred_element_type=wide_float_type)
    grad_act = jnp.einsum("td,fd->tf", cotangent, full_down, preferred_element_type=wide_float_type)
    grad_g = (grad_act * up_val * (sigma * (1.0 + gate * (1.0 - sigma)))).astype(narrow_float_type)
    grad_u = (grad_act * silu).astype(narrow_float_type)
    grad_gatew = jnp.einsum("tc,tf->cf", h_normed, grad_g, preferred_element_type=wide_float_type)
    grad_upw = jnp.einsum("tc,tf->cf", h_normed, grad_u, preferred_element_type=wide_float_type)
    normed_part = jnp.einsum(
        "tf,cf->tc", grad_g, full_gate, preferred_element_type=wide_float_type
    ) + jnp.einsum("tf,cf->tc", grad_u, full_up, preferred_element_type=wide_float_type)
    grad_normed = lax.psum(normed_part, HEADS)
    grad_mlp_gain = jnp.sum(grad_normed * h_hat, axis=0)
    grad_h = cotangent.astype(wide_float_type) + norm_backward(
        grad_normed * mlp_scale, h_hat, h_scale
    )
    grad_hb = grad_h.astype(narrow_float_type)
    grad_ow = jnp.einsum(
        "tq,td->qd", attention_backward, grad_hb, preferred_element_type=wide_float_type
    )
    output_gradient_backward = jnp.einsum(
        "td,qd->tq", grad_hb, full_o, preferred_element_type=wide_float_type
    ).astype(narrow_float_type)
    grouped_output_gradient = output_gradient_backward.reshape(
        tokens, kv_local, group_size, HEAD_SIZE
    )
    delta_rows = jnp.sum(
        grouped_output_gradient.astype(wide_float_type)
        * attention_backward.reshape(tokens, kv_local, group_size, HEAD_SIZE).astype(
            wide_float_type
        ),
        axis=-1,
    )
    delta_rows = jnp.transpose(delta_rows, (1, 2, 0))
    keys_all, values_all = (
        lax.all_gather(k_flat, ROWS, axis=0, tiled=True),
        lax.all_gather(value_rows_backward, ROWS, axis=0, tiled=True),
    )
    width = math.gcd(seq_len, 512)
    steps_all = seq_len // width
    all_places = row_places(block_pair, jnp.arange(seq_len, dtype=jnp.int32), block_len).reshape(
        steps_all, width
    )

    def backward_step(grad_q_acc, blockset):
        key_tile, value_tile, place_blk = blockset
        score_matrix, allowed = masked_scores(
            grouped_queries, key_tile, own_places, place_blk, softmax_scale
        )
        probability_rows = jnp.where(allowed, jnp.exp(score_matrix - log_total[..., None]), 0.0)
        grad_v_blk = jnp.einsum(
            "mojp,jmof->pmf",
            probability_rows.astype(narrow_float_type),
            grouped_output_gradient,
            preferred_element_type=wide_float_type,
        )
        probability_gradient = jnp.einsum(
            "oblh,wbh->blow",
            grouped_output_gradient,
            value_tile,
            preferred_element_type=wide_float_type,
        )
        score_gradient = (probability_rows * (probability_gradient - delta_rows[..., None])).astype(
            narrow_float_type
        )
        grad_q_acc = (
            grad_q_acc
            + jnp.einsum(
                "xwzq,qxp->zxwp", score_gradient, key_tile, preferred_element_type=wide_float_type
            )
            * softmax_scale
        )
        grad_k_blk = (
            jnp.einsum(
                "mojp,jmof->pmf",
                score_gradient,
                grouped_queries,
                preferred_element_type=wide_float_type,
            )
            * softmax_scale
        )
        return (grad_q_acc, (grad_k_blk, grad_v_blk))

    rotated_query_gradient, stacked = lax.scan(
        backward_step,
        jnp.zeros((tokens, kv_local, group_size, HEAD_SIZE), wide_float_type),
        (
            keys_all.reshape(steps_all, width, kv_local, HEAD_SIZE),
            values_all.reshape(steps_all, width, kv_local, HEAD_SIZE),
            all_places,
        ),
    )
    grad_k_all = stacked[0].reshape(seq_len, kv_local * HEAD_SIZE)
    grad_v_all = stacked[1].reshape(seq_len, kv_local * HEAD_SIZE)
    grad_k_own, grad_v_own = (
        lax.psum_scatter(grad_k_all, ROWS, scatter_dimension=0, tiled=True),
        lax.psum_scatter(grad_v_all, ROWS, scatter_dimension=0, tiled=True),
    )
    grad_qg = unrotate(
        rotated_query_gradient.reshape(tokens, q_local, HEAD_SIZE), cosine_table, sine_table
    )
    q_gain_part = jnp.sum(grad_qg * normalized_queries, axis=(0, 1))
    query_gradient = (
        norm_backward(grad_qg * query_gain_vector, normalized_queries, q_scale)
        .reshape(tokens, q_local * HEAD_SIZE)
        .astype(narrow_float_type)
    )
    key_gain_gradient = unrotate(
        grad_k_own.reshape(tokens, kv_local, HEAD_SIZE), cosine_table, sine_table
    )
    k_gain_part = jnp.sum(key_gain_gradient * normalized_keys, axis=(0, 1))
    key_gradient = (
        norm_backward(key_gain_gradient * key_gain_vector, normalized_keys, key_norm_scale)
        .reshape(tokens, kv_local * HEAD_SIZE)
        .astype(narrow_float_type)
    )
    value_gradient_backward = grad_v_own.astype(narrow_float_type)
    grad_qw = jnp.einsum(
        "tc,tq->cq", normalized_input, query_gradient, preferred_element_type=wide_float_type
    )
    grad_kw = jnp.einsum(
        "tc,tq->cq", normalized_input, key_gradient, preferred_element_type=wide_float_type
    )
    grad_vw = jnp.einsum(
        "tc,tq->cq",
        normalized_input,
        value_gradient_backward,
        preferred_element_type=wide_float_type,
    )
    xn_part = (
        jnp.einsum("tq,cq->tc", query_gradient, full_q, preferred_element_type=wide_float_type)
        + jnp.einsum("tq,cq->tc", key_gradient, full_k, preferred_element_type=wide_float_type)
        + jnp.einsum(
            "tq,cq->tc", value_gradient_backward, full_v, preferred_element_type=wide_float_type
        )
    )
    grad_xn, grad_q_gain, grad_k_gain = lax.psum((xn_part, q_gain_part, k_gain_part), HEADS)
    grad_attn_gain = jnp.sum(grad_xn * x_hat, axis=0)
    input_grad = grad_h + norm_backward(grad_xn * attn_scale, x_hat, x_scale)
    owned = (
        lax.psum_scatter(grad_attn_gain, ROWS, scatter_dimension=0, tiled=True),
        lax.psum_scatter(grad_qw, ROWS, scatter_dimension=0, tiled=True),
        lax.psum_scatter(grad_kw, ROWS, scatter_dimension=0, tiled=True),
        lax.psum_scatter(grad_vw, ROWS, scatter_dimension=0, tiled=True),
        lax.psum_scatter(grad_q_gain, ROWS, scatter_dimension=0, tiled=True),
        lax.psum_scatter(grad_k_gain, ROWS, scatter_dimension=0, tiled=True),
        lax.psum_scatter(grad_ow, ROWS, scatter_dimension=1, tiled=True),
        lax.psum_scatter(grad_mlp_gain, ROWS, scatter_dimension=0, tiled=True),
        lax.psum_scatter(grad_gatew, ROWS, scatter_dimension=0, tiled=True),
        lax.psum_scatter(grad_upw, ROWS, scatter_dimension=0, tiled=True),
        lax.psum_scatter(grad_downw, ROWS, scatter_dimension=1, tiled=True),
    )
    return (
        block_out,
        input_grad,
        owned[0],
        owned[1],
        owned[2],
        owned[3],
        owned[4],
        owned[5],
        owned[6],
        owned[7],
        owned[8],
        owned[9],
        owned[10],
    )


MESH = pl.DeviceIdType.MESH
HBM = pl.BlockSpec(memory_space=pltpu.HBM)
VM = pl.BlockSpec(memory_space=pltpu.VMEM)
SLOTS = 256
NT = (((1,), (1,)), ((), ()))
TN = (((0,), (0,)), ((), ()))
BF = jnp.bfloat16
F32 = jnp.float32


class Net:
    def __init__(self, shards, send, recv, loc):
        self.C = shards
        self.send, self.recv, self.loc = send, recv, loc
        self.used = self.used_local = 0
        self.c, f, self.y = (lax.axis_index(a) for a in (CONTEXT, FSDP, HEADS))
        self.x, self.k = f // 2, f % 2

    def at(self, c=None, x=None, k=None, y=None):
        c, x, k, y = (own if v is None else v for v, own in ((c, self.c), (x, self.x), (k, self.k), (y, self.y)))
        return (c, 2 * x + k, y)

    def core(self):
        return self.at(k=1 - self.k)

    def over_x(self):
        return self.at(x=1 - self.x)

    def over_y(self):
        return self.at(y=1 - self.y)

    def shard(self, step):
        return lax.rem(self.c + step + self.C, self.C)

    def slot(self):
        self.used += 1
        return self.used - 1

    def remote(self, src, dst, slot, to):
        return pltpu.make_async_remote_copy(
            src_ref=src, dst_ref=dst, send_sem=self.send.at[slot], recv_sem=self.recv.at[slot],
            device_id=to, device_id_type=MESH,
        )

    def local(self, src, dst):
        self.used_local += 1
        return pltpu.make_async_copy(src, dst, self.loc.at[self.used_local - 1])

    def meet(self, devices):
        barrier = pltpu.get_barrier_semaphore()
        for to in devices:
            pl.semaphore_signal(barrier, inc=1, device_id=to, device_id_type=MESH)
        pl.semaphore_wait(barrier, len(devices))

    def group(self):
        return [
            self.at(c=self.shard(dc), k=(self.k + dk) % 2)
            for dc in range(self.C) for dk in range(2) if (dc, dk) != (0, 0)
        ]


def run(*parts):
    live = list(parts)
    while live:
        live = [p for p in live if next(p, 0) != 0]


def gather_rows(net, src, dst, half):
    C, c, k, y = net.C, net.c, net.k, net.y
    H = dst.shape[-1] // 2
    mine = pl.ds(pl.multiple_of(y * H, 128), H)
    other = pl.ds(pl.multiple_of((1 - y) * H, 128), H)
    own_cols = mine if half else pl.ds(0, 2 * H)
    own_half = src if half else src.at[:, mine]
    right, left = net.at(c=c + 1), net.at(c=c - 1)
    core, over_y = net.core(), net.over_y()
    keep = net.local(src, dst.at[k, c, :, own_cols])
    keep.start()
    hops = [(d, s) for s in range(1, C) for d in (0, 1)]
    zslot = {h: net.slot() for h in hops}
    yslot = {h: net.slot() for h in hops}
    aslot = {h: net.slot() for h in hops}
    bslot = {h: net.slot() for h in hops}
    own_core, own_y, own_core2 = net.slot(), net.slot(), net.slot()
    no_right, no_left = c < C - 1, c > 0

    def chunk(d, s):
        return (c - s, c - s >= 0) if d == 0 else (c + s, c + s < C)

    def z_send(d, s, source, q):
        to = right if d == 0 else left
        return net.remote(source, dst.at[k, q, :, mine], zslot[d, s], to)

    @pl.when(no_right)
    def _():
        z_send(0, 1, own_half, c).start()

    @pl.when(no_left)
    def _():
        z_send(1, 1, own_half, c).start()

    to_core = net.remote(src, dst.at[k, c, :, own_cols], own_core, core)
    to_core.start()
    if half:
        to_y = net.remote(src, dst.at[k, c, :, mine], own_y, over_y)
        to_y.start()
    yield 1
    for d, s in hops:
        q, valid = chunk(d, s)

        @pl.when(valid)
        def _(d=d, s=s, q=q):
            piece = dst.at[k, q, :, mine]
            z_send(d, s, piece, q).wait_recv()
            if s < C - 1:
                @pl.when(no_right if d == 0 else no_left)
                def _():
                    z_send(d, s + 1, piece, q).start()
            net.remote(piece, piece, yslot[d, s], over_y).start()
            net.remote(piece, piece, aslot[d, s], core).start()
        yield 1
    if half:
        piece = dst.at[k, c, :, other]
        net.remote(piece, piece, own_y, over_y).wait_recv()
        net.remote(piece, piece, own_core2, core).start()
    for d, s in hops:
        q, valid = chunk(d, s)

        @pl.when(valid)
        def _(d=d, s=s, q=q):
            piece = dst.at[k, q, :, other]
            net.remote(piece, piece, yslot[d, s], over_y).wait_recv()
            net.remote(piece, piece, bslot[d, s], core).start()
        yield 1
    to_core_in = net.remote(src, dst.at[1 - k, c, :, own_cols], own_core, core)
    to_core_in.wait_recv()
    to_core_in.wait_send()
    if half:
        piece = dst.at[1 - k, c, :, other]
        net.remote(piece, piece, own_core2, core).wait()
        to_y.wait_send()
    for d, s in hops:
        q, valid = chunk(d, s)

        @pl.when(valid)
        def _(d=d, s=s, q=q):
            a, b = dst.at[1 - k, q, :, mine], dst.at[1 - k, q, :, other]
            net.remote(a, a, aslot[d, s], core).wait()
            net.remote(b, b, bslot[d, s], core).wait()
            net.remote(a, a, yslot[d, s], over_y).wait_send()

        sent = jnp.logical_and(no_right if d == 0 else no_left, chunk(d, s - 1)[1])

        @pl.when(sent)
        def _(d=d, s=s):
            piece = dst.at[k, c, :, mine]
            z_send(d, s, piece, c).wait_send()
    keep.wait()
    yield 1


class Hand:
    def __init__(self, net, groups):
        self.net, self.groups = net, groups
        self.steps = [(dc, dk) for dc in range(net.C) for dk in range(2)]
        self.steps = self.steps[1:] + self.steps[:1]
        self.zs = {(g, s): net.slot() for s in self.steps for g in range(len(groups))}
        self.xs = {(g, s): net.slot() for s in self.steps for g in range(len(groups))}
        self.keeps = []
        self.posted = self.relayed = 0

    def post(self, count):
        net = self.net
        mine = net.c * 4 + 2 * net.x + net.k
        for s in self.steps[self.posted:self.posted + count]:
            tc, tk = net.shard(s[0]), (net.k + s[1]) % 2
            for g, (pieces, whole) in enumerate(self.groups):
                for src, pick, put in pieces:
                    if s == (0, 0):
                        net.remote(src.at[pick(tc, tk)], put(mine), self.xs[g, s], net.over_x()).start()
                        keep = net.local(src.at[pick(tc, tk)], put(mine))
                        keep.start()
                        self.keeps.append(keep)
                    else:
                        net.remote(src.at[pick(tc, tk)], put(mine), self.zs[g, s], net.at(c=tc, k=tk)).start()
        self.posted += count

    def block(self, g, s, x):
        net = self.net
        return self.groups[g][1](net.shard(-s[0]) * 4 + 2 * x + (net.k + s[1]) % 2)

    def relay(self, count):
        net = self.net
        for s in self.steps[self.relayed:min(self.relayed + count, len(self.steps) - 1)]:
            for g in range(len(self.groups)):
                block = self.block(g, s, net.x)
                net.remote(block, block, self.zs[g, s], net.over_x()).wait_recv()
                net.remote(block, block, self.xs[g, s], net.over_x()).start()
        self.relayed += count

    def finish(self):
        net = self.net
        for s in self.steps:
            for g in range(len(self.groups)):
                block = self.block(g, s, 1 - net.x)
                net.remote(block, block, self.xs[g, s], net.over_x()).wait()
                if s != (0, 0):
                    net.remote(block, block, self.zs[g, s], net.over_x()).wait_send()
        for keep in self.keeps:
            keep.wait()


def reduce_scratch(C, rows, width, tiles):
    w = width // tiles
    return [
        pltpu.VMEM((tiles // 2, C, rows, w), BF),
        pltpu.VMEM((tiles, C, rows, w), BF),
        pltpu.VMEM((tiles // 2, C, rows, w), BF),
        pltpu.VMEM((tiles // 2, C, rows, w), BF),
        pltpu.VMEM((tiles // 2, C, rows, w), F32),
        pltpu.VMEM((tiles // 2, C - 1, rows, w), BF),
        pltpu.VMEM((tiles // 2, C - 1, rows, w), BF),
    ]


def reduce_rows(net, product, scratch, out):
    osend, orecv, ysend, yrecv, sums, zsend, zrecv = scratch
    tiles, C, rows, w = orecv.shape
    n = tiles // 2
    k, y = net.k, net.y
    core, over_y = net.core(), net.over_y()
    column = [(1 - y) * n + j for j in range(n)] + [y * n + j for j in range(n)]
    copies = []
    for j in range(tiles):
        if j >= n:
            copies[j - n].wait_send()
        osend[j % n] = product(1 - k, column[j]).astype(BF).reshape(C, rows, w)
        cp = net.remote(osend.at[j % n], orecv.at[j], net.slot(), core)
        cp.start()
        copies.append(cp)
        yield 1
    ycopies = []
    for j in range(n):
        own = product(k, column[j]).reshape(C, rows, w)
        copies[j].wait_recv()
        ysend[j] = (own + orecv[j].astype(F32)).astype(BF)
        cp = net.remote(ysend.at[j], yrecv.at[j], net.slot(), over_y)
        cp.start()
        ycopies.append(cp)
        yield 1
    zcopies = []
    for j in range(n):
        own = product(k, column[n + j]).reshape(C, rows, w)
        copies[n + j].wait_recv()
        own = own + orecv[n + j].astype(F32)
        sums[j] = own
        ycopies[j].wait_recv()
        sums[j] = sums[j] + yrecv[j].astype(F32)
        for dc in range(1, C):
            to = net.shard(dc)
            zsend[j, dc - 1] = sums[j, to].astype(BF)
            cp = net.remote(zsend.at[j, dc - 1], zrecv.at[j, dc - 1], net.slot(), net.at(c=to))
            cp.start()
            zcopies.append(cp)
        yield 1
    for j in range(n):
        total = sums[j, net.c]
        for dc in range(1, C):
            zcopies[j * (C - 1) + dc - 1].wait_recv()
            total = total + zrecv[j, dc - 1].astype(F32)
        out[j] = total
        yield 1
    for cp in copies[n:] + ycopies + zcopies:
        cp.wait_send()
    yield 1


def half_of(ref, y, width):
    return ref[:, pl.ds(pl.multiple_of(y * width, 128), width)]


def gain_half(gains, y, row, blocks):
    return [gains[y * blocks + i].astype(F32)[row:row + 1] for i in range(blocks)]


def times_gain(value, rows):
    w = value.shape[1] // len(rows)
    return jnp.concatenate([value[:, i * w:(i + 1) * w] * r for i, r in enumerate(rows)], axis=1)


def swap_sums(net, part, out_buf, in_buf):
    out_buf[...] = jnp.broadcast_to(part, out_buf.shape)
    cp = net.remote(out_buf, in_buf, net.slot(), net.over_y())
    cp.start()
    cp.wait()
    return part + in_buf[:, 0:1]


def rotate(value, cosine, sine):
    return value * cosine + pltpu.roll(value, value.shape[1] // 2, 1) * sine


def steps_of(part, count):
    for _ in range(count):
        if next(part, 0) == 0:
            return


def front_kernel(C, tiles, head, scale, tile, x_ref, g_ref, cot, qp, kp, cosine, sine, wq, wk, wv, wo, wg, wu, wd,
                 xg_out, ghg, wqkv, wod, wdd, gains, raw, q_out, kv, kvp, o_out, lse, act, h_out, gh_out, part_out,
                 g_out, u_out, d_out, zgu, zd,
                 xn, xg, ht, ct, wgu, m_s, l_s, acc, red, rs, hn, gb, s_out, s_in, s_out2, s_in2, ggu, ggu_t, act_t, from_x, to_x,
                 send, recv, loc):
    net = Net(C, send, recv, loc)
    c, x, y, k = net.c, net.x, net.y, net.k
    B, unit = wg.shape[0], wdd.shape[0]
    R, D = x_ref.shape
    H = D // 2
    T = 2 * C * R
    w = D // tiles
    blocks = gains.shape[0]
    plane = [(dc, dx, dk) for dc in range(C) for dx in range(2) for dk in range(2)][1:]
    mates = [net.at(c=net.shard(dc), x=(x + dx) % 2, k=(k + dk) % 2) for dc, dx, dk in plane]
    net.meet(mates + [net.over_y()])
    me = c * 4 + 2 * x + k
    sent = []
    for to in mates:
        cp = net.remote(g_ref, gains.at[me], net.slot(), to)
        cp.start()
        sent.append(cp)
    own = net.local(g_ref, gains.at[me])
    own.start()
    full = slice(None)
    lanes = lambda n, m: pl.ds(pl.multiple_of(n * m, 128), m)
    rows = lambda b: pl.ds(pl.multiple_of(b * B, B), B)
    part = lambda tc, tk, m: pl.ds(pl.multiple_of((2 * tc + tk) * m, 128), m)
    g_qkv = (
        [(wq, lambda tc, tk: (full, part(tc, tk, head)), lambda b: wqkv.at[rows(b), pl.ds(0, head)]),
         (wk, lambda tc, tk: (full, lanes(tc, head)), lambda b: wqkv.at[rows(b), pl.ds(head, head)]),
         (wv, lambda tc, tk: (full, lanes(tc, head)), lambda b: wqkv.at[rows(b), pl.ds(2 * head, head)])],
        lambda b: wqkv.at[rows(b), :])
    g_o = ([(wo, lambda tc, tk: (part(tc, tk, head), full), lambda b: wod.at[:, lanes(b, B)])],
           lambda b: wod.at[:, lanes(b, B)])
    g_gu = (
        [(wg, lambda tc, tk: (full, part(tc, tk, unit)), lambda b: wgu.at[rows(b), pl.ds(0, unit)]),
         (wu, lambda tc, tk: (full, part(tc, tk, unit)), lambda b: wgu.at[rows(b), pl.ds(unit, unit)])],
        lambda b: wgu.at[rows(b), :])
    g_d = ([(wd, lambda tc, tk: (part(tc, tk, unit), full), lambda b: wdd.at[:, lanes(b, B)])],
           lambda b: wdd.at[:, lanes(b, B)])
    h_qkv, h_o, h_mlp = Hand(net, [g_qkv]), Hand(net, [g_o]), Hand(net, [g_gu, g_d])
    every = 2 * C
    h_qkv.post(4)
    own.wait()
    for cp in sent:
        cp.wait()
    value = x_ref[...].astype(F32)
    hat = value * lax.rsqrt(jnp.mean(value * value, axis=-1, keepdims=True) + EPS)
    xn[...] = times_gain(hat, [gains[b].astype(F32)[0:1] for b in range(blocks)]).astype(BF)
    rows_x = gather_rows(net, xn, xg, False)
    next(rows_x)
    h_qkv.post(every - 4)
    for _ in range(C - 1):
        steps_of(rows_x, 2)
        h_qkv.relay(2)
    h_qkv.relay(1)
    run(rows_x)
    h_qkv.finish()
    h_o.post(every)
    h_mlp.post(every - 1)
    keep = net.local(xg, xg_out)
    keep.start()
    per = tile // R
    gain_sum = jnp.sum(gains[...].astype(F32), axis=0)
    qg, kg = gain_sum[2:3], gain_sum[3:4]
    for kk in range(2):
        def project(i, _, kk=kk):
            r = pl.ds(pl.multiple_of(kk * C * R + i * tile, tile), tile)
            v = jnp.dot(xg[kk, pl.ds(i * per, per)].reshape(tile, D), wqkv[...], preferred_element_type=F32)
            raw[r] = v[:, :2 * head]
            cs, sn = cosine[r], sine[r]
            q = v[:, :head]
            q = q * lax.rsqrt(jnp.mean(q * q, axis=-1, keepdims=True) + EPS)
            q_out[r] = rotate(q * qg, cs, sn).astype(BF)
            key = v[:, head:2 * head]
            key = key * lax.rsqrt(jnp.mean(key * key, axis=-1, keepdims=True) + EPS)
            kv[r, 0:head] = rotate(key * kg, cs, sn).astype(BF)
            kv[r, head:2 * head] = v[:, 2 * head:].astype(BF)
            return 0

        lax.fori_loop(0, C * R // tile, project, 0)
    swap = net.remote(kv, kvp, net.slot(), net.over_x())
    swap.start()
    h_mlp.post(1)

    def attend(i, _):
        r = pl.ds(pl.multiple_of(i * tile, tile), tile)
        s = lax.dot_general(q_out[r], kv[:, :head], NT, preferred_element_type=F32) * scale
        s = jnp.where(kp[0:1] <= qp[r, 0:1], s, NEG)
        top = jnp.max(s, axis=-1, keepdims=True)
        e = jnp.exp(s - top)
        m_s[r] = jnp.broadcast_to(top, (tile, 128))
        l_s[r] = jnp.broadcast_to(jnp.sum(e, axis=-1, keepdims=True), (tile, 128))
        acc[r] = jnp.dot(e.astype(BF), kv[:, head:], preferred_element_type=F32)
        return 0

    def attend_more(i, _):
        r = pl.ds(pl.multiple_of(i * tile, tile), tile)
        s = lax.dot_general(q_out[r], kvp[:, :head], NT, preferred_element_type=F32) * scale
        old = m_s[r, 0:1]
        top = jnp.maximum(old, jnp.max(s, axis=-1, keepdims=True))
        e = jnp.exp(s - top)
        shrink = jnp.exp(old - top)
        m_s[r] = jnp.broadcast_to(top, (tile, 128))
        l_s[r] = jnp.broadcast_to(l_s[r, 0:1] * shrink + jnp.sum(e, axis=-1, keepdims=True), (tile, 128))
        acc[r] = acc[r] * shrink + jnp.dot(e.astype(BF), kvp[:, head:], preferred_element_type=F32)
        return 0

    steps = T // tile
    lax.fori_loop(0, steps, attend, 0)
    h_o.relay(every - 1)
    swap.wait()

    @pl.when(x == 1)
    def _():
        lax.fori_loop(0, steps, attend_more, 0)

    o_out[...] = (acc[...] / l_s[...]).astype(BF)
    for i in range(steps):
        r = pl.ds(i * tile, tile)
        lse[:, r] = (m_s[r] + jnp.log(l_s[r])).T[0:8]
    h_o.finish()

    def product(kk, t):
        return jnp.dot(o_out[pl.ds(pl.multiple_of(kk * C * R, C * R), C * R)], wod[:, lanes(t, w)],
                       preferred_element_type=F32)

    reduce = reduce_rows(net, product, red, rs)
    steps_of(reduce, tiles + tiles // 2)
    h_mlp.relay(2)
    for _ in range(tiles // 2):
        steps_of(reduce, 1)
        h_mlp.relay(1)
    cots = gather_rows(net, cot, ct, False)
    next(cots)
    h_mlp.relay(every - 3 - tiles // 2)
    run(reduce)
    half = half_of(x_ref, y, H).astype(F32) + jnp.concatenate([rs[j] for j in range(tiles // 2)], axis=1)
    total = swap_sums(net, jnp.sum(half * half, axis=-1, keepdims=True), s_out, s_in)
    hs = lax.rsqrt(total / D + EPS)
    h_out[...] = half
    hn[...] = times_gain(half * hs, gain_half(gains, y, 1, blocks // 2)).astype(BF)
    rows_h = gather_rows(net, hn, ht, True)
    next(rows_h)
    run(cots, rows_h)
    h_mlp.finish()

    for kk in range(2):
        def swiglu(i, _, kk=kk):
            rr = pl.ds(pl.multiple_of(i * tile, tile), tile)
            r = pl.ds(pl.multiple_of(kk * C * R + i * tile, tile), tile)
            gu = jnp.dot(ht[kk, pl.ds(i * per, per)].reshape(tile, D), wgu[...], preferred_element_type=F32)
            ga = lax.dot_general(ct[kk, pl.ds(i * per, per)].reshape(tile, D), wdd[...], NT,
                                 preferred_element_type=F32)
            gate, up = gu[:, :unit], gu[:, unit:]
            sigma = jax.nn.sigmoid(gate)
            silu = gate * sigma
            a = (silu * up).astype(BF)
            act[kk, rr] = a
            act_t[:, r] = a.T
            gg = (ga * up * (sigma * (1.0 + gate * (1.0 - sigma)))).astype(BF)
            gu = (ga * silu).astype(BF)
            ggu[kk, rr, 0:unit] = gg
            ggu[kk, rr, unit:2 * unit] = gu
            ggu_t[0:unit, r] = gg.T
            ggu_t[unit:2 * unit, r] = gu.T
            return 0

        lax.fori_loop(0, C * R // tile, swiglu, 0)

    def normed(kk, t):
        return lax.dot_general(ggu[kk], wgu[lanes(t, w), :], NT, preferred_element_type=F32)

    pair = 2 * B

    def weight_grads(block, out):
        t = lanes(block, pair)
        out(0, 2 * unit, jnp.dot(ggu_t[...], ht[:, :, :, t].reshape(T, pair), preferred_element_type=F32))
        out(2 * unit, 3 * unit, jnp.dot(act_t[...], ct[:, :, :, t].reshape(T, pair), preferred_element_type=F32))

    swaps = []

    def send_partial(q):
        def out(a, b, v):
            to_x[q, a:b] = v.astype(BF)

        weight_grads(net.shard(q + 1) * 2 + 1 - x, out)
        cp = net.remote(to_x.at[q], from_x.at[q], net.slot(), net.over_x())
        cp.start()
        swaps.append(cp)

    place = lambda a, b, m: pl.ds(pl.multiple_of((2 * a + b) * m, 128), m)

    def add_partial(q):
        dc = (q + 1) % C
        swaps[q].wait_recv()

        def out(a, b, v):
            v = v + from_x[q, a:b].astype(F32)
            for kk in range(2):
                part = v[:, kk * B:(kk + 1) * B]
                dk = lax.rem(kk + k, 2)
                if a:
                    zd[2 * dc + dk] = part.astype(BF)
                else:
                    zgu[2 * dc + dk] = part.T.astype(BF)

        weight_grads(net.shard(dc) * 2 + x, out)

    hand_out = Deal(net, swiglu_groups(g_out, u_out, d_out, zgu, zd, unit))
    reduce = reduce_rows(net, normed, red, rs)
    steps_of(reduce, tiles + tiles // 2)
    for q in range(C):
        send_partial(q)
        steps_of(reduce, tiles // 2 // C)
    add_partial(0)
    hand_out.post(2)
    run(reduce)
    g = jnp.concatenate([rs[j] for j in range(tiles // 2)], axis=1)
    hat = half * hs
    col = jnp.sum(g * hat, axis=0, keepdims=True)
    for i in range(part_out.shape[0]):
        n = part_out.shape[1]
        part_out[i:i + 1] = col[:, i * n:(i + 1) * n]
    m = times_gain(g, gain_half(gains, y, 1, blocks // 2))
    mean = swap_sums(net, jnp.sum(m * hat, axis=-1, keepdims=True), s_out2, s_in2) / D
    gh = half_of(cot, y, H).astype(F32) + hs * (m - hat * mean)
    gh_out[...] = gh
    gb[...] = gh.astype(BF)
    rows_g = gather_rows(net, gb, ghg, True)
    next(rows_g)
    add_partial(1)
    run(rows_g)
    add_partial(2)
    add_partial(3)
    hand_out.finish()
    for cp in swaps:
        cp.wait_send()
    keep.wait()


def swiglu_groups(g_out, u_out, d_out, zgu, zd, unit):
    full = slice(None)
    place = lambda a, b: pl.ds(pl.multiple_of((2 * a + b) * unit, 128), unit)
    return [
        (None, None, None, zgu,
         [((full, pl.ds(0, unit)), lambda a, b: g_out.at[:, place(a, b)]),
          ((full, pl.ds(unit, unit)), lambda a, b: u_out.at[:, place(a, b)])], None, False),
        (None, None, None, zd, [((full, full), lambda a, b: d_out.at[place(a, b), :])], None, False),
    ]


class Deal:
    def __init__(self, net, groups):
        self.net, self.groups = net, groups
        self.order = [(dc, dk) for dc in range(1, net.C) for dk in range(2)] + [(0, 1), (0, 0)]
        self.xs, self.zs = {}, []
        self.added = self.posted = 0

    def start(self):
        net = self.net
        for s in self.order:
            b = net.shard(s[0]) * 4 + 2 * (1 - net.x) + (net.k + s[1]) % 2
            for g, (partial, place, from_x, *_) in enumerate(self.groups):
                cp = net.remote(partial.at[place(b)], from_x.at[2 * s[0] + s[1]], net.slot(), net.over_x())
                cp.start()
                self.xs[g, s] = cp

    def add(self, count):
        net = self.net
        for s in self.order[self.added:self.added + count]:
            i = 2 * s[0] + s[1]
            b = net.shard(s[0]) * 4 + 2 * net.x + (net.k + s[1]) % 2
            for g, (partial, place, from_x, sums, puts, keep, flip) in enumerate(self.groups):
                self.xs[g, s].wait_recv()
                total = partial[place(b)].astype(F32) + from_x[i].astype(F32)
                if flip:
                    total = total.T
                if s == (0, 0) and keep is not None:
                    keep(total)
                else:
                    sums[i] = total.astype(BF)
        self.added += count

    def post(self, count):
        net = self.net
        for s in self.order[self.posted:min(self.posted + count, len(self.order) - 1)]:
            i = 2 * s[0] + s[1]
            to = net.at(c=net.shard(s[0]), k=(net.k + s[1]) % 2)
            for partial, place, from_x, sums, puts, keep, flip in self.groups:
                slot = net.slot()
                for take, put in puts:
                    net.remote(sums.at[(i,) + take], put(net.c, net.k), slot, to).start()
                self.zs.append((sums, i, slot))
        self.posted += count

    def both(self, count):
        for _ in range(count):
            self.add(1)
            self.post(1)

    def finish(self):
        for sums, i, slot in self.zs:
            self.net.remote(sums.at[i], sums.at[i], slot, self.net.over_x()).wait()
        for cp in self.xs.values():
            cp.wait_send()


def back_kernel(C, tiles, head, scale, tile, q_ref, kv, kvp, o_ref, lse, qp, kp, cosine, sine, raw, wqkv, wod, gains,
                x_ref, gh_ref, h_ref, parts, act, wdd, zgu, zd, g_in, u_in, d_in, ghg, xg,
                blk, ig, sums_out, g_out, u_out, d_out, q_out, kv_out, o_out,
                gt, xt, do, delta, dq, own, peer, kvg, cin, xs, xin, gqk, dqk, dow, xq, zq, xo, zo, vec, vin, vx, vz,
                s_out, s_in, red_d, rs_d, red, rs, send, recv, loc):
    net = Net(C, send, recv, loc)
    c, x, y, k = net.c, net.x, net.y, net.k
    T = q_ref.shape[0]
    R, D = x_ref.shape
    H = D // 2
    w = D // tiles
    blocks = gains.shape[0]
    load_g = net.local(ghg, gt)
    load_x = net.local(xg, xt)
    load_g.start()
    load_x.start()
    unit, B = wdd.shape[0], u_out.shape[0]
    place = lambda a, b, m: pl.ds(pl.multiple_of((2 * a + b) * m, 128), m)
    g_out[...], u_out[...], d_out[...] = g_in[...], u_in[...], d_in[...]
    g_out[:, place(c, k, unit)] = zgu[0, :, 0:unit]
    u_out[:, place(c, k, unit)] = zgu[0, :, unit:2 * unit]
    d_out[place(c, k, unit), :] = zd[0]
    net.meet(net.group() + [net.over_x(), net.over_y()])
    full = slice(None)
    lanes = lambda n, m: pl.ds(pl.multiple_of(n * m, 128), m)
    deal_u = Deal(net, swiglu_groups(g_out, u_out, d_out, zgu, zd, unit))
    deal_u.posted = 2
    deal_u.post(2 * C)
    steps = T // tile
    half = T // 2

    def rows_of(i):
        return pl.ds(pl.multiple_of(i * tile, tile), tile)

    load_g.wait()

    def grad_o(i, _):
        r = rows_of(i)
        per = tile // R
        g = lax.dot_general(gt[i // (steps // 2), pl.ds((i % (steps // 2)) * per, per)].reshape(tile, D), wod[...], NT,
                            preferred_element_type=F32).astype(BF)
        do[r] = g
        d = jnp.sum(g.astype(F32) * o_ref[r].astype(F32), axis=-1, keepdims=True)
        delta[:, r] = jnp.broadcast_to(d, (tile, 128)).T[0:8]
        return 0

    lax.fori_loop(0, steps, grad_o, 0)
    dq[...] = jnp.zeros_like(dq)
    own[...] = jnp.zeros_like(own)

    def sweep(keys, grads, masked):
        def step(i, _):
            r = rows_of(i)
            q, g = q_ref[r], do[r]
            s = lax.dot_general(keys[:, :head], q, NT, preferred_element_type=F32) * scale
            p = jnp.exp(s - lse[0:1, r])
            if masked:
                p = jnp.where(kp[:, 0:1] <= qp[0:1, r], p, 0.0)
            grads[1] += jnp.dot(p.astype(BF), g, preferred_element_type=F32)
            dp = lax.dot_general(keys[:, head:], g, NT, preferred_element_type=F32)
            ds = (p * (dp - delta[0:1, r])).astype(BF)
            grads[0] += jnp.dot(ds, q, preferred_element_type=F32)
            dq[r] += lax.dot_general(ds, keys[:, :head], TN, preferred_element_type=F32)
            return 0

        lax.fori_loop(0, steps, step, 0)

    one = net.remote(peer.at[1 - k], cin.at[0], net.slot(), net.core())
    two = net.remote(xs, xin, net.slot(), net.over_x())
    three = net.remote(own.at[1 - k], cin.at[1], net.slot(), net.core())

    @pl.when(x == 1)
    def _():
        peer[...] = jnp.zeros_like(peer)
        sweep(kvp, peer, False)
        one.start()
        one.wait()
        xs[...] = peer[k] + cin[0]
        two.start()

    sweep(kv, own, True)
    three.start()

    def down(kk, t):
        return jnp.dot(act[kk], wdd[:, lanes(t, w)], preferred_element_type=F32)

    reduce_d = reduce_rows(net, down, red_d, rs_d)
    steps_of(reduce_d, tiles + tiles // 2)
    gain_sum = jnp.sum(gains[...].astype(F32), axis=0)
    qg, kg = gain_sum[2:3], gain_sum[3:4]
    n = vec.shape[2]
    count = H // n
    vec[0] = parts[...]

    def back_norm(grad, value, gain, r):
        rotated = grad * cosine[r] - pltpu.roll(grad, head // 2, 1) * sine[r]
        factor = lax.rsqrt(jnp.mean(value * value, axis=-1, keepdims=True) + EPS)
        hat = value * factor
        m = rotated * gain
        result = factor * (m - hat * jnp.mean(m * hat, axis=-1, keepdims=True))
        return result, jnp.sum(rotated * hat, axis=0, keepdims=True)

    def finish_q(i, total):
        r = rows_of(i)
        g, col = back_norm(dq[r] * scale, raw[r, 0:head], qg, r)
        gqk[r, 0:head] = g.astype(BF)
        return total + col

    vec[0, 2 * count:2 * count + 1] = lax.fori_loop(0, steps, finish_q, jnp.zeros((1, head), F32))
    dow[...] = lax.dot_general(o_ref[...], gt[...].reshape(T, D), TN, preferred_element_type=F32).astype(BF)
    three.wait()
    kvg[...] = own[k] + cin[1]

    @pl.when(x == 1)
    def _():
        two.wait_send()

    @pl.when(x == 0)
    def _():
        two.wait_recv()
        kvg[...] = kvg[...] + xin[...]

    def finish_kv(i, total):
        r = rows_of(i)
        v = kvg[r]
        g, col = back_norm(v * scale, raw[r, head:2 * head], kg, r)
        gqk[r, head:2 * head] = jnp.where(k == 0, g, v).astype(BF)
        return total + jnp.where(k == 0, col, 0.0)

    vec[0, 2 * count + 1:2 * count + 2] = lax.fori_loop(0, steps, finish_kv, jnp.zeros((1, head), F32))

    def product(kk, t):
        r = pl.ds(pl.multiple_of(kk * half, half), half)
        a = lax.dot_general(gqk[r, 0:head], wqkv[lanes(t, w), 0:head], NT, preferred_element_type=F32)
        return a + lax.dot_general(gqk[r, head:2 * head], wqkv[lanes(t, w), lanes(1 + k, head)], NT,
                                   preferred_element_type=F32)

    def keep_q(v):
        q_out[:, place(c, k, head)] = v[:, :head].astype(BF)
        kv_out[k, :, lanes(c, head)] = v[:, head:].astype(BF)

    def keep_o(v):
        o_out[place(c, k, head), :] = v.astype(BF)

    deal_q = Deal(net, [
        (dqk, lambda b: (full, lanes(b, B)), xq, zq,
         [((full, pl.ds(0, head)), lambda a, b: q_out.at[:, place(a, b, head)]),
          ((full, pl.ds(head, head)), lambda a, b: kv_out.at[b, :, lanes(a, head)])], keep_q, True),
        (dow, lambda b: (full, lanes(b, B)), xo, zo,
         [((full, full), lambda a, b: o_out.at[place(a, b, head), :])], keep_o, False),
    ])
    reduce = reduce_rows(net, product, red, rs)
    steps_of(reduce, tiles + tiles // 2)
    load_x.wait()
    for i in range(tiles):
        t = pl.ds(i * w, w)
        dqk[:, t] = lax.dot_general(gqk[...], xt[:, :, :, t].reshape(T, w), TN, preferred_element_type=F32).astype(BF)
    deal_q.start()
    steps_of(reduce_d, tiles // 2)
    steps_of(reduce, tiles // 2)
    deal_q.both(2 * C)
    run(reduce_d)
    blk[y] = (h_ref[...] + jnp.concatenate([rs_d[j] for j in range(tiles // 2)], axis=1)).astype(BF)
    swap_b = net.remote(blk.at[y], blk.at[y], net.slot(), net.over_y())
    swap_b.start()
    run(reduce)
    value = x_ref[...].astype(F32)
    xscale = lax.rsqrt(jnp.mean(value * value, axis=-1, keepdims=True) + EPS)
    hat = half_of(x_ref, y, H).astype(F32) * xscale
    g = jnp.concatenate([rs[j] for j in range(tiles // 2)], axis=1)
    col = jnp.sum(g * hat, axis=0, keepdims=True)
    for i in range(count):
        vec[0, i:i + 1] = col[:, i * n:(i + 1) * n]
    first = net.remote(vec.at[0], vin, net.slot(), net.core())
    first.start()
    m = times_gain(g, gain_half(gains, y, 0, blocks // 2))
    mean = swap_sums(net, jnp.sum(m * hat, axis=-1, keepdims=True), s_out, s_in) / D
    ig[y] = (gh_ref[...] + xscale * (m - hat * mean)).astype(BF)
    swap = net.remote(ig.at[y], ig.at[y], net.slot(), net.over_y())
    swap.start()
    first.wait()
    vec[1] = vec[0] + vin[...]
    second = net.remote(vec.at[1], vx, net.slot(), net.over_x())
    second.start()
    second.wait()
    vz[c] = vec[1] + vx[...]
    third = []
    for dc in range(1, C):
        cp = net.remote(vz.at[c], vz.at[c], net.slot(), net.at(c=net.shard(dc)))
        cp.start()
        third.append(cp)
    for cp in third:
        cp.wait()
    total = vz[0]
    for i in range(1, C):
        total = total + vz[i]
    sums_out[y] = total
    last = net.remote(sums_out.at[y], sums_out.at[y], net.slot(), net.over_y())
    last.start()
    deal_u.finish()
    deal_q.finish()
    last.wait()
    swap.wait()
    swap_b.wait()


def call(kernel, name, cid, out_shape, in_specs, out_specs, scratch, *args):
    return pl.pallas_call(
        kernel, name=name, out_shape=out_shape, in_specs=in_specs, out_specs=out_specs,
        scratch_shapes=scratch + [
            pltpu.SemaphoreType.DMA((SLOTS,)), pltpu.SemaphoreType.DMA((SLOTS,)), pltpu.SemaphoreType.DMA((32,)),
        ],
        compiler_params=pltpu.CompilerParams(
            collective_id=cid, has_side_effects=True, vmem_limit_bytes=60 * 1024 * 1024
        ),
    )(*args)


def tensor_parallel(layer_input, block_pair, attn_gain, q_weight, key_projection, value_projection, q_gain, k_gain,
                    o_weight, mlp_gain, gate_weight, up_weight, down_weight, cotangent):
    C = lax.axis_size(CONTEXT)
    R, D = layer_input.shape
    B = q_weight.shape[0]
    NB = 4 * C
    T = 2 * C * R
    H = D // 2
    head = HEAD_SIZE
    unit = gate_weight.shape[1] // (2 * C)
    scale = 1.0 / math.sqrt(head)
    half = head // 2
    S = jax.ShapeDtypeStruct
    k = lax.axis_index(FSDP) % 2
    x = lax.axis_index(FSDP) // 2
    TILES = 8

    red = lambda: reduce_scratch(C, R, D, TILES)
    rs = lambda: pltpu.VMEM((TILES // 2, R, D // TILES), F32)
    stat = lambda: pltpu.VMEM((R, 128), F32)
    mine = lax.axis_index(CONTEXT) * 4 + lax.axis_index(FSDP)
    spread = lambda v: lax.dynamic_update_slice_in_dim(jnp.zeros((head,), BF), v, mine * v.shape[0], 0)
    packed = jnp.pad(jnp.stack([attn_gain, mlp_gain, spread(q_gain), spread(k_gain)]), ((0, 12), (0, 0)))
    order = jnp.arange(T, dtype=jnp.int32)
    ids = (order // R % C) * (4 * R) + x * (2 * R) + (order // (C * R)) * R + order % R
    places = row_places(block_pair, ids, 2 * R)
    cosine, sine = (t[:, 0, :] for t in rope_tables(places, head))
    cosine = jnp.concatenate([cosine, cosine], axis=1)
    sine = jnp.concatenate([-sine, sine], axis=1)
    p_col = jnp.broadcast_to(places[:, None], (T, 128))
    p_row = jnp.broadcast_to(places[None, :], (8, T))
    vm = lambda *shape: pltpu.VMEM(shape, BF)
    (xg, ghg, wqkv, wo, wd, gains, raw, q_rot, kv, kvp, attn_o, lse, act, h_half, gh_half, mlp_part, g_in, u_in, d_in,
     zgu, zd) = call(
        lambda *r: front_kernel(C, TILES, head, scale, 256, *r[:43], r[43:50], *r[50:]), "front", 1,
        (S((2, C, R, D), BF), S((2, C, R, D), BF), S((D, 3 * head), BF), S((head, D), BF), S((unit, D), BF),
         S((NB, 16, B), BF), S((T, 2 * head), F32), S((T, head), BF), S((T, 2 * head), BF), S((T, 2 * head), BF),
         S((T, head), BF), S((8, T), F32), S((2, C * R, unit), BF), S((R, H), F32), S((R, H), F32),
         S((H // 128, 128), F32), S((B, 2 * C * unit), BF), S((B, 2 * C * unit), BF), S((2 * C * unit, B), BF),
         S((2 * C, B, 2 * unit), BF), S((2 * C, unit, B), BF)),
        [VM] * 7 + [HBM] * 7, (HBM,) * 2 + (VM,) * 19,
        [vm(R, D), vm(2, C, R, D), vm(2, C, R, D), vm(2, C, R, D), vm(D, 2 * unit), pltpu.VMEM((T, 128), F32),
         pltpu.VMEM((T, 128), F32), pltpu.VMEM((T, head), F32)] + red()
        + [rs(), vm(R, H), vm(R, H), stat(), stat(), stat(), stat(), vm(2, C * R, 2 * unit), vm(2 * unit, T),
           vm(unit, T), vm(C, 3 * unit, 2 * B), vm(C, 3 * unit, 2 * B)],
        layer_input, packed, cotangent, p_col, p_row, cosine, sine,
        q_weight, key_projection, value_projection, o_weight, gate_weight, up_weight, down_weight,
    )
    n_rows = H // 128
    parts = jnp.concatenate([jnp.zeros_like(mlp_part), mlp_part, jnp.zeros((8, 128), F32)], axis=0)
    V = parts.shape
    wide = lambda: pltpu.VMEM((2, T, head), F32)
    one = lambda: pltpu.VMEM((T, head), F32)
    blk, ig, sums, g_w, u_w, d_w, q_w, kv_w, o_w = call(
        lambda *r: back_kernel(C, TILES, head, scale, 256, *r[:59], r[59:66], r[66], r[67:74], *r[74:]), "back", 3,
        (S((2, R, H), BF), S((2, R, H), BF), S((2,) + V, F32), S((B, 2 * C * unit), BF), S((B, 2 * C * unit), BF),
         S((2 * C * unit, B), BF), S((B, 2 * C * head), BF), S((2, B, C * head), BF), S((2 * C * head, B), BF)),
        [VM] * 24 + [HBM] * 2, (VM,) * 9,
        [pltpu.VMEM((2, C, R, D), BF), pltpu.VMEM((2, C, R, D), BF), pltpu.VMEM((T, head), BF), pltpu.VMEM((8, T), F32),
         one(), wide(), wide(), one(), wide(), one(), one(), pltpu.VMEM((T, 2 * head), BF),
         pltpu.VMEM((2 * head, D), BF), pltpu.VMEM((head, D), BF), pltpu.VMEM((2 * C, 2 * head, B), BF),
         pltpu.VMEM((2 * C, B, 2 * head), BF), pltpu.VMEM((2 * C, head, B), BF), pltpu.VMEM((2 * C, head, B), BF),
         pltpu.VMEM((2,) + V, F32), pltpu.VMEM(V, F32), pltpu.VMEM(V, F32), pltpu.VMEM((C,) + V, F32), stat(), stat()]
        + red() + [rs()] + red() + [rs()],
        q_rot, kv, kvp, attn_o, lse, p_row, p_col, cosine, sine, raw, wqkv, wo, gains, layer_input, gh_half, h_half,
        parts, act, wd, zgu, zd, g_in, u_in, d_in, ghg, xg,
    )
    join = lambda v: jnp.concatenate([v[0], v[1]], axis=1)
    both = sums[:, :n_rows].reshape(2 * n_rows, 128)
    both_mlp = sums[:, n_rows:2 * n_rows].reshape(2 * n_rows, 128)
    pick = lambda v: lax.dynamic_slice_in_dim(v.reshape(-1), mine * B, B)
    few = q_gain.shape[0]
    pick_few = lambda v: lax.dynamic_slice_in_dim(v, mine * few, few)
    head_sums = sums[0, 2 * n_rows:] + sums[1, 2 * n_rows:]
    return (
        join(blk), join(ig).astype(F32), pick(both), q_w.astype(F32), kv_w[0].astype(F32), kv_w[1].astype(F32),
        pick_few(head_sums[0]), pick_few(head_sums[1]), o_w.astype(F32), pick(both_mlp), g_w.astype(F32),
        u_w.astype(F32), d_w.astype(F32),
    )


def fits(mesh_shape, layer_input, q_weight, key_projection, gate_weight):
    C = mesh_shape[CONTEXT]
    return (
        mesh_shape[FSDP] == 4 and mesh_shape[HEADS] == 2
        and key_projection.shape[1] == C * HEAD_SIZE and q_weight.shape[1] == 2 * C * HEAD_SIZE
        and gate_weight.shape[1] % (2 * C * 128) == 0 and q_weight.shape[0] == 128
        and layer_input.shape[0] % 128 == 0 and layer_input.shape[1] % (8 * 128) == 0
    )


def solution(mesh):
    def program(*args):
        layer_input, q_weight, key_projection, gate_weight = args[0], args[3], args[4], args[10]
        if fits(dict(mesh.shape), layer_input, q_weight, key_projection, gate_weight):
            return tensor_parallel(*args)
        return per_device(*args)

    return jax.shard_map(
        program,
        mesh=mesh,
        in_specs=(
            P(ROWS, None),
            P(),
            P(ROWS),
            P(ROWS, HEADS),
            P(ROWS, HEADS),
            P(ROWS, HEADS),
            P(ROWS),
            P(ROWS),
            P(HEADS, ROWS),
            P(ROWS),
            P(ROWS, HEADS),
            P(ROWS, HEADS),
            P(HEADS, ROWS),
            P(ROWS, None),
        ),
        out_specs=(
            P(ROWS, None),
            P(ROWS, None),
            P(ROWS),
            P(ROWS, HEADS),
            P(ROWS, HEADS),
            P(ROWS, HEADS),
            P(ROWS),
            P(ROWS),
            P(HEADS, ROWS),
            P(ROWS),
            P(ROWS, HEADS),
            P(ROWS, HEADS),
            P(HEADS, ROWS),
        ),
        check_vma=False,
    )
```

```python
import functools
import math

import jax
import jax.numpy as jnp
import numpy as np
from jax import lax
from jax.experimental import pallas as pl
from jax.experimental.pallas import tpu as pltpu
from jax.sharding import PartitionSpec as P

HEAD_SIZE = 128
CONTEXT, FSDP, HEADS = "context", "fsdp", "heads"
ROWS = (CONTEXT, FSDP)


EPS = 1e-06
THETA = 1000000.0
NEG = -1e30


def row_places(block_pair, row_ids, block_len):
    owners = block_pair.shape[0]
    holder = row_ids // (2 * block_len)
    within = row_ids % (2 * block_len)
    match = holder[:, None] == jnp.arange(owners, dtype=jnp.int32)[None, :]
    paired = jnp.sum(jnp.where(match, block_pair[None, :], 0), axis=1)
    which = jnp.where(within >= block_len, 2 * owners - 1 - paired, paired)
    return which * block_len + within % block_len


def rope_tables(places, head_dim):
    half = head_dim // 2
    freq = jnp.exp(jnp.arange(half, dtype=jnp.float32) * (-2.0 * math.log(THETA) / head_dim))
    angle = places.astype(jnp.float32)[:, None] * freq[None, :]
    return (jnp.cos(angle)[:, None, :], jnp.sin(angle)[:, None, :])


def apply_rotary(field, cosine_table, sine_table):
    half = field.shape[-1] // 2
    first = field[..., :half]
    second = field[..., half:]
    return jnp.concatenate(
        [first * cosine_table - second * sine_table, second * cosine_table + first * sine_table],
        axis=-1,
    )


def unrotate(grad, cosine_table, sine_table):
    half = grad.shape[-1] // 2
    first = grad[..., :half]
    second = grad[..., half:]
    return jnp.concatenate(
        [first * cosine_table + second * sine_table, second * cosine_table - first * sine_table],
        axis=-1,
    )


def row_norm(field):
    factor = lax.rsqrt(jnp.mean(field * field, axis=-1, keepdims=True) + EPS)
    return (field * factor, factor)


def norm_backward(grad_hat, normed, factor):
    return factor * (grad_hat - normed * jnp.mean(grad_hat * normed, axis=-1, keepdims=True))


def masked_scores(query_matrix, key_rows, query_places, key_places, softmax_scale):
    score_matrix = (
        jnp.einsum("oblh,wbh->blow", query_matrix, key_rows, preferred_element_type=jnp.float32)
        * softmax_scale
    )
    allowed = key_places[None, :] <= query_places[:, None]
    return (jnp.where(allowed, score_matrix, NEG), allowed)


def per_device(
    layer_input,
    block_pair,
    attn_gain,
    q_weight,
    key_projection,
    value_projection,
    q_gain,
    k_gain,
    o_weight,
    mlp_gain,
    gate_weight,
    up_weight,
    down_weight,
    cotangent,
):
    wide_float_type = jnp.float32
    narrow_float_type = jnp.bfloat16
    tokens = layer_input.shape[0]
    members = lax.axis_size(ROWS)
    seq_len = tokens * members
    block_len = tokens * lax.axis_size(FSDP) // 2
    kv_local = key_projection.shape[1] // HEAD_SIZE
    q_local = q_weight.shape[1] // HEAD_SIZE
    group_size = q_local // kv_local
    softmax_scale = 1.0 / math.sqrt(HEAD_SIZE)
    (
        full_attn_gain,
        full_q,
        full_k,
        full_v,
        full_q_gain,
        full_k_gain,
        full_o,
        full_mlp_gain,
        full_gate,
        full_up,
        full_down,
    ) = (
        lax.all_gather(attn_gain, ROWS, axis=0, tiled=True),
        lax.all_gather(q_weight, ROWS, axis=0, tiled=True),
        lax.all_gather(key_projection, ROWS, axis=0, tiled=True),
        lax.all_gather(value_projection, ROWS, axis=0, tiled=True),
        lax.all_gather(q_gain, ROWS, axis=0, tiled=True),
        lax.all_gather(k_gain, ROWS, axis=0, tiled=True),
        lax.all_gather(o_weight, ROWS, axis=1, tiled=True),
        lax.all_gather(mlp_gain, ROWS, axis=0, tiled=True),
        lax.all_gather(gate_weight, ROWS, axis=0, tiled=True),
        lax.all_gather(up_weight, ROWS, axis=0, tiled=True),
        lax.all_gather(down_weight, ROWS, axis=1, tiled=True),
    )
    own_rows = lax.axis_index(ROWS) * tokens + jnp.arange(tokens, dtype=jnp.int32)
    own_places = row_places(block_pair, own_rows, block_len)
    cosine_table, sine_table = rope_tables(own_places, HEAD_SIZE)
    x_full = layer_input.astype(wide_float_type)
    x_hat, x_scale = row_norm(x_full)
    attn_scale = full_attn_gain.astype(wide_float_type)
    normalized_input = (x_hat * attn_scale).astype(narrow_float_type)
    q_raw = jnp.dot(normalized_input, full_q, preferred_element_type=wide_float_type).reshape(
        tokens, q_local, HEAD_SIZE
    )
    unnormalized_keys = jnp.dot(
        normalized_input, full_k, preferred_element_type=wide_float_type
    ).reshape(tokens, kv_local, HEAD_SIZE)
    value_rows_backward = jnp.dot(
        normalized_input, full_v, preferred_element_type=wide_float_type
    ).astype(narrow_float_type)
    normalized_queries, q_scale = row_norm(q_raw)
    normalized_keys, key_norm_scale = row_norm(unnormalized_keys)
    query_gain_vector = full_q_gain.astype(wide_float_type)
    key_gain_vector = full_k_gain.astype(wide_float_type)
    rotated_queries = apply_rotary(
        normalized_queries * query_gain_vector, cosine_table, sine_table
    ).astype(narrow_float_type)
    grouped_queries = rotated_queries.reshape(tokens, kv_local, group_size, HEAD_SIZE)
    k_flat = (
        apply_rotary(normalized_keys * key_gain_vector, cosine_table, sine_table)
        .astype(narrow_float_type)
        .reshape(tokens, kv_local * HEAD_SIZE)
    )
    start_state = (
        jnp.full((kv_local, group_size, tokens), NEG, wide_float_type),
        jnp.zeros((kv_local, group_size, tokens), wide_float_type),
        jnp.zeros((kv_local, group_size, tokens, HEAD_SIZE), wide_float_type),
    )
    key_piece = lax.all_gather(k_flat, ROWS, axis=0, tiled=True)
    value_piece = lax.all_gather(value_rows_backward, ROWS, axis=0, tiled=True)
    count = key_piece.shape[0]
    width = math.gcd(count, 512)
    steps_here = count // width
    key_blocks = key_piece.reshape(steps_here, width, kv_local, HEAD_SIZE)
    value_blocks = value_piece.reshape(steps_here, width, kv_local, HEAD_SIZE)
    key_places = row_places(block_pair, jnp.arange(count, dtype=jnp.int32), block_len).reshape(
        steps_here, width
    )

    def online(state, blockset):
        top, total, softmax_numerator = state
        key_tile, value_tile, place_blk = blockset
        score_matrix, allowed = masked_scores(
            grouped_queries, key_tile, own_places, place_blk, softmax_scale
        )
        new_top = jnp.maximum(top, jnp.max(score_matrix, axis=-1))
        shrink = jnp.exp(top - new_top)
        weight_set = jnp.where(allowed, jnp.exp(score_matrix - new_top[..., None]), 0.0)
        total = total * shrink + jnp.sum(weight_set, axis=-1)
        softmax_numerator = softmax_numerator * shrink[..., None] + jnp.einsum(
            "nwqf,fny->nwqy",
            weight_set.astype(narrow_float_type),
            value_tile,
            preferred_element_type=wide_float_type,
        )
        return ((new_top, total, softmax_numerator), None)

    result, _ = lax.scan(online, start_state, (key_blocks, value_blocks, key_places))
    top, total, softmax_numerator = result
    log_total = top + jnp.log(total)
    attention_backward = (
        jnp.transpose(softmax_numerator / total[..., None], (2, 0, 1, 3))
        .reshape(tokens, q_local * HEAD_SIZE)
        .astype(narrow_float_type)
    )
    attn_part = jnp.dot(attention_backward, full_o, preferred_element_type=wide_float_type)
    hidden = x_full + lax.psum(attn_part, HEADS)
    mlp_scale = full_mlp_gain.astype(wide_float_type)
    h_hat, h_scale = row_norm(hidden)
    h_normed = (h_hat * mlp_scale).astype(narrow_float_type)
    gate = jnp.dot(h_normed, full_gate, preferred_element_type=wide_float_type)
    up_val = jnp.dot(h_normed, full_up, preferred_element_type=wide_float_type)
    sigma = jax.nn.sigmoid(gate)
    silu = gate * sigma
    act = (silu * up_val).astype(narrow_float_type)
    mlp_part = jnp.dot(act, full_down, preferred_element_type=wide_float_type)
    block_out = (hidden + lax.psum(mlp_part, HEADS)).astype(narrow_float_type)
    (
        full_attn_gain,
        full_q,
        full_k,
        full_v,
        full_q_gain,
        full_k_gain,
        full_o,
        full_mlp_gain,
        full_gate,
        full_up,
        full_down,
    ) = (
        lax.all_gather(attn_gain, ROWS, axis=0, tiled=True),
        lax.all_gather(q_weight, ROWS, axis=0, tiled=True),
        lax.all_gather(key_projection, ROWS, axis=0, tiled=True),
        lax.all_gather(value_projection, ROWS, axis=0, tiled=True),
        lax.all_gather(q_gain, ROWS, axis=0, tiled=True),
        lax.all_gather(k_gain, ROWS, axis=0, tiled=True),
        lax.all_gather(o_weight, ROWS, axis=1, tiled=True),
        lax.all_gather(mlp_gain, ROWS, axis=0, tiled=True),
        lax.all_gather(gate_weight, ROWS, axis=0, tiled=True),
        lax.all_gather(up_weight, ROWS, axis=0, tiled=True),
        lax.all_gather(down_weight, ROWS, axis=1, tiled=True),
    )
    grad_downw = jnp.einsum("tf,td->fd", act, cotangent, preferred_element_type=wide_float_type)
    grad_act = jnp.einsum("td,fd->tf", cotangent, full_down, preferred_element_type=wide_float_type)
    grad_g = (grad_act * up_val * (sigma * (1.0 + gate * (1.0 - sigma)))).astype(narrow_float_type)
    grad_u = (grad_act * silu).astype(narrow_float_type)
    grad_gatew = jnp.einsum("tc,tf->cf", h_normed, grad_g, preferred_element_type=wide_float_type)
    grad_upw = jnp.einsum("tc,tf->cf", h_normed, grad_u, preferred_element_type=wide_float_type)
    normed_part = jnp.einsum(
        "tf,cf->tc", grad_g, full_gate, preferred_element_type=wide_float_type
    ) + jnp.einsum("tf,cf->tc", grad_u, full_up, preferred_element_type=wide_float_type)
    grad_normed = lax.psum(normed_part, HEADS)
    grad_mlp_gain = jnp.sum(grad_normed * h_hat, axis=0)
    grad_h = cotangent.astype(wide_float_type) + norm_backward(
        grad_normed * mlp_scale, h_hat, h_scale
    )
    grad_hb = grad_h.astype(narrow_float_type)
    grad_ow = jnp.einsum(
        "tq,td->qd", attention_backward, grad_hb, preferred_element_type=wide_float_type
    )
    output_gradient_backward = jnp.einsum(
        "td,qd->tq", grad_hb, full_o, preferred_element_type=wide_float_type
    ).astype(narrow_float_type)
    grouped_output_gradient = output_gradient_backward.reshape(
        tokens, kv_local, group_size, HEAD_SIZE
    )
    delta_rows = jnp.sum(
        grouped_output_gradient.astype(wide_float_type)
        * attention_backward.reshape(tokens, kv_local, group_size, HEAD_SIZE).astype(
            wide_float_type
        ),
        axis=-1,
    )
    delta_rows = jnp.transpose(delta_rows, (1, 2, 0))
    keys_all, values_all = (
        lax.all_gather(k_flat, ROWS, axis=0, tiled=True),
        lax.all_gather(value_rows_backward, ROWS, axis=0, tiled=True),
    )
    width = math.gcd(seq_len, 512)
    steps_all = seq_len // width
    all_places = row_places(block_pair, jnp.arange(seq_len, dtype=jnp.int32), block_len).reshape(
        steps_all, width
    )

    def backward_step(grad_q_acc, blockset):
        key_tile, value_tile, place_blk = blockset
        score_matrix, allowed = masked_scores(
            grouped_queries, key_tile, own_places, place_blk, softmax_scale
        )
        probability_rows = jnp.where(allowed, jnp.exp(score_matrix - log_total[..., None]), 0.0)
        grad_v_blk = jnp.einsum(
            "mojp,jmof->pmf",
            probability_rows.astype(narrow_float_type),
            grouped_output_gradient,
            preferred_element_type=wide_float_type,
        )
        probability_gradient = jnp.einsum(
            "oblh,wbh->blow",
            grouped_output_gradient,
            value_tile,
            preferred_element_type=wide_float_type,
        )
        score_gradient = (probability_rows * (probability_gradient - delta_rows[..., None])).astype(
            narrow_float_type
        )
        grad_q_acc = (
            grad_q_acc
            + jnp.einsum(
                "xwzq,qxp->zxwp", score_gradient, key_tile, preferred_element_type=wide_float_type
            )
            * softmax_scale
        )
        grad_k_blk = (
            jnp.einsum(
                "mojp,jmof->pmf",
                score_gradient,
                grouped_queries,
                preferred_element_type=wide_float_type,
            )
            * softmax_scale
        )
        return (grad_q_acc, (grad_k_blk, grad_v_blk))

    rotated_query_gradient, stacked = lax.scan(
        backward_step,
        jnp.zeros((tokens, kv_local, group_size, HEAD_SIZE), wide_float_type),
        (
            keys_all.reshape(steps_all, width, kv_local, HEAD_SIZE),
            values_all.reshape(steps_all, width, kv_local, HEAD_SIZE),
            all_places,
        ),
    )
    grad_k_all = stacked[0].reshape(seq_len, kv_local * HEAD_SIZE)
    grad_v_all = stacked[1].reshape(seq_len, kv_local * HEAD_SIZE)
    grad_k_own, grad_v_own = (
        lax.psum_scatter(grad_k_all, ROWS, scatter_dimension=0, tiled=True),
        lax.psum_scatter(grad_v_all, ROWS, scatter_dimension=0, tiled=True),
    )
    grad_qg = unrotate(
        rotated_query_gradient.reshape(tokens, q_local, HEAD_SIZE), cosine_table, sine_table
    )
    q_gain_part = jnp.sum(grad_qg * normalized_queries, axis=(0, 1))
    query_gradient = (
        norm_backward(grad_qg * query_gain_vector, normalized_queries, q_scale)
        .reshape(tokens, q_local * HEAD_SIZE)
        .astype(narrow_float_type)
    )
    key_gain_gradient = unrotate(
        grad_k_own.reshape(tokens, kv_local, HEAD_SIZE), cosine_table, sine_table
    )
    k_gain_part = jnp.sum(key_gain_gradient * normalized_keys, axis=(0, 1))
    key_gradient = (
        norm_backward(key_gain_gradient * key_gain_vector, normalized_keys, key_norm_scale)
        .reshape(tokens, kv_local * HEAD_SIZE)
        .astype(narrow_float_type)
    )
    value_gradient_backward = grad_v_own.astype(narrow_float_type)
    grad_qw = jnp.einsum(
        "tc,tq->cq", normalized_input, query_gradient, preferred_element_type=wide_float_type
    )
    grad_kw = jnp.einsum(
        "tc,tq->cq", normalized_input, key_gradient, preferred_element_type=wide_float_type
    )
    grad_vw = jnp.einsum(
        "tc,tq->cq",
        normalized_input,
        value_gradient_backward,
        preferred_element_type=wide_float_type,
    )
    xn_part = (
        jnp.einsum("tq,cq->tc", query_gradient, full_q, preferred_element_type=wide_float_type)
        + jnp.einsum("tq,cq->tc", key_gradient, full_k, preferred_element_type=wide_float_type)
        + jnp.einsum(
            "tq,cq->tc", value_gradient_backward, full_v, preferred_element_type=wide_float_type
        )
    )
    grad_xn, grad_q_gain, grad_k_gain = lax.psum((xn_part, q_gain_part, k_gain_part), HEADS)
    grad_attn_gain = jnp.sum(grad_xn * x_hat, axis=0)
    input_grad = grad_h + norm_backward(grad_xn * attn_scale, x_hat, x_scale)
    owned = (
        lax.psum_scatter(grad_attn_gain, ROWS, scatter_dimension=0, tiled=True),
        lax.psum_scatter(grad_qw, ROWS, scatter_dimension=0, tiled=True),
        lax.psum_scatter(grad_kw, ROWS, scatter_dimension=0, tiled=True),
        lax.psum_scatter(grad_vw, ROWS, scatter_dimension=0, tiled=True),
        lax.psum_scatter(grad_q_gain, ROWS, scatter_dimension=0, tiled=True),
        lax.psum_scatter(grad_k_gain, ROWS, scatter_dimension=0, tiled=True),
        lax.psum_scatter(grad_ow, ROWS, scatter_dimension=1, tiled=True),
        lax.psum_scatter(grad_mlp_gain, ROWS, scatter_dimension=0, tiled=True),
        lax.psum_scatter(grad_gatew, ROWS, scatter_dimension=0, tiled=True),
        lax.psum_scatter(grad_upw, ROWS, scatter_dimension=0, tiled=True),
        lax.psum_scatter(grad_downw, ROWS, scatter_dimension=1, tiled=True),
    )
    return (
        block_out,
        input_grad,
        owned[0],
        owned[1],
        owned[2],
        owned[3],
        owned[4],
        owned[5],
        owned[6],
        owned[7],
        owned[8],
        owned[9],
        owned[10],
    )


MESH = pl.DeviceIdType.MESH
HBM = pl.BlockSpec(memory_space=pltpu.HBM)
VM = pl.BlockSpec(memory_space=pltpu.VMEM)
SLOTS = 368
LOCAL_SLOTS = 18
NT = (((1,), (1,)), ((), ()))
TN = (((0,), (0,)), ((), ()))
BF = jnp.bfloat16
F32 = jnp.float32


class Net:
    def __init__(self, shards, send, recv, loc):
        self.C = shards
        self.send, self.recv, self.loc = send, recv, loc
        self.used = self.used_local = 0
        self.c, f, self.y = (lax.axis_index(a) for a in (CONTEXT, FSDP, HEADS))
        self.x, self.k = f // 2, f % 2

    def at(self, c=None, x=None, k=None, y=None):
        c, x, k, y = (own if v is None else v for v, own in ((c, self.c), (x, self.x), (k, self.k), (y, self.y)))
        return (c, 2 * x + k, y)

    def core(self):
        return self.at(k=1 - self.k)

    def over_x(self):
        return self.at(x=1 - self.x)

    def over_y(self):
        return self.at(y=1 - self.y)

    def shard(self, step):
        return lax.rem(self.c + step + self.C, self.C)

    def slots(self, count):
        self.used += count
        assert self.used <= SLOTS
        return self.used - count

    def slot(self):
        return self.slots(1)

    def remote(self, src, dst, slot, to):
        return pltpu.make_async_remote_copy(
            src_ref=src, dst_ref=dst, send_sem=self.send.at[slot], recv_sem=self.recv.at[slot],
            device_id=to, device_id_type=MESH,
        )

    def local(self, src, dst):
        self.used_local += 1
        assert self.used_local <= LOCAL_SLOTS
        return pltpu.make_async_copy(src, dst, self.loc.at[self.used_local - 1])

    def meet(self, devices):
        barrier = pltpu.get_barrier_semaphore()
        for to in devices:
            pl.semaphore_signal(barrier, inc=1, device_id=to, device_id_type=MESH)
        pl.semaphore_wait(barrier, len(devices))

    def group(self):
        return [
            self.at(c=self.shard(dc), k=(self.k + dk) % 2)
            for dc in range(self.C) for dk in range(2) if (dc, dk) != (0, 0)
        ]


def run(*parts):
    live = list(parts)
    while live:
        live = [p for p in live if next(p, 0) != 0]


def gather_rows(net, src, dst, half, done=None):
    C, c, k, y = net.C, net.c, net.k, net.y
    H = dst.shape[-1] // 2
    mine = pl.ds(pl.multiple_of(y * H, 128), H)
    other = pl.ds(pl.multiple_of((1 - y) * H, 128), H)
    own_cols = mine if half else pl.ds(0, 2 * H)
    own_half = src if half else src.at[:, mine]
    right, left = net.at(c=c + 1), net.at(c=c - 1)
    core, over_y = net.core(), net.over_y()
    keep = net.local(src, dst.at[k, c, :, own_cols])
    keep.start()
    done = done or (lambda kk, q: None)
    hops = [(d, s) for s in range(1, C) for d in (0, 1)]
    zslot = {h: net.slot() for h in hops}
    yslot = {h: net.slot() for h in hops}
    aslot = {h: net.slot() for h in hops}
    bslot = {h: net.slot() for h in hops}
    own_core, own_y, own_core2 = net.slot(), net.slot(), net.slot()
    no_right, no_left = c < C - 1, c > 0

    def chunk(d, s):
        return (c - s, c - s >= 0) if d == 0 else (c + s, c + s < C)

    def z_send(d, s, source, q):
        to = right if d == 0 else left
        return net.remote(source, dst.at[k, q, :, mine], zslot[d, s], to)

    @pl.when(no_right)
    def _():
        z_send(0, 1, own_half, c).start()

    @pl.when(no_left)
    def _():
        z_send(1, 1, own_half, c).start()

    to_core = net.remote(src, dst.at[k, c, :, own_cols], own_core, core)
    to_core.start()
    if half:
        to_y = net.remote(src, dst.at[k, c, :, mine], own_y, over_y)
        to_y.start()
    yield 1
    for d, s in hops:
        q, valid = chunk(d, s)

        @pl.when(valid)
        def _(d=d, s=s, q=q):
            piece = dst.at[k, q, :, mine]
            z_send(d, s, piece, q).wait_recv()
            if s < C - 1:
                @pl.when(no_right if d == 0 else no_left)
                def _():
                    z_send(d, s + 1, piece, q).start()
            net.remote(piece, piece, yslot[d, s], over_y).start()
            net.remote(piece, piece, aslot[d, s], core).start()
        yield 1
    if half:
        piece = dst.at[k, c, :, other]
        net.remote(piece, piece, own_y, over_y).wait_recv()
        net.remote(piece, piece, own_core2, core).start()
    for d, s in hops:
        q, valid = chunk(d, s)

        @pl.when(valid)
        def _(d=d, s=s, q=q):
            piece = dst.at[k, q, :, other]
            net.remote(piece, piece, yslot[d, s], over_y).wait_recv()
            net.remote(piece, piece, bslot[d, s], core).start()
            done(k, q)
        yield 1
    keep.wait()
    done(k, c)
    to_core_in = net.remote(src, dst.at[1 - k, c, :, own_cols], own_core, core)
    to_core_in.wait_recv()
    done(1 - k, c)
    to_core_in.wait_send()
    if half:
        piece = dst.at[1 - k, c, :, other]
        net.remote(piece, piece, own_core2, core).wait()
        to_y.wait_send()
    for d, s in hops:
        q, valid = chunk(d, s)

        @pl.when(valid)
        def _(d=d, s=s, q=q):
            a, b = dst.at[1 - k, q, :, mine], dst.at[1 - k, q, :, other]
            net.remote(a, a, aslot[d, s], core).wait()
            net.remote(b, b, bslot[d, s], core).wait()
            done(1 - k, q)
            net.remote(a, a, yslot[d, s], over_y).wait_send()

        sent = jnp.logical_and(no_right if d == 0 else no_left, chunk(d, s - 1)[1])

        @pl.when(sent)
        def _(d=d, s=s):
            piece = dst.at[k, c, :, mine]
            z_send(d, s, piece, c).wait_send()
    yield 1


class Hand:
    def __init__(self, net, groups):
        self.net, self.groups = net, groups
        self.steps = [(dc, dk) for dc in range(net.C) for dk in range(2)]
        self.steps = self.steps[1:] + self.steps[:1]
        self.zs = {(g, s): net.slot() for s in self.steps for g in range(len(groups))}
        self.xs = {(g, s): net.slot() for s in self.steps for g in range(len(groups))}
        self.keeps = []
        self.posted = self.relayed = 0

    def post(self, count):
        net = self.net
        mine = net.c * 4 + 2 * net.x + net.k
        for s in self.steps[self.posted:self.posted + count]:
            tc, tk = net.shard(s[0]), (net.k + s[1]) % 2
            for g, (pieces, whole) in enumerate(self.groups):
                for src, pick, put in pieces:
                    if s == (0, 0):
                        net.remote(src.at[pick(tc, tk)], put(mine), self.xs[g, s], net.over_x()).start()
                        keep = net.local(src.at[pick(tc, tk)], put(mine))
                        keep.start()
                        self.keeps.append(keep)
                    else:
                        net.remote(src.at[pick(tc, tk)], put(mine), self.zs[g, s], net.at(c=tc, k=tk)).start()
        self.posted += count

    def block(self, g, s, x):
        net = self.net
        return self.groups[g][1](net.shard(-s[0]) * 4 + 2 * x + (net.k + s[1]) % 2)

    def relay(self, count):
        net = self.net
        for s in self.steps[self.relayed:min(self.relayed + count, len(self.steps) - 1)]:
            for g in range(len(self.groups)):
                block = self.block(g, s, net.x)
                net.remote(block, block, self.zs[g, s], net.over_x()).wait_recv()
                net.remote(block, block, self.xs[g, s], net.over_x()).start()
        self.relayed += count

    def finish(self):
        net = self.net
        for s in self.steps:
            for g in range(len(self.groups)):
                block = self.block(g, s, 1 - net.x)
                net.remote(block, block, self.xs[g, s], net.over_x()).wait()
                if s != (0, 0):
                    net.remote(block, block, self.zs[g, s], net.over_x()).wait_send()
        for keep in self.keeps:
            keep.wait()


class Columns:
    def __init__(self, ref, first, width):
        self.ref, self.first, self.width = ref, first, width
        self.at = self

    def lanes(self, j):
        return pl.ds(pl.multiple_of((self.first + j) * self.width, 128), self.width)

    def __getitem__(self, j):
        return Slot(self.ref, self.lanes(j))

    def __setitem__(self, j, value):
        self.ref[:, :, self.lanes(j)] = value


def Slot(ref, lanes):
    return ref.at[:, :, lanes]


def reduce_scratch(C, rows, width, tiles, wire):
    w = width // tiles
    n = tiles // 2
    return [
        pltpu.VMEM((2, C, rows, w), wire),
        pltpu.VMEM((tiles, C, rows, w), wire),
        pltpu.VMEM((n, C, rows, w), BF),
        pltpu.VMEM((n, C, rows, w), BF),
        pltpu.VMEM((n, C, rows, w), F32),
        pltpu.VMEM((n, C - 1, rows, w), BF),
        pltpu.VMEM((n, C - 1, rows, w), BF),
        pltpu.VMEM((n, rows, w), BF),
    ]


def reduce_rows(net, product, scratch, out):
    osend, orecv, ysend, yrecv, sums, zsend, zrecv, joined = scratch
    n, C, rows, w = zsend.shape
    tiles, C = 2 * n, C + 1
    c, k, y = net.c, net.k, net.y
    core, over_y = net.core(), net.over_y()
    depth = osend.shape[0]
    cslot, yslot, jslot, zslot = net.slots(tiles), net.slots(n), net.slots(n), net.slots(n * (C - 1))

    def to_core(j):
        return net.remote(osend.at[j % depth], orecv.at[j], cslot + j, core)

    def to_y(j):
        return net.remote(ysend.at[j], yrecv.at[j], yslot + j, over_y)

    def column(j):
        return (j // n + 1 + y) % 2 * n + j % n

    def step(j, _):
        @pl.when(j < tiles)
        def _():
            @pl.when(j >= depth)
            def _():
                to_core(j - depth).wait_send()

            osend[j % depth] = product(1 - k, column(j)).astype(osend.dtype).reshape(C, rows, w)
            to_core(j).start()

        @pl.when(j > 0)
        def _():
            i = j - 1
            own = product(k, column(i)).reshape(C, rows, w)
            to_core(i).wait_recv()
            own = own + orecv.at[i][...].astype(F32)

            @pl.when(i < n)
            def _():
                ysend[i % n] = own.astype(BF)
                to_y(i % n).start()

            @pl.when(i >= n)
            def _():
                sums[i % n] = own

        return 0

    lax.fori_loop(0, tiles + 1, step, 0)
    yield 1
    low, high = c == 0, c == C - 1
    inner = jnp.logical_and(c > 0, c < C - 1)
    beside = net.at(c=jnp.where(low, 1, C - 2))

    def z(j, dc):
        return net.remote(zsend.at[j, dc - 1], zrecv.at[j, dc - 1], zslot + j * (C - 1) + dc - 1, net.at(c=net.shard(dc)))

    def join(j, dc):
        return net.remote(zsend.at[j, dc - 1], joined.at[j], jslot + j, beside)

    def through(j):
        zsend[j, 1] = sums[j, net.shard(2)].astype(BF)

        @pl.when(inner)
        def _():
            join(j, 2).wait_recv()
            zsend[j, 1] = (sums[j, net.shard(2)] + joined[j].astype(F32)).astype(BF)

        z(j, 2).start()

    ends = ((1, high), (C - 1, low))
    for j in range(n):
        to_y(j).wait_recv()
        sums[j] = sums[j] + yrecv.at[j][...].astype(F32)
        for dc, far in ends:
            zsend[j, dc - 1] = sums[j, net.shard(dc)].astype(BF)

            @pl.when(far)
            def _(dc=dc):
                join(j, dc).start()

            @pl.when(jnp.logical_not(far))
            def _(dc=dc):
                z(j, dc).start()

        if j:
            through(j - 1)
        if j == n - 1:
            through(j)
        yield 1
    for j in range(n):
        z(j, 2).wait_recv()
        out[j] = sums[j, c] + zrecv[j, 1].astype(F32)
        for dc, absent in ((1, low), (C - 1, high)):
            @pl.when(jnp.logical_not(absent))
            def _(dc=dc):
                z(j, dc).wait_recv()
                out[j] = out[j] + zrecv[j, dc - 1].astype(F32)
        yield 1
    for j in range(n):
        if j < depth:
            to_core(tiles - depth + j).wait_send()
        to_y(j).wait_send()
        z(j, 2).wait_send()
        for dc, far in ends:
            @pl.when(far)
            def _(dc=dc):
                join(j, dc).wait_send()

            @pl.when(jnp.logical_not(far))
            def _(dc=dc):
                z(j, dc).wait_send()
    yield 1


def half_of(ref, y, width):
    return ref[:, pl.ds(pl.multiple_of(y * width, 128), width)]


def gain_half(gains, y, row, blocks):
    return [gains[y * blocks + i].astype(F32)[row:row + 1] for i in range(blocks)]


def times_gain(value, rows):
    w = value.shape[1] // len(rows)
    return jnp.concatenate([value[:, i * w:(i + 1) * w] * r for i, r in enumerate(rows)], axis=1)


def swap_sums(net, part, out_buf, in_buf):
    out_buf[...] = jnp.broadcast_to(part, out_buf.shape)
    cp = net.remote(out_buf, in_buf, net.slot(), net.over_y())
    cp.start()
    cp.wait()
    return part + in_buf[:, 0:1]


def rotate(value, cosine, sine):
    return value * cosine + pltpu.roll(value, value.shape[1] // 2, 1) * sine


def steps_of(part, count):
    for _ in range(count):
        if next(part, 0) == 0:
            return


def layer_kernel(C, tiles, head, scale, tile, few, x_ref, a_gain, m_gain, few_gains, cot, freq, pair, wq, wk, wv, wo, wg, wu, wd,
                 xg_out, g_out, u_out, d_out, blk, ig, sums_out, q_grad, kv_grad, o_grad,
                 g_ref, gains, h_out, gh_out, zgu, zd, mine, act, wdd, xg, ht, ct, wgu, m_s, l_s, acc, red, rs, hn, gb, stats,
                 ggu, ggu_t, act_t, from_x, delta, own, peer, cin, xin, xq, zq, xo, zo, vec, vin, vx, vz, red_x, rs_x,
                 send, recv, loc):
    qp, kp, cosine, sine, wqkv, wod, raw, q_out, kv, kvp, o_out, lse = mine
    net = Net(C, send, recv, loc)
    c, x, y, k = net.c, net.x, net.y, net.k
    B, unit = wg.shape[0], wdd.shape[0]
    R, D = x_ref.shape
    H = D // 2
    T = 2 * C * R
    w = D // tiles
    blocks = gains.shape[0]
    plane = [(dc, dx, dk) for dc in range(C) for dx in range(2) for dk in range(2)][1:]
    mates = [net.at(c=net.shard(dc), x=(x + dx) % 2, k=(k + dk) % 2) for dc, dx, dk in plane]
    net.meet(mates + [net.over_y()])
    me = c * 4 + 2 * x + k
    g_ref[...] = jnp.concatenate(
        [a_gain[...].astype(F32), m_gain[...].astype(F32), pltpu.roll(few_gains[...], me * few, 1)[0:2],
         jnp.zeros((12, B), F32)], axis=0).astype(BF)
    sent = []
    for to in mates:
        cp = net.remote(g_ref, gains.at[me], net.slot(), to)
        cp.start()
        sent.append(cp)
    own_gains = net.local(g_ref, gains.at[me])
    own_gains.start()
    full = slice(None)
    lanes = lambda n, m: pl.ds(pl.multiple_of(n * m, 128), m)
    rows = lambda b: pl.ds(pl.multiple_of(b * B, B), B)
    part = lambda tc, tk, m: pl.ds(pl.multiple_of((2 * tc + tk) * m, 128), m)
    g_qkv = (
        [(wq, lambda tc, tk: (full, part(tc, tk, head)), lambda b: wqkv.at[rows(b), pl.ds(0, head)]),
         (wk, lambda tc, tk: (full, lanes(tc, head)), lambda b: wqkv.at[rows(b), pl.ds(head, head)]),
         (wv, lambda tc, tk: (full, lanes(tc, head)), lambda b: wqkv.at[rows(b), pl.ds(2 * head, head)])],
        lambda b: wqkv.at[rows(b), :])
    g_o = ([(wo, lambda tc, tk: (part(tc, tk, head), full), lambda b: wod.at[:, lanes(b, B)])],
           lambda b: wod.at[:, lanes(b, B)])
    g_gu = (
        [(wg, lambda tc, tk: (full, part(tc, tk, unit)), lambda b: wgu.at[rows(b), pl.ds(0, unit)]),
         (wu, lambda tc, tk: (full, part(tc, tk, unit)), lambda b: wgu.at[rows(b), pl.ds(unit, unit)])],
        lambda b: wgu.at[rows(b), :])
    g_d = ([(wd, lambda tc, tk: (part(tc, tk, unit), full), lambda b: wdd.at[:, lanes(b, B)])],
           lambda b: wdd.at[:, lanes(b, B)])
    h_qkv, h_o, h_mlp = Hand(net, [g_qkv]), Hand(net, [g_o]), Hand(net, [g_gu, g_d])
    every = 2 * C

    def normalise(kk, q):
        value = ht[kk, q].astype(F32)
        hat = value * lax.rsqrt(jnp.mean(value * value, axis=-1, keepdims=True) + EPS)
        for b in range(blocks):
            t = pl.ds(b * B, B)
            xg[kk, q, :, t] = (hat[:, b * B:(b + 1) * B] * gains[b].astype(F32)[0:1]).astype(BF)

    rows_x = gather_rows(net, x_ref, ht, False, normalise)
    next(rows_x)
    h_qkv.post(2)
    for kk in range(2):
        for q in range(C):
            base = jnp.where(x == 0, pair[q], 2 * C - 1 - pair[q]) * (2 * R) + kk * R
            r = pl.ds((kk * C + q) * R, R)
            spot = lax.broadcasted_iota(jnp.int32, (R, 128), 0) + base
            qp[r] = spot
            kp[:, r] = lax.broadcasted_iota(jnp.int32, (8, R), 1) + base
            angle = spot.astype(F32) * freq[0:1]
            sign = jnp.where(lax.broadcasted_iota(jnp.int32, (R, 128), 1) < head // 2, -1.0, 1.0)
            cosine[r] = jnp.cos(angle)
            sine[r] = jnp.sin(angle) * sign

    for _ in range(C - 1):
        steps_of(rows_x, 2)
        h_qkv.post(2)
        h_qkv.relay(2)
    own_gains.wait()
    for cp in sent:
        cp.wait()
    h_qkv.relay(1)
    run(rows_x)
    h_qkv.finish()
    h_o.post(every)
    h_mlp.post(every - 1)
    keep = net.local(xg, xg_out)
    keep.start()
    per = tile // R
    gain_sum = jnp.sum(gains[...].astype(F32), axis=0)
    qg, kg = gain_sum[2:3], gain_sum[3:4]
    for kk in range(2):
        def project(i, _, kk=kk):
            r = pl.ds(pl.multiple_of(kk * C * R + i * tile, tile), tile)
            v = jnp.dot(xg[kk, pl.ds(i * per, per)].reshape(tile, D), wqkv[...], preferred_element_type=F32)
            raw[r] = v[:, :2 * head]
            cs, sn = cosine[r], sine[r]
            q = v[:, :head]
            q = q * lax.rsqrt(jnp.mean(q * q, axis=-1, keepdims=True) + EPS)
            q_out[r] = rotate(q * qg, cs, sn).astype(BF)
            key = v[:, head:2 * head]
            key = key * lax.rsqrt(jnp.mean(key * key, axis=-1, keepdims=True) + EPS)
            kv[r, 0:head] = rotate(key * kg, cs, sn).astype(BF)
            kv[r, head:2 * head] = v[:, 2 * head:].astype(BF)
            return 0

        lax.fori_loop(0, C * R // tile, project, 0)
    swap = net.remote(kv, kvp, net.slot(), net.over_x())
    swap.start()
    h_mlp.post(1)

    def attend(i, _):
        r = pl.ds(pl.multiple_of(i * tile, tile), tile)
        s = lax.dot_general(q_out[r], kv[:, :head], NT, preferred_element_type=F32) * scale
        s = jnp.where(kp[0:1] <= qp[r, 0:1], s, NEG)
        top = jnp.max(s, axis=-1, keepdims=True)
        e = jnp.exp(s - top)
        m_s[r] = jnp.broadcast_to(top, (tile, 128))
        l_s[r] = jnp.broadcast_to(jnp.sum(e, axis=-1, keepdims=True), (tile, 128))
        acc[r] = jnp.dot(e.astype(BF), kv[:, head:], preferred_element_type=F32)
        return 0

    def attend_more(i, _):
        r = pl.ds(pl.multiple_of(i * tile, tile), tile)
        s = lax.dot_general(q_out[r], kvp[:, :head], NT, preferred_element_type=F32) * scale
        old = m_s[r, 0:1]
        top = jnp.maximum(old, jnp.max(s, axis=-1, keepdims=True))
        e = jnp.exp(s - top)
        shrink = jnp.exp(old - top)
        m_s[r] = jnp.broadcast_to(top, (tile, 128))
        l_s[r] = jnp.broadcast_to(l_s[r, 0:1] * shrink + jnp.sum(e, axis=-1, keepdims=True), (tile, 128))
        acc[r] = acc[r] * shrink + jnp.dot(e.astype(BF), kvp[:, head:], preferred_element_type=F32)
        return 0

    steps = T // tile
    lax.fori_loop(0, steps, attend, 0)
    h_o.relay(every - 1)
    swap.wait()

    @pl.when(x == 1)
    def _():
        lax.fori_loop(0, steps, attend_more, 0)

    o_out[...] = (acc[...] / l_s[...]).astype(BF)
    for i in range(steps):
        r = pl.ds(i * tile, tile)
        lse[:, r] = (m_s[r] + jnp.log(l_s[r])).T[0:8]
    h_o.finish()

    def product(kk, t):
        return jnp.dot(o_out[pl.ds(pl.multiple_of(kk * C * R, C * R), C * R)], wod[:, lanes(t, w)],
                       preferred_element_type=F32)

    reduce = reduce_rows(net, product, red, rs)
    next(reduce)
    h_mlp.relay(2)
    for _ in range(tiles // 2):
        steps_of(reduce, 1)
        h_mlp.relay(1)
    cots = gather_rows(net, cot, ct, False)
    next(cots)
    h_mlp.relay(every - 3 - tiles // 2)
    run(reduce)
    half = half_of(x_ref, y, H).astype(F32) + jnp.concatenate([rs[j] for j in range(tiles // 2)], axis=1)
    total = swap_sums(net, jnp.sum(half * half, axis=-1, keepdims=True), stats.at[0], stats.at[1])
    hs = lax.rsqrt(total / D + EPS)
    h_out[...] = half
    hn[...] = times_gain(half * hs, gain_half(gains, y, 1, blocks // 2)).astype(BF)
    rows_h = gather_rows(net, hn, ht, True)
    next(rows_h)
    run(cots, rows_h)
    h_mlp.finish()

    for kk in range(2):
        def swiglu(i, _, kk=kk):
            rr = pl.ds(pl.multiple_of(i * tile, tile), tile)
            r = pl.ds(pl.multiple_of(kk * C * R + i * tile, tile), tile)
            gu = jnp.dot(ht[kk, pl.ds(i * per, per)].reshape(tile, D), wgu[...], preferred_element_type=F32)
            ga = lax.dot_general(ct[kk, pl.ds(i * per, per)].reshape(tile, D), wdd[...], NT,
                                 preferred_element_type=F32)
            gate, up = gu[:, :unit], gu[:, unit:]
            sigma = jax.nn.sigmoid(gate)
            silu = gate * sigma
            a = (silu * up).astype(BF)
            act[kk, rr] = a
            act_t[:, r] = a.T
            gg = (ga * up * (sigma * (1.0 + gate * (1.0 - sigma)))).astype(BF)
            gu = (ga * silu).astype(BF)
            ggu[kk, rr, 0:unit] = gg
            ggu[kk, rr, unit:2 * unit] = gu
            ggu_t[0:unit, r] = gg.T
            ggu_t[unit:2 * unit, r] = gu.T
            return 0

        lax.fori_loop(0, C * R // tile, swiglu, 0)

    def normed(kk, t):
        return lax.dot_general(ggu[kk], wgu[lanes(t, w), :], NT, preferred_element_type=F32)

    pair = 2 * B

    def weight_grads(block, out):
        t = lanes(block, pair)
        out(0, 2 * unit, jnp.dot(ggu_t[...], ht[:, :, :, t].reshape(T, pair), preferred_element_type=F32))
        out(2 * unit, 3 * unit, jnp.dot(act_t[...], ct[:, :, :, t].reshape(T, pair), preferred_element_type=F32))

    swaps = []

    def to_x(q):
        if q < C - 1:
            return wgu.at[pl.ds(0, 2 * unit), pl.ds(q * pair, pair)], wgu.at[pl.ds(2 * unit, unit), pl.ds(q * pair, pair)]
        return wgu.at[pl.ds(3 * unit, 2 * unit), pl.ds(0, pair)], wgu.at[pl.ds(3 * unit, unit), pl.ds(pair, pair)]

    def send_partial(q):
        def out(a, b, v):
            to_x(q)[a // (2 * unit)][...] = v.astype(BF)

        weight_grads(net.shard(q + 1) * 2 + 1 - x, out)
        pieces = pl.ds(0, 2 * unit), pl.ds(2 * unit, unit)
        swaps.append([net.remote(a, from_x.at[q, r], net.slot(), net.over_x()) for a, r in zip(to_x(q), pieces)])
        for cp in swaps[q]:
            cp.start()

    place = lambda a, b, m: pl.ds(pl.multiple_of((2 * a + b) * m, 128), m)

    def add_partial(q):
        dc = (q + 1) % C
        for cp in swaps[q]:
            cp.wait_recv()

        def out(a, b, v):
            v = v + from_x[q, a:b].astype(F32)
            for kk in range(2):
                part = v[:, kk * B:(kk + 1) * B]
                dk = lax.rem(kk + k, 2)
                if a:
                    zd[2 * dc + dk] = part.astype(BF)
                else:
                    zgu[2 * dc + dk] = part.T.astype(BF)

        weight_grads(net.shard(dc) * 2 + x, out)

    keep.wait()
    hand_out = Deal(net, swiglu_groups(g_out, u_out, d_out, zgu, zd, unit))
    reduce = reduce_rows(net, normed, red, rs)
    next(reduce)
    for q in range(C):
        send_partial(q)
        steps_of(reduce, tiles // 2 // C)
    run(reduce)
    g = jnp.concatenate([rs[j] for j in range(tiles // 2)], axis=1)
    hat = half * hs
    col = jnp.sum(g * hat, axis=0, keepdims=True)
    n = vec.shape[2]
    count = H // n
    vec[0] = jnp.zeros(vec.shape[1:], F32)
    for i in range(count):
        vec[0, count + i:count + i + 1] = col[:, i * n:(i + 1) * n]
    m = times_gain(g, gain_half(gains, y, 1, blocks // 2))
    mean = swap_sums(net, jnp.sum(m * hat, axis=-1, keepdims=True), stats.at[2], stats.at[3]) / D
    gh = half_of(cot, y, H).astype(F32) + hs * (m - hat * mean)
    gh_out[...] = gh
    gb[...] = gh.astype(BF)
    rows_g = gather_rows(net, gb, xg, True)
    next(rows_g)
    add_partial(0)
    steps_of(rows_g, 2)
    add_partial(1)
    steps_of(rows_g, 4)
    add_partial(2)
    run(rows_g)
    hand_out.post(6)

    def rows_of(i):
        return pl.ds(pl.multiple_of(i * tile, tile), tile)

    def grad_o(i, _):
        r = rows_of(i)
        per = tile // R
        g = lax.dot_general(xg[i // (steps // 2), pl.ds((i % (steps // 2)) * per, per)].reshape(tile, D), wod[...], NT,
                            preferred_element_type=F32).astype(BF)
        ggu[i // (steps // 2), pl.ds(pl.multiple_of(i % (steps // 2) * tile, tile), tile), pl.ds(2 * head, head)] = g
        d = jnp.sum(g.astype(F32) * o_out[r].astype(F32), axis=-1, keepdims=True)
        delta[:, r] = jnp.broadcast_to(d, (tile, 128)).T[0:8]
        return 0

    lax.fori_loop(0, steps, grad_o, 0)
    add_partial(C - 1)
    hand_out.post(2)
    keeps = [net.local(zgu.at[0, :, pl.ds(0, unit)], g_out.at[:, place(c, k, unit)]),
             net.local(zgu.at[0, :, pl.ds(unit, unit)], u_out.at[:, place(c, k, unit)]),
             net.local(zd.at[0], d_out.at[place(c, k, unit), :])]
    load_x = net.local(xg_out, ct)
    for cp in keeps + [load_x]:
        cp.start()
    for copies in swaps:
        for cp in copies:
            cp.wait_send()
    acc[...] = jnp.zeros_like(acc)
    own[...] = jnp.zeros_like(own)

    def sweep(keys, grads, masked):
        def step(i, _):
            r = rows_of(i)
            q = q_out[r]
            g = ggu[i // (steps // 2), pl.ds(pl.multiple_of(i % (steps // 2) * tile, tile), tile), pl.ds(2 * head, head)]
            s = lax.dot_general(keys[:, :head], q, NT, preferred_element_type=F32) * scale
            p = jnp.exp(s - lse[0:1, r])
            if masked:
                p = jnp.where(qp[:, 0:1] <= kp[0:1, r], p, 0.0)
            grads[1] += jnp.dot(p.astype(BF), g, preferred_element_type=F32)
            dp = lax.dot_general(keys[:, head:], g, NT, preferred_element_type=F32)
            ds = (p * (dp - delta[0:1, r])).astype(BF)
            grads[0] += jnp.dot(ds, q, preferred_element_type=F32)
            acc[r] += lax.dot_general(ds, keys[:, :head], TN, preferred_element_type=F32)
            return 0

        lax.fori_loop(0, steps, step, 0)

    one = net.remote(peer.at[1 - k], cin.at[0], net.slot(), net.core())
    two = net.remote(l_s, xin, net.slot(), net.over_x())
    three = net.remote(own.at[1 - k], cin.at[1], net.slot(), net.core())

    @pl.when(x == 1)
    def _():
        peer[...] = jnp.zeros_like(peer)
        sweep(kvp, peer, False)
        one.start()
        one.wait()
        l_s[...] = peer[k] + cin[0]
        two.start()

    sweep(kv, own, True)
    three.start()

    def down(kk, t):
        return jnp.dot(act[kk], wdd[:, lanes(t, w)], preferred_element_type=F32)

    reduce_d = reduce_rows(net, down, red, rs)
    next(reduce_d)

    def back_norm(grad, value, gain, r):
        rotated = grad * cosine[r] - pltpu.roll(grad, head // 2, 1) * sine[r]
        factor = lax.rsqrt(jnp.mean(value * value, axis=-1, keepdims=True) + EPS)
        hat = value * factor
        m = rotated * gain
        result = factor * (m - hat * jnp.mean(m * hat, axis=-1, keepdims=True))
        return result, jnp.sum(rotated * hat, axis=0, keepdims=True)

    def finish_q(i, total):
        r = rows_of(i)
        g, col = back_norm(acc[r] * scale, raw[r, 0:head], qg, r)
        ggu[i // (steps // 2), pl.ds(pl.multiple_of(i % (steps // 2) * tile, tile), tile), pl.ds(0, head)] = g.astype(BF)
        return total + col

    vec[0, 2 * count:2 * count + 1] = lax.fori_loop(0, steps, finish_q, jnp.zeros((1, head), F32))
    def keep_o(v):
        o_grad[place(c, k, head), :] = v.astype(BF)

    deal_o = Deal(net, [
        (from_x, lambda b: (2, pl.ds(pl.multiple_of(b // 2 * head, head), head), lanes(b % 2, B)), xo, zo,
         [((full, full), lambda a, b: o_grad.at[place(a, b, head), :])], keep_o, False),
    ])
    for i in range(tiles):
        from_x[2, pl.ds(i * head, head), :] = lax.dot_general(
            o_out[...], xg[:, :, :, pl.ds(i * w, w)].reshape(T, w), TN, preferred_element_type=F32).astype(BF)
    three.wait()
    m_s[...] = own[k] + cin[1]

    @pl.when(x == 1)
    def _():
        two.wait_send()

    @pl.when(x == 0)
    def _():
        two.wait_recv()
        m_s[...] = m_s[...] + xin[...]

    def finish_kv(i, total):
        r = rows_of(i)
        v = m_s[r]
        g, col = back_norm(v * scale, raw[r, head:2 * head], kg, r)
        ggu[i // (steps // 2), pl.ds(pl.multiple_of(i % (steps // 2) * tile, tile), tile), pl.ds(head, head)] = jnp.where(k == 0, g, v).astype(BF)
        return total + jnp.where(k == 0, col, 0.0)

    deal_o.start()
    vec[0, 2 * count + 1:2 * count + 2] = lax.fori_loop(0, steps, finish_kv, jnp.zeros((1, head), F32))

    def product(kk, t):
        a = lax.dot_general(ggu[kk, :, 0:head], wqkv[lanes(t, w), 0:head], NT, preferred_element_type=F32)
        return a + lax.dot_general(ggu[kk, :, head:2 * head], wqkv[lanes(t, w), lanes(1 + k, head)], NT,
                                   preferred_element_type=F32)

    def keep_q(v):
        q_grad[:, place(c, k, head)] = v[:, :head].astype(BF)
        kv_grad[k, :, lanes(c, head)] = v[:, head:].astype(BF)

    deal_q = Deal(net, [
        (from_x, lambda b: (b // 8, pl.ds(pl.multiple_of(b // 2 % 4 * (2 * head), 2 * head), 2 * head), lanes(b % 2, B)), xq, zq,
         [((full, pl.ds(0, head)), lambda a, b: q_grad.at[:, place(a, b, head)]),
          ((full, pl.ds(head, head)), lambda a, b: kv_grad.at[b, :, lanes(a, head)])], keep_q, True),
    ])
    steps_of(reduce_d, 1)
    reduce = reduce_rows(net, product, red_x, rs_x)
    load_x.wait()
    next(reduce)
    for i in range(tiles):
        t = pl.ds(i * w, w)
        from_x[i // 4, pl.ds(i % 4 * 2 * head, 2 * head), :] = lax.dot_general(
            ggu[:, :, 0:2 * head].reshape(T, 2 * head), ct[:, :, :, t].reshape(T, w), TN,
            preferred_element_type=F32).astype(BF)
    deal_q.start()
    steps_of(reduce, 1)
    for _ in range(tiles // 2 - 1):
        steps_of(reduce_d, 1)
        steps_of(reduce, 1)
    deal_o.both(2 * C)
    deal_q.both(2 * C)
    run(reduce_d)
    blk[y] = (h_out[...] + jnp.concatenate([rs[j] for j in range(tiles // 2)], axis=1)).astype(BF)
    swap_b = net.remote(blk.at[y], blk.at[y], net.slot(), net.over_y())
    swap_b.start()
    run(reduce)
    value = x_ref[...].astype(F32)
    xscale = lax.rsqrt(jnp.mean(value * value, axis=-1, keepdims=True) + EPS)
    hat = half_of(x_ref, y, H).astype(F32) * xscale
    g = jnp.concatenate([rs_x[j] for j in range(tiles // 2)], axis=1)
    col = jnp.sum(g * hat, axis=0, keepdims=True)
    for i in range(count):
        vec[0, i:i + 1] = col[:, i * n:(i + 1) * n]
    first = net.remote(vec.at[0], vin, net.slot(), net.core())
    first.start()
    m = times_gain(g, gain_half(gains, y, 0, blocks // 2))
    mean = swap_sums(net, jnp.sum(m * hat, axis=-1, keepdims=True), stats.at[4], stats.at[5]) / D
    ig[y] = (gh_out[...] + xscale * (m - hat * mean)).astype(BF)
    swap = net.remote(ig.at[y], ig.at[y], net.slot(), net.over_y())
    swap.start()
    first.wait()
    vec[1] = vec[0] + vin[...]
    second = net.remote(vec.at[1], vx, net.slot(), net.over_x())
    second.start()
    second.wait()
    vz[c] = vec[1] + vx[...]
    third = []
    for dc in range(1, C):
        cp = net.remote(vz.at[c], vz.at[c], net.slot(), net.at(c=net.shard(dc)))
        cp.start()
        third.append(cp)
    for cp in third:
        cp.wait()
    total = vz[0]
    for i in range(1, C):
        total = total + vz[i]
    sums_out[y] = total
    last = net.remote(sums_out.at[y], sums_out.at[y], net.slot(), net.over_y())
    last.start()
    hand_out.finish()
    deal_o.finish()
    deal_q.finish()
    last.wait()
    swap.wait()
    swap_b.wait()
    for cp in keeps:
        cp.wait()


def swiglu_groups(g_out, u_out, d_out, zgu, zd, unit):
    full = slice(None)
    place = lambda a, b: pl.ds(pl.multiple_of((2 * a + b) * unit, 128), unit)
    return [
        (None, None, None, zgu,
         [((full, pl.ds(0, unit)), lambda a, b: g_out.at[:, place(a, b)]),
          ((full, pl.ds(unit, unit)), lambda a, b: u_out.at[:, place(a, b)])], None, False),
        (None, None, None, zd, [((full, full), lambda a, b: d_out.at[place(a, b), :])], None, False),
    ]


class Deal:
    def __init__(self, net, groups):
        self.net, self.groups = net, groups
        self.order = [(dc, dk) for dc in range(1, net.C) for dk in range(2)] + [(0, 1), (0, 0)]
        self.xs, self.zs = {}, []
        self.added = self.posted = 0

    def start(self):
        net = self.net
        for s in self.order:
            b = net.shard(s[0]) * 4 + 2 * (1 - net.x) + (net.k + s[1]) % 2
            for g, (partial, place, from_x, *_) in enumerate(self.groups):
                cp = net.remote(partial.at[place(b)], from_x.at[2 * s[0] + s[1]], net.slot(), net.over_x())
                cp.start()
                self.xs[g, s] = cp

    def add(self, count):
        net = self.net
        for s in self.order[self.added:self.added + count]:
            i = 2 * s[0] + s[1]
            b = net.shard(s[0]) * 4 + 2 * net.x + (net.k + s[1]) % 2
            for g, (partial, place, from_x, sums, puts, keep, flip) in enumerate(self.groups):
                self.xs[g, s].wait_recv()
                total = partial[place(b)].astype(F32) + from_x[i].astype(F32)
                if flip:
                    total = total.T
                if s == (0, 0) and keep is not None:
                    keep(total)
                else:
                    sums[i] = total.astype(BF)
        self.added += count

    def post(self, count):
        net = self.net
        for s in self.order[self.posted:min(self.posted + count, len(self.order) - 1)]:
            i = 2 * s[0] + s[1]
            to = net.at(c=net.shard(s[0]), k=(net.k + s[1]) % 2)
            for partial, place, from_x, sums, puts, keep, flip in self.groups:
                slot = net.slot()
                for take, put in puts:
                    net.remote(sums.at[(i,) + take], put(net.c, net.k), slot, to).start()
                self.zs.append((sums, i, slot))
        self.posted += count

    def both(self, count):
        for _ in range(count):
            self.add(1)
            self.post(1)

    def finish(self):
        for sums, i, slot in self.zs:
            self.net.remote(sums.at[i], sums.at[i], slot, self.net.over_x()).wait()
        for cp in self.xs.values():
            cp.wait_send()


def finish_kernel(few, blk, ig, sums, g, u, d, q, kv, o, block_out, input_grad, a_gain, q_w, k_w, v_w, q_gain, k_gain,
                  o_w, m_gain, g_w, u_w, d_w):
    mine = lax.axis_index(CONTEXT) * 4 + lax.axis_index(FSDP)
    H = blk.shape[2]
    n = H // sums.shape[2]
    for i in range(2):
        block_out[:, i * H:(i + 1) * H] = blk[i]
        input_grad[:, i * H:(i + 1) * H] = ig[i].astype(F32)
    for out, value in ((q_w, q), (o_w, o), (g_w, g), (u_w, u), (d_w, d)):
        out[...] = value[...].astype(F32)
    k_w[...] = kv[0].astype(F32)
    v_w[...] = kv[1].astype(F32)
    half, row = mine // n, mine % n
    a_gain[...] = sums[half, pl.ds(row, 1)]
    m_gain[...] = sums[half, pl.ds(n + row, 1)]
    lanes = sums.shape[2]
    total = sums[0] + sums[1]
    shift = lax.rem(lanes - mine * few, lanes)
    q_gain[...] = pltpu.roll(total[2 * n:2 * n + 8], shift, 1)[0:1, 0:few]
    k_gain[...] = pltpu.roll(total[2 * n:2 * n + 8], shift, 1)[1:2, 0:few]


def call(kernel, name, cid, out_shape, in_specs, out_specs, scratch, *args):
    return pl.pallas_call(
        kernel, name=name, out_shape=out_shape, in_specs=in_specs, out_specs=out_specs,
        scratch_shapes=scratch + [
            pltpu.SemaphoreType.DMA((SLOTS,)), pltpu.SemaphoreType.DMA((SLOTS,)), pltpu.SemaphoreType.DMA((LOCAL_SLOTS,)),
        ],
        compiler_params=pltpu.CompilerParams(
            collective_id=cid, has_side_effects=True, vmem_limit_bytes=67043328
        ),
    )(*args)


def tensor_parallel(layer_input, block_pair, attn_gain, q_weight, key_projection, value_projection, q_gain, k_gain,
                    o_weight, mlp_gain, gate_weight, up_weight, down_weight, cotangent):
    C = lax.axis_size(CONTEXT)
    R, D = layer_input.shape
    B = q_weight.shape[0]
    NB = 4 * C
    T = 2 * C * R
    H = D // 2
    head = HEAD_SIZE
    unit = gate_weight.shape[1] // (2 * C)
    scale = 1.0 / math.sqrt(head)
    S = jax.ShapeDtypeStruct
    k = lax.axis_index(FSDP) % 2
    x = lax.axis_index(FSDP) // 2
    TILES = 8

    red = lambda wire: reduce_scratch(C, R, D, TILES, wire)
    rs = lambda: pltpu.VMEM((TILES // 2, R, D // TILES), F32)
    stat = lambda: pltpu.VMEM((R, 128), F32)
    mine = lax.axis_index(CONTEXT) * 4 + lax.axis_index(FSDP)
    rows_of = lambda v: v.reshape(1, -1)
    freq = np.exp(np.arange(head // 2, dtype=np.float32) * np.float32(-2.0 * math.log(THETA) / head))
    freq = np.broadcast_to(np.concatenate([freq, freq])[None, :], (8, head))
    small = jnp.pad(jnp.stack([q_gain, k_gain]), ((0, 6), (0, head - q_gain.shape[0]))).astype(F32)
    vm = lambda *shape: pltpu.VMEM(shape, BF)
    f32 = lambda *shape: pltpu.VMEM(shape, F32)
    mine_s = [pltpu.VMEM((T, 128), jnp.int32), pltpu.VMEM((8, T), jnp.int32), f32(T, 128), f32(T, 128), vm(D, 3 * head),
              vm(head, D), f32(T, 2 * head), vm(T, head), vm(T, 2 * head), vm(T, 2 * head), vm(T, head), f32(8, T)]
    E = len(mine_s)
    V = (2 * (H // 128) + 8, 128)
    wide = lambda: pltpu.VMEM((2, T, head), F32)
    one = lambda: pltpu.VMEM((T, head), F32)
    narrow = red(BF)
    inner = [narrow[0]] + narrow[4:]

    def layer(*r):
        a = 24 + 6
        b = a + E
        c = b + 9
        d = c + 8
        e = d + 8 + 13
        osend, *rest = r[e:e + 5]
        ht = r[b + 3]
        views = (osend, Columns(ht.at[0], 0, D // TILES), Columns(ht.at[1], 0, D // TILES),
                 Columns(ht.at[1], TILES // 2, D // TILES), *rest)
        return layer_kernel(C, TILES, head, scale, 256, q_gain.shape[0], *r[:a], r[a:b], *r[b:c], r[c:d], *r[d:e], views, *r[e + 5:])

    g_w, u_w, d_w, blk, ig, sums, q_w, kv_w, o_w = call(
        layer, "layer", 1,
        (S((2, C, R, D), BF), S((B, 2 * C * unit), BF), S((B, 2 * C * unit), BF), S((2 * C * unit, B), BF),
         S((2, R, H), BF), S((2, R, H), BF), S((2,) + V, F32), S((B, 2 * C * head), BF), S((2, B, C * head), BF),
         S((2 * C * head, B), BF)),
        [VM] * 6 + [pl.BlockSpec(memory_space=pltpu.SMEM)] + [HBM] * 7, (HBM,) * 4 + (VM,) * 6,
        [vm(16, B), vm(NB, 16, B), f32(R, H), f32(R, H), vm(2 * C, B, 2 * unit), vm(2 * C, unit, B)] + mine_s
        + [vm(2, C * R, unit), vm(unit, D), vm(2, C, R, D), vm(2, C, R, D), vm(2, C, R, D), vm(D, 2 * unit),
           f32(T, 128), f32(T, 128), f32(T, head)] + red(F32)
        + [rs(), vm(R, H), vm(R, H), f32(6, R, 128), vm(2, C * R, 2 * unit), vm(2 * unit, T), vm(unit, T),
           vm(C, 3 * unit, 2 * B)]
        + [f32(8, T), wide(), wide(), wide(), one(), vm(2 * C, 2 * head, B), vm(2 * C, B, 2 * head), vm(2 * C, head, B),
           vm(2 * C, head, B), f32(2, *V), f32(*V), f32(*V), f32(C, *V)]
        + inner + [rs()],
        layer_input, rows_of(attn_gain), rows_of(mlp_gain), small, cotangent, freq, block_pair,
        q_weight, key_projection, value_projection, o_weight, gate_weight, up_weight, down_weight,
    )[1:]
    few = q_gain.shape[0]
    wide_w = lambda v: S(v.shape, F32)
    STEPS = 4
    part = lambda *shape: pl.BlockSpec((shape[0] // STEPS,) + shape[1:], lambda i: (i,) + (0,) * (len(shape) - 1))
    inner_part = lambda n, m, w: pl.BlockSpec((n, m // STEPS, w), lambda i: (0, i, 0))
    same = lambda *shape: pl.BlockSpec(shape, lambda i: (0,) * len(shape))
    kv_part = part(*kv_w.shape[1:])
    out = pl.pallas_call(
        functools.partial(finish_kernel, few), name="finish", grid=(STEPS,),
        out_shape=(S((R, D), BF), S((R, D), F32), S((1, B), F32), wide_w(q_w), S(kv_w.shape[1:], F32),
                   S(kv_w.shape[1:], F32), S((1, few), F32), S((1, few), F32), wide_w(o_w), S((1, B), F32),
                   wide_w(g_w), wide_w(u_w), wide_w(d_w)),
        in_specs=[inner_part(*blk.shape), inner_part(*ig.shape), same(*sums.shape), part(*g_w.shape), part(*u_w.shape),
                  part(*d_w.shape), part(*q_w.shape), inner_part(*kv_w.shape), part(*o_w.shape)],
        out_specs=(part(R, D), part(R, D), same(1, B), part(*q_w.shape), kv_part, kv_part, same(1, few), same(1, few),
                   part(*o_w.shape), same(1, B), part(*g_w.shape), part(*u_w.shape), part(*d_w.shape)),
        compiler_params=pltpu.CompilerParams(vmem_limit_bytes=60 * 1024 * 1024),
    )(blk, ig, sums, g_w, u_w, d_w, q_w, kv_w, o_w)
    return tuple(v.reshape(v.shape[1:]) if i in (2, 6, 7, 9) else v for i, v in enumerate(out))


def fits(mesh_shape, layer_input, q_weight, key_projection, gate_weight):
    C = mesh_shape[CONTEXT]
    return (
        mesh_shape[FSDP] == 4 and mesh_shape[HEADS] == 2
        and key_projection.shape[1] == C * HEAD_SIZE and q_weight.shape[1] == 2 * C * HEAD_SIZE
        and gate_weight.shape[1] % (2 * C * 128) == 0 and 5 * gate_weight.shape[1] <= 2 * C * layer_input.shape[1]
        and gate_weight.shape[1] >= 6 * C * 128 and q_weight.shape[0] == 128
        and C == 4 and layer_input.shape[0] % 128 == 0 and layer_input.shape[1] % (8 * 128) == 0
    )


def solution(mesh):
    def program(*args):
        layer_input, q_weight, key_projection, gate_weight = args[0], args[3], args[4], args[10]
        if fits(dict(mesh.shape), layer_input, q_weight, key_projection, gate_weight):
            return tensor_parallel(*args)
        return per_device(*args)

    return jax.shard_map(
        program,
        mesh=mesh,
        in_specs=(
            P(ROWS, None),
            P(),
            P(ROWS),
            P(ROWS, HEADS),
            P(ROWS, HEADS),
            P(ROWS, HEADS),
            P(ROWS),
            P(ROWS),
            P(HEADS, ROWS),
            P(ROWS),
            P(ROWS, HEADS),
            P(ROWS, HEADS),
            P(HEADS, ROWS),
            P(ROWS, None),
        ),
        out_specs=(
            P(ROWS, None),
            P(ROWS, None),
            P(ROWS),
            P(ROWS, HEADS),
            P(ROWS, HEADS),
            P(ROWS, HEADS),
            P(ROWS),
            P(ROWS),
            P(HEADS, ROWS),
            P(ROWS),
            P(ROWS, HEADS),
            P(ROWS, HEADS),
            P(HEADS, ROWS),
        ),
        check_vma=False,
    )
```

```python
import functools
import math

import jax
import jax.numpy as jnp
import numpy as np
from jax import lax
from jax.experimental import pallas as pl
from jax.experimental.pallas import tpu as pltpu
from jax.sharding import PartitionSpec as P

HEAD_SIZE = 128
CONTEXT, FSDP, HEADS = "context", "fsdp", "heads"
ROWS = (CONTEXT, FSDP)


EPS = 1e-06
THETA = 1000000.0
NEG = -1e30


def row_places(block_pair, row_ids, block_len):
    owners = block_pair.shape[0]
    holder = row_ids // (2 * block_len)
    within = row_ids % (2 * block_len)
    match = holder[:, None] == jnp.arange(owners, dtype=jnp.int32)[None, :]
    paired = jnp.sum(jnp.where(match, block_pair[None, :], 0), axis=1)
    which = jnp.where(within >= block_len, 2 * owners - 1 - paired, paired)
    return which * block_len + within % block_len


def rope_tables(places, head_dim):
    half = head_dim // 2
    freq = jnp.exp(jnp.arange(half, dtype=jnp.float32) * (-2.0 * math.log(THETA) / head_dim))
    angle = places.astype(jnp.float32)[:, None] * freq[None, :]
    return (jnp.cos(angle)[:, None, :], jnp.sin(angle)[:, None, :])


def apply_rotary(field, cosine_table, sine_table):
    half = field.shape[-1] // 2
    first = field[..., :half]
    second = field[..., half:]
    return jnp.concatenate(
        [first * cosine_table - second * sine_table, second * cosine_table + first * sine_table],
        axis=-1,
    )


def unrotate(grad, cosine_table, sine_table):
    half = grad.shape[-1] // 2
    first = grad[..., :half]
    second = grad[..., half:]
    return jnp.concatenate(
        [first * cosine_table + second * sine_table, second * cosine_table - first * sine_table],
        axis=-1,
    )


def row_norm(field):
    factor = lax.rsqrt(jnp.mean(field * field, axis=-1, keepdims=True) + EPS)
    return (field * factor, factor)


def norm_backward(grad_hat, normed, factor):
    return factor * (grad_hat - normed * jnp.mean(grad_hat * normed, axis=-1, keepdims=True))


def masked_scores(query_matrix, key_rows, query_places, key_places, softmax_scale):
    score_matrix = (
        jnp.einsum("oblh,wbh->blow", query_matrix, key_rows, preferred_element_type=jnp.float32)
        * softmax_scale
    )
    allowed = key_places[None, :] <= query_places[:, None]
    return (jnp.where(allowed, score_matrix, NEG), allowed)


def per_device(
    layer_input,
    block_pair,
    attn_gain,
    q_weight,
    key_projection,
    value_projection,
    q_gain,
    k_gain,
    o_weight,
    mlp_gain,
    gate_weight,
    up_weight,
    down_weight,
    cotangent,
):
    wide_float_type = jnp.float32
    narrow_float_type = jnp.bfloat16
    tokens = layer_input.shape[0]
    members = lax.axis_size(ROWS)
    seq_len = tokens * members
    block_len = tokens * lax.axis_size(FSDP) // 2
    kv_local = key_projection.shape[1] // HEAD_SIZE
    q_local = q_weight.shape[1] // HEAD_SIZE
    group_size = q_local // kv_local
    softmax_scale = 1.0 / math.sqrt(HEAD_SIZE)
    (
        full_attn_gain,
        full_q,
        full_k,
        full_v,
        full_q_gain,
        full_k_gain,
        full_o,
        full_mlp_gain,
        full_gate,
        full_up,
        full_down,
    ) = (
        lax.all_gather(attn_gain, ROWS, axis=0, tiled=True),
        lax.all_gather(q_weight, ROWS, axis=0, tiled=True),
        lax.all_gather(key_projection, ROWS, axis=0, tiled=True),
        lax.all_gather(value_projection, ROWS, axis=0, tiled=True),
        lax.all_gather(q_gain, ROWS, axis=0, tiled=True),
        lax.all_gather(k_gain, ROWS, axis=0, tiled=True),
        lax.all_gather(o_weight, ROWS, axis=1, tiled=True),
        lax.all_gather(mlp_gain, ROWS, axis=0, tiled=True),
        lax.all_gather(gate_weight, ROWS, axis=0, tiled=True),
        lax.all_gather(up_weight, ROWS, axis=0, tiled=True),
        lax.all_gather(down_weight, ROWS, axis=1, tiled=True),
    )
    own_rows = lax.axis_index(ROWS) * tokens + jnp.arange(tokens, dtype=jnp.int32)
    own_places = row_places(block_pair, own_rows, block_len)
    cosine_table, sine_table = rope_tables(own_places, HEAD_SIZE)
    x_full = layer_input.astype(wide_float_type)
    x_hat, x_scale = row_norm(x_full)
    attn_scale = full_attn_gain.astype(wide_float_type)
    normalized_input = (x_hat * attn_scale).astype(narrow_float_type)
    q_raw = jnp.dot(normalized_input, full_q, preferred_element_type=wide_float_type).reshape(
        tokens, q_local, HEAD_SIZE
    )
    unnormalized_keys = jnp.dot(
        normalized_input, full_k, preferred_element_type=wide_float_type
    ).reshape(tokens, kv_local, HEAD_SIZE)
    value_rows_backward = jnp.dot(
        normalized_input, full_v, preferred_element_type=wide_float_type
    ).astype(narrow_float_type)
    normalized_queries, q_scale = row_norm(q_raw)
    normalized_keys, key_norm_scale = row_norm(unnormalized_keys)
    query_gain_vector = full_q_gain.astype(wide_float_type)
    key_gain_vector = full_k_gain.astype(wide_float_type)
    rotated_queries = apply_rotary(
        normalized_queries * query_gain_vector, cosine_table, sine_table
    ).astype(narrow_float_type)
    grouped_queries = rotated_queries.reshape(tokens, kv_local, group_size, HEAD_SIZE)
    k_flat = (
        apply_rotary(normalized_keys * key_gain_vector, cosine_table, sine_table)
        .astype(narrow_float_type)
        .reshape(tokens, kv_local * HEAD_SIZE)
    )
    start_state = (
        jnp.full((kv_local, group_size, tokens), NEG, wide_float_type),
        jnp.zeros((kv_local, group_size, tokens), wide_float_type),
        jnp.zeros((kv_local, group_size, tokens, HEAD_SIZE), wide_float_type),
    )
    key_piece = lax.all_gather(k_flat, ROWS, axis=0, tiled=True)
    value_piece = lax.all_gather(value_rows_backward, ROWS, axis=0, tiled=True)
    count = key_piece.shape[0]
    width = math.gcd(count, 512)
    steps_here = count // width
    key_blocks = key_piece.reshape(steps_here, width, kv_local, HEAD_SIZE)
    value_blocks = value_piece.reshape(steps_here, width, kv_local, HEAD_SIZE)
    key_places = row_places(block_pair, jnp.arange(count, dtype=jnp.int32), block_len).reshape(
        steps_here, width
    )

    def online(state, blockset):
        top, total, softmax_numerator = state
        key_tile, value_tile, place_blk = blockset
        score_matrix, allowed = masked_scores(
            grouped_queries, key_tile, own_places, place_blk, softmax_scale
        )
        new_top = jnp.maximum(top, jnp.max(score_matrix, axis=-1))
        shrink = jnp.exp(top - new_top)
        weight_set = jnp.where(allowed, jnp.exp(score_matrix - new_top[..., None]), 0.0)
        total = total * shrink + jnp.sum(weight_set, axis=-1)
        softmax_numerator = softmax_numerator * shrink[..., None] + jnp.einsum(
            "nwqf,fny->nwqy",
            weight_set.astype(narrow_float_type),
            value_tile,
            preferred_element_type=wide_float_type,
        )
        return ((new_top, total, softmax_numerator), None)

    result, _ = lax.scan(online, start_state, (key_blocks, value_blocks, key_places))
    top, total, softmax_numerator = result
    log_total = top + jnp.log(total)
    attention_backward = (
        jnp.transpose(softmax_numerator / total[..., None], (2, 0, 1, 3))
        .reshape(tokens, q_local * HEAD_SIZE)
        .astype(narrow_float_type)
    )
    attn_part = jnp.dot(attention_backward, full_o, preferred_element_type=wide_float_type)
    hidden = x_full + lax.psum(attn_part, HEADS)
    mlp_scale = full_mlp_gain.astype(wide_float_type)
    h_hat, h_scale = row_norm(hidden)
    h_normed = (h_hat * mlp_scale).astype(narrow_float_type)
    gate = jnp.dot(h_normed, full_gate, preferred_element_type=wide_float_type)
    up_val = jnp.dot(h_normed, full_up, preferred_element_type=wide_float_type)
    sigma = jax.nn.sigmoid(gate)
    silu = gate * sigma
    act = (silu * up_val).astype(narrow_float_type)
    mlp_part = jnp.dot(act, full_down, preferred_element_type=wide_float_type)
    block_out = (hidden + lax.psum(mlp_part, HEADS)).astype(narrow_float_type)
    (
        full_attn_gain,
        full_q,
        full_k,
        full_v,
        full_q_gain,
        full_k_gain,
        full_o,
        full_mlp_gain,
        full_gate,
        full_up,
        full_down,
    ) = (
        lax.all_gather(attn_gain, ROWS, axis=0, tiled=True),
        lax.all_gather(q_weight, ROWS, axis=0, tiled=True),
        lax.all_gather(key_projection, ROWS, axis=0, tiled=True),
        lax.all_gather(value_projection, ROWS, axis=0, tiled=True),
        lax.all_gather(q_gain, ROWS, axis=0, tiled=True),
        lax.all_gather(k_gain, ROWS, axis=0, tiled=True),
        lax.all_gather(o_weight, ROWS, axis=1, tiled=True),
        lax.all_gather(mlp_gain, ROWS, axis=0, tiled=True),
        lax.all_gather(gate_weight, ROWS, axis=0, tiled=True),
        lax.all_gather(up_weight, ROWS, axis=0, tiled=True),
        lax.all_gather(down_weight, ROWS, axis=1, tiled=True),
    )
    grad_downw = jnp.einsum("tf,td->fd", act, cotangent, preferred_element_type=wide_float_type)
    grad_act = jnp.einsum("td,fd->tf", cotangent, full_down, preferred_element_type=wide_float_type)
    grad_g = (grad_act * up_val * (sigma * (1.0 + gate * (1.0 - sigma)))).astype(narrow_float_type)
    grad_u = (grad_act * silu).astype(narrow_float_type)
    grad_gatew = jnp.einsum("tc,tf->cf", h_normed, grad_g, preferred_element_type=wide_float_type)
    grad_upw = jnp.einsum("tc,tf->cf", h_normed, grad_u, preferred_element_type=wide_float_type)
    normed_part = jnp.einsum(
        "tf,cf->tc", grad_g, full_gate, preferred_element_type=wide_float_type
    ) + jnp.einsum("tf,cf->tc", grad_u, full_up, preferred_element_type=wide_float_type)
    grad_normed = lax.psum(normed_part, HEADS)
    grad_mlp_gain = jnp.sum(grad_normed * h_hat, axis=0)
    grad_h = cotangent.astype(wide_float_type) + norm_backward(
        grad_normed * mlp_scale, h_hat, h_scale
    )
    grad_hb = grad_h.astype(narrow_float_type)
    grad_ow = jnp.einsum(
        "tq,td->qd", attention_backward, grad_hb, preferred_element_type=wide_float_type
    )
    output_gradient_backward = jnp.einsum(
        "td,qd->tq", grad_hb, full_o, preferred_element_type=wide_float_type
    ).astype(narrow_float_type)
    grouped_output_gradient = output_gradient_backward.reshape(
        tokens, kv_local, group_size, HEAD_SIZE
    )
    delta_rows = jnp.sum(
        grouped_output_gradient.astype(wide_float_type)
        * attention_backward.reshape(tokens, kv_local, group_size, HEAD_SIZE).astype(
            wide_float_type
        ),
        axis=-1,
    )
    delta_rows = jnp.transpose(delta_rows, (1, 2, 0))
    keys_all, values_all = (
        lax.all_gather(k_flat, ROWS, axis=0, tiled=True),
        lax.all_gather(value_rows_backward, ROWS, axis=0, tiled=True),
    )
    width = math.gcd(seq_len, 512)
    steps_all = seq_len // width
    all_places = row_places(block_pair, jnp.arange(seq_len, dtype=jnp.int32), block_len).reshape(
        steps_all, width
    )

    def backward_step(grad_q_acc, blockset):
        key_tile, value_tile, place_blk = blockset
        score_matrix, allowed = masked_scores(
            grouped_queries, key_tile, own_places, place_blk, softmax_scale
        )
        probability_rows = jnp.where(allowed, jnp.exp(score_matrix - log_total[..., None]), 0.0)
        grad_v_blk = jnp.einsum(
            "mojp,jmof->pmf",
            probability_rows.astype(narrow_float_type),
            grouped_output_gradient,
            preferred_element_type=wide_float_type,
        )
        probability_gradient = jnp.einsum(
            "oblh,wbh->blow",
            grouped_output_gradient,
            value_tile,
            preferred_element_type=wide_float_type,
        )
        score_gradient = (probability_rows * (probability_gradient - delta_rows[..., None])).astype(
            narrow_float_type
        )
        grad_q_acc = (
            grad_q_acc
            + jnp.einsum(
                "xwzq,qxp->zxwp", score_gradient, key_tile, preferred_element_type=wide_float_type
            )
            * softmax_scale
        )
        grad_k_blk = (
            jnp.einsum(
                "mojp,jmof->pmf",
                score_gradient,
                grouped_queries,
                preferred_element_type=wide_float_type,
            )
            * softmax_scale
        )
        return (grad_q_acc, (grad_k_blk, grad_v_blk))

    rotated_query_gradient, stacked = lax.scan(
        backward_step,
        jnp.zeros((tokens, kv_local, group_size, HEAD_SIZE), wide_float_type),
        (
            keys_all.reshape(steps_all, width, kv_local, HEAD_SIZE),
            values_all.reshape(steps_all, width, kv_local, HEAD_SIZE),
            all_places,
        ),
    )
    grad_k_all = stacked[0].reshape(seq_len, kv_local * HEAD_SIZE)
    grad_v_all = stacked[1].reshape(seq_len, kv_local * HEAD_SIZE)
    grad_k_own, grad_v_own = (
        lax.psum_scatter(grad_k_all, ROWS, scatter_dimension=0, tiled=True),
        lax.psum_scatter(grad_v_all, ROWS, scatter_dimension=0, tiled=True),
    )
    grad_qg = unrotate(
        rotated_query_gradient.reshape(tokens, q_local, HEAD_SIZE), cosine_table, sine_table
    )
    q_gain_part = jnp.sum(grad_qg * normalized_queries, axis=(0, 1))
    query_gradient = (
        norm_backward(grad_qg * query_gain_vector, normalized_queries, q_scale)
        .reshape(tokens, q_local * HEAD_SIZE)
        .astype(narrow_float_type)
    )
    key_gain_gradient = unrotate(
        grad_k_own.reshape(tokens, kv_local, HEAD_SIZE), cosine_table, sine_table
    )
    k_gain_part = jnp.sum(key_gain_gradient * normalized_keys, axis=(0, 1))
    key_gradient = (
        norm_backward(key_gain_gradient * key_gain_vector, normalized_keys, key_norm_scale)
        .reshape(tokens, kv_local * HEAD_SIZE)
        .astype(narrow_float_type)
    )
    value_gradient_backward = grad_v_own.astype(narrow_float_type)
    grad_qw = jnp.einsum(
        "tc,tq->cq", normalized_input, query_gradient, preferred_element_type=wide_float_type
    )
    grad_kw = jnp.einsum(
        "tc,tq->cq", normalized_input, key_gradient, preferred_element_type=wide_float_type
    )
    grad_vw = jnp.einsum(
        "tc,tq->cq",
        normalized_input,
        value_gradient_backward,
        preferred_element_type=wide_float_type,
    )
    xn_part = (
        jnp.einsum("tq,cq->tc", query_gradient, full_q, preferred_element_type=wide_float_type)
        + jnp.einsum("tq,cq->tc", key_gradient, full_k, preferred_element_type=wide_float_type)
        + jnp.einsum(
            "tq,cq->tc", value_gradient_backward, full_v, preferred_element_type=wide_float_type
        )
    )
    grad_xn, grad_q_gain, grad_k_gain = lax.psum((xn_part, q_gain_part, k_gain_part), HEADS)
    grad_attn_gain = jnp.sum(grad_xn * x_hat, axis=0)
    input_grad = grad_h + norm_backward(grad_xn * attn_scale, x_hat, x_scale)
    owned = (
        lax.psum_scatter(grad_attn_gain, ROWS, scatter_dimension=0, tiled=True),
        lax.psum_scatter(grad_qw, ROWS, scatter_dimension=0, tiled=True),
        lax.psum_scatter(grad_kw, ROWS, scatter_dimension=0, tiled=True),
        lax.psum_scatter(grad_vw, ROWS, scatter_dimension=0, tiled=True),
        lax.psum_scatter(grad_q_gain, ROWS, scatter_dimension=0, tiled=True),
        lax.psum_scatter(grad_k_gain, ROWS, scatter_dimension=0, tiled=True),
        lax.psum_scatter(grad_ow, ROWS, scatter_dimension=1, tiled=True),
        lax.psum_scatter(grad_mlp_gain, ROWS, scatter_dimension=0, tiled=True),
        lax.psum_scatter(grad_gatew, ROWS, scatter_dimension=0, tiled=True),
        lax.psum_scatter(grad_upw, ROWS, scatter_dimension=0, tiled=True),
        lax.psum_scatter(grad_downw, ROWS, scatter_dimension=1, tiled=True),
    )
    return (
        block_out,
        input_grad,
        owned[0],
        owned[1],
        owned[2],
        owned[3],
        owned[4],
        owned[5],
        owned[6],
        owned[7],
        owned[8],
        owned[9],
        owned[10],
    )


MESH = pl.DeviceIdType.MESH
HBM = pl.BlockSpec(memory_space=pltpu.HBM)
VM = pl.BlockSpec(memory_space=pltpu.VMEM)
SLOTS = 258
LOCAL_SLOTS = 18
NT = (((1,), (1,)), ((), ()))
TN = (((0,), (0,)), ((), ()))
BF = jnp.bfloat16
F32 = jnp.float32


class Net:
    def __init__(self, shards, send, recv, loc):
        self.C = shards
        self.send, self.recv, self.loc = send, recv, loc
        self.used = self.used_local = 0
        self.c, f, self.y = (lax.axis_index(a) for a in (CONTEXT, FSDP, HEADS))
        self.x, self.k = f // 2, f % 2

    def at(self, c=None, x=None, k=None, y=None):
        c, x, k, y = (own if v is None else v for v, own in ((c, self.c), (x, self.x), (k, self.k), (y, self.y)))
        return (c, 2 * x + k, y)

    def core(self):
        return self.at(k=1 - self.k)

    def over_x(self):
        return self.at(x=1 - self.x)

    def over_y(self):
        return self.at(y=1 - self.y)

    def shard(self, step):
        return lax.rem(self.c + step + self.C, self.C)

    def slots(self, count):
        self.used += count
        assert self.used <= SLOTS
        return self.used - count

    def again(self, start, part):
        top, self.used = self.used, start
        next(part)
        self.used = max(top, self.used)

    def slot(self):
        return self.slots(1)

    def remote(self, src, dst, slot, to):
        return pltpu.make_async_remote_copy(
            src_ref=src, dst_ref=dst, send_sem=self.send.at[slot], recv_sem=self.recv.at[slot],
            device_id=to, device_id_type=MESH,
        )

    def local(self, src, dst):
        self.used_local += 1
        assert self.used_local <= LOCAL_SLOTS
        return pltpu.make_async_copy(src, dst, self.loc.at[self.used_local - 1])

    def meet(self, devices):
        barrier = pltpu.get_barrier_semaphore()
        for to in devices:
            pl.semaphore_signal(barrier, inc=1, device_id=to, device_id_type=MESH)
        pl.semaphore_wait(barrier, len(devices))

    def group(self):
        return [
            self.at(c=self.shard(dc), k=(self.k + dk) % 2)
            for dc in range(self.C) for dk in range(2) if (dc, dk) != (0, 0)
        ]


def run(*parts):
    live = list(parts)
    while live:
        live = [p for p in live if next(p, 0) != 0]


def gather_rows(net, src, dst, half, done=None):
    C, c, k, y = net.C, net.c, net.k, net.y
    H = dst.shape[-1] // 2
    mine = pl.ds(pl.multiple_of(y * H, 128), H)
    other = pl.ds(pl.multiple_of((1 - y) * H, 128), H)
    own_cols = mine if half else pl.ds(0, 2 * H)
    own_half = src if half else src.at[:, mine]
    right, left = net.at(c=c + 1), net.at(c=c - 1)
    core, over_y = net.core(), net.over_y()
    keep = net.local(src, dst.at[k, c, :, own_cols])
    keep.start()
    done = done or (lambda kk, q: None)
    hops = [(d, s) for s in range(1, C) for d in (0, 1)]
    zslot = {h: net.slot() for h in hops}
    yslot = {h: net.slot() for h in hops}
    aslot = {h: net.slot() for h in hops}
    bslot = {h: net.slot() for h in hops}
    own_core, own_y, own_core2 = net.slot(), net.slot(), net.slot()
    no_right, no_left = c < C - 1, c > 0

    def chunk(d, s):
        return (c - s, c - s >= 0) if d == 0 else (c + s, c + s < C)

    def z_send(d, s, source, q):
        to = right if d == 0 else left
        return net.remote(source, dst.at[k, q, :, mine], zslot[d, s], to)

    @pl.when(no_right)
    def _():
        z_send(0, 1, own_half, c).start()

    @pl.when(no_left)
    def _():
        z_send(1, 1, own_half, c).start()

    to_core = net.remote(src, dst.at[k, c, :, own_cols], own_core, core)
    to_core.start()
    if half:
        to_y = net.remote(src, dst.at[k, c, :, mine], own_y, over_y)
        to_y.start()
    yield 1
    for d, s in hops:
        q, valid = chunk(d, s)

        @pl.when(valid)
        def _(d=d, s=s, q=q):
            piece = dst.at[k, q, :, mine]
            z_send(d, s, piece, q).wait_recv()
            if s < C - 1:
                @pl.when(no_right if d == 0 else no_left)
                def _():
                    z_send(d, s + 1, piece, q).start()
            net.remote(piece, piece, yslot[d, s], over_y).start()
            net.remote(piece, piece, aslot[d, s], core).start()
        yield 1
    if half:
        piece = dst.at[k, c, :, other]
        net.remote(piece, piece, own_y, over_y).wait_recv()
        net.remote(piece, piece, own_core2, core).start()
    for d, s in hops:
        q, valid = chunk(d, s)

        @pl.when(valid)
        def _(d=d, s=s, q=q):
            piece = dst.at[k, q, :, other]
            net.remote(piece, piece, yslot[d, s], over_y).wait_recv()
            net.remote(piece, piece, bslot[d, s], core).start()
            done(k, q)
        yield 1
    keep.wait()
    done(k, c)
    to_core_in = net.remote(src, dst.at[1 - k, c, :, own_cols], own_core, core)
    to_core_in.wait_recv()
    done(1 - k, c)
    to_core_in.wait_send()
    if half:
        piece = dst.at[1 - k, c, :, other]
        net.remote(piece, piece, own_core2, core).wait()
        to_y.wait_send()
    for d, s in hops:
        q, valid = chunk(d, s)

        @pl.when(valid)
        def _(d=d, s=s, q=q):
            a, b = dst.at[1 - k, q, :, mine], dst.at[1 - k, q, :, other]
            net.remote(a, a, aslot[d, s], core).wait()
            net.remote(b, b, bslot[d, s], core).wait()
            done(1 - k, q)
            net.remote(a, a, yslot[d, s], over_y).wait_send()

        sent = jnp.logical_and(no_right if d == 0 else no_left, chunk(d, s - 1)[1])

        @pl.when(sent)
        def _(d=d, s=s):
            piece = dst.at[k, c, :, mine]
            z_send(d, s, piece, c).wait_send()
    yield 1


class Hand:
    def __init__(self, net, groups):
        self.net, self.groups = net, groups
        self.steps = [(dc, dk) for dc in range(net.C) for dk in range(2)]
        self.steps = self.steps[1:] + self.steps[:1]
        self.zs = {(g, s): net.slot() for s in self.steps for g in range(len(groups))}
        self.xs = {(g, s): net.slot() for s in self.steps for g in range(len(groups))}
        self.keeps = []
        self.posted = self.relayed = 0

    def post(self, count):
        net = self.net
        mine = net.c * 4 + 2 * net.x + net.k
        for s in self.steps[self.posted:self.posted + count]:
            tc, tk = net.shard(s[0]), (net.k + s[1]) % 2
            for g, (pieces, whole) in enumerate(self.groups):
                for src, pick, put in pieces:
                    if s == (0, 0):
                        net.remote(src.at[pick(tc, tk)], put(mine), self.xs[g, s], net.over_x()).start()
                        keep = net.local(src.at[pick(tc, tk)], put(mine))
                        keep.start()
                        self.keeps.append(keep)
                    else:
                        net.remote(src.at[pick(tc, tk)], put(mine), self.zs[g, s], net.at(c=tc, k=tk)).start()
        self.posted += count

    def block(self, g, s, x):
        net = self.net
        return self.groups[g][1](net.shard(-s[0]) * 4 + 2 * x + (net.k + s[1]) % 2)

    def relay(self, count):
        net = self.net
        for s in self.steps[self.relayed:min(self.relayed + count, len(self.steps) - 1)]:
            for g in range(len(self.groups)):
                block = self.block(g, s, net.x)
                net.remote(block, block, self.zs[g, s], net.over_x()).wait_recv()
                net.remote(block, block, self.xs[g, s], net.over_x()).start()
        self.relayed += count

    def finish(self):
        net = self.net
        for s in self.steps:
            for g in range(len(self.groups)):
                block = self.block(g, s, 1 - net.x)
                net.remote(block, block, self.xs[g, s], net.over_x()).wait()
                if s != (0, 0):
                    net.remote(block, block, self.zs[g, s], net.over_x()).wait_send()
        for keep in self.keeps:
            keep.wait()


class Columns:
    def __init__(self, ref, first, width):
        self.ref, self.first, self.width = ref, first, width
        self.at = self

    def lanes(self, j):
        return pl.ds(pl.multiple_of((self.first + j) * self.width, 128), self.width)

    def __getitem__(self, j):
        return Slot(self.ref, self.lanes(j))

    def __setitem__(self, j, value):
        self.ref[:, :, self.lanes(j)] = value


def Slot(ref, lanes):
    return ref.at[:, :, lanes]


def reduce_scratch(C, rows, width, tiles, wire):
    w = width // tiles
    n = tiles // 2
    return [
        pltpu.VMEM((2, C, rows, w), wire),
        pltpu.VMEM((tiles, C, rows, w), wire),
        pltpu.VMEM((n, C, rows, w), BF),
        pltpu.VMEM((n, C, rows, w), BF),
        pltpu.VMEM((n, C, rows, w), F32),
        pltpu.VMEM((n, C - 1, rows, w), BF),
        pltpu.VMEM((n, C - 1, rows, w), BF),
        pltpu.VMEM((n, rows, w), BF),
    ]


def reduce_rows(net, product, scratch, out):
    osend, orecv, ysend, yrecv, sums, zsend, zrecv, joined = scratch
    n, C, rows, w = zsend.shape
    tiles, C = 2 * n, C + 1
    c, k, y = net.c, net.k, net.y
    core, over_y = net.core(), net.over_y()
    depth = osend.shape[0]
    cslot, yslot, jslot, zslot = net.slots(tiles), net.slots(n), net.slots(n), net.slots(n * (C - 1))

    def to_core(j):
        return net.remote(osend.at[j % depth], orecv.at[j], cslot + j, core)

    def to_y(j):
        return net.remote(ysend.at[j], yrecv.at[j], yslot + j, over_y)

    def column(j):
        return (j // n + 1 + y) % 2 * n + j % n

    def step(j, _):
        @pl.when(j < tiles)
        def _():
            @pl.when(j >= depth)
            def _():
                to_core(j - depth).wait_send()

            osend[j % depth] = product(1 - k, column(j)).astype(osend.dtype).reshape(C, rows, w)
            to_core(j).start()

        @pl.when(j > 0)
        def _():
            i = j - 1
            own = product(k, column(i)).reshape(C, rows, w)
            to_core(i).wait_recv()
            own = own + orecv.at[i][...].astype(F32)

            @pl.when(i < n)
            def _():
                ysend[i % n] = own.astype(BF)
                to_y(i % n).start()

            @pl.when(i >= n)
            def _():
                sums[i % n] = own

        return 0

    lax.fori_loop(0, tiles + 1, step, 0)
    yield 1
    low, high = c == 0, c == C - 1
    inner = jnp.logical_and(c > 0, c < C - 1)
    beside = net.at(c=jnp.where(low, 1, C - 2))

    def z(j, dc):
        return net.remote(zsend.at[j, dc - 1], zrecv.at[j, dc - 1], zslot + j * (C - 1) + dc - 1, net.at(c=net.shard(dc)))

    def join(j, dc):
        return net.remote(zsend.at[j, dc - 1], joined.at[j], jslot + j, beside)

    def through(j):
        zsend[j, 1] = sums[j, net.shard(2)].astype(BF)

        @pl.when(inner)
        def _():
            join(j, 2).wait_recv()
            zsend[j, 1] = (sums[j, net.shard(2)] + joined[j].astype(F32)).astype(BF)

        z(j, 2).start()

    ends = ((1, high), (C - 1, low))
    for j in range(n):
        to_y(j).wait_recv()
        sums[j] = sums[j] + yrecv.at[j][...].astype(F32)
        for dc, far in ends:
            zsend[j, dc - 1] = sums[j, net.shard(dc)].astype(BF)

            @pl.when(far)
            def _(dc=dc):
                join(j, dc).start()

            @pl.when(jnp.logical_not(far))
            def _(dc=dc):
                z(j, dc).start()

        if j:
            through(j - 1)
        if j == n - 1:
            through(j)
        yield 1
    for j in range(n):
        z(j, 2).wait_recv()
        out[j] = sums[j, c] + zrecv[j, 1].astype(F32)
        for dc, absent in ((1, low), (C - 1, high)):
            @pl.when(jnp.logical_not(absent))
            def _(dc=dc):
                z(j, dc).wait_recv()
                out[j] = out[j] + zrecv[j, dc - 1].astype(F32)
        yield 1
    for j in range(n):
        if j < depth:
            to_core(tiles - depth + j).wait_send()
        to_y(j).wait_send()
        z(j, 2).wait_send()
        for dc, far in ends:
            @pl.when(far)
            def _(dc=dc):
                join(j, dc).wait_send()

            @pl.when(jnp.logical_not(far))
            def _(dc=dc):
                z(j, dc).wait_send()
    yield 1


def half_of(ref, y, width):
    return ref[:, pl.ds(pl.multiple_of(y * width, 128), width)]


def gain_half(gains, y, row, blocks):
    return [gains[y * blocks + i].astype(F32)[row:row + 1] for i in range(blocks)]


def times_gain(value, rows):
    w = value.shape[1] // len(rows)
    return jnp.concatenate([value[:, i * w:(i + 1) * w] * r for i, r in enumerate(rows)], axis=1)


def swap_sums(net, part, out_buf, in_buf):
    out_buf[...] = jnp.broadcast_to(part, out_buf.shape)
    cp = net.remote(out_buf, in_buf, net.slot(), net.over_y())
    cp.start()
    cp.wait()
    return part + in_buf[:, 0:1]


def rotate(value, cosine, sine):
    return value * cosine + pltpu.roll(value, value.shape[1] // 2, 1) * sine


def steps_of(part, count):
    for _ in range(count):
        if next(part, 0) == 0:
            return


def layer_kernel(C, tiles, head, scale, tile, few, x_ref, a_gain, m_gain, few_gains, cot, freq, pair, wq, wk, wv, wo, wg, wu, wd,
                 xg_out, g_out, u_out, d_out, blk, ig, sums_out, q_grad, kv_grad, o_grad,
                 g_ref, gains, h_out, gh_out, zgu, zd, mine, act, wdd, xg, ht, ct, wgu, m_s, l_s, acc, red, rs, hn, gb, stats,
                 ggu, ggu_t, act_t, from_x, delta, own, peer, cin, xin, xq, zq, xo, zo, vec, vin, vx, vz, red_x, rs_x,
                 send, recv, loc):
    qp, kp, cosine, sine, wqkv, wod, raw, q_out, kv, kvp, o_out, lse = mine
    net = Net(C, send, recv, loc)
    c, x, y, k = net.c, net.x, net.y, net.k
    B, unit = wg.shape[0], wdd.shape[0]
    R, D = x_ref.shape
    H = D // 2
    T = 2 * C * R
    w = D // tiles
    blocks = gains.shape[0]
    plane = [(dc, dx, dk) for dc in range(C) for dx in range(2) for dk in range(2)][1:]
    mates = [net.at(c=net.shard(dc), x=(x + dx) % 2, k=(k + dk) % 2) for dc, dx, dk in plane]
    net.meet(mates + [net.over_y()])
    me = c * 4 + 2 * x + k
    g_ref[...] = jnp.concatenate(
        [a_gain[...].astype(F32), m_gain[...].astype(F32), pltpu.roll(few_gains[...], me * few, 1)[0:2],
         jnp.zeros((12, B), F32)], axis=0).astype(BF)
    sent = []
    for to in mates:
        cp = net.remote(g_ref, gains.at[me], net.slot(), to)
        cp.start()
        sent.append(cp)
    own_gains = net.local(g_ref, gains.at[me])
    own_gains.start()
    full = slice(None)
    lanes = lambda n, m: pl.ds(pl.multiple_of(n * m, 128), m)
    rows = lambda b: pl.ds(pl.multiple_of(b * B, B), B)
    part = lambda tc, tk, m: pl.ds(pl.multiple_of((2 * tc + tk) * m, 128), m)
    g_qkv = (
        [(wq, lambda tc, tk: (full, part(tc, tk, head)), lambda b: wqkv.at[rows(b), pl.ds(0, head)]),
         (wk, lambda tc, tk: (full, lanes(tc, head)), lambda b: wqkv.at[rows(b), pl.ds(head, head)]),
         (wv, lambda tc, tk: (full, lanes(tc, head)), lambda b: wqkv.at[rows(b), pl.ds(2 * head, head)])],
        lambda b: wqkv.at[rows(b), :])
    g_o = ([(wo, lambda tc, tk: (part(tc, tk, head), full), lambda b: wod.at[:, lanes(b, B)])],
           lambda b: wod.at[:, lanes(b, B)])
    g_gu = (
        [(wg, lambda tc, tk: (full, part(tc, tk, unit)), lambda b: wgu.at[rows(b), pl.ds(0, unit)]),
         (wu, lambda tc, tk: (full, part(tc, tk, unit)), lambda b: wgu.at[rows(b), pl.ds(unit, unit)])],
        lambda b: wgu.at[rows(b), :])
    g_d = ([(wd, lambda tc, tk: (part(tc, tk, unit), full), lambda b: wdd.at[:, lanes(b, B)])],
           lambda b: wdd.at[:, lanes(b, B)])
    h_qkv, h_o, h_mlp = Hand(net, [g_qkv]), Hand(net, [g_o]), Hand(net, [g_gu, g_d])
    every = 2 * C

    def normalise(kk, q):
        value = ht[kk, q].astype(F32)
        hat = value * lax.rsqrt(jnp.mean(value * value, axis=-1, keepdims=True) + EPS)
        for b in range(blocks):
            t = pl.ds(b * B, B)
            xg[kk, q, :, t] = (hat[:, b * B:(b + 1) * B] * gains[b].astype(F32)[0:1]).astype(BF)

    rows_x = gather_rows(net, x_ref, ht, False, normalise)
    row_slots = net.used
    next(rows_x)
    h_qkv.post(2)
    for kk in range(2):
        for q in range(C):
            base = jnp.where(x == 0, pair[q], 2 * C - 1 - pair[q]) * (2 * R) + kk * R
            r = pl.ds((kk * C + q) * R, R)
            spot = lax.broadcasted_iota(jnp.int32, (R, 128), 0) + base
            qp[r] = spot
            kp[:, r] = lax.broadcasted_iota(jnp.int32, (8, R), 1) + base
            angle = spot.astype(F32) * freq[0:1]
            sign = jnp.where(lax.broadcasted_iota(jnp.int32, (R, 128), 1) < head // 2, -1.0, 1.0)
            cosine[r] = jnp.cos(angle)
            sine[r] = jnp.sin(angle) * sign

    for _ in range(C - 1):
        steps_of(rows_x, 2)
        h_qkv.post(2)
        h_qkv.relay(2)
    own_gains.wait()
    for cp in sent:
        cp.wait()
    h_qkv.relay(1)
    run(rows_x)
    h_qkv.finish()
    h_o.post(every)
    h_mlp.post(every - 1)
    keep = net.local(xg, xg_out)
    keep.start()
    per = tile // R
    gain_sum = jnp.sum(gains[...].astype(F32), axis=0)
    qg, kg = gain_sum[2:3], gain_sum[3:4]
    for kk in range(2):
        def project(i, _, kk=kk):
            r = pl.ds(pl.multiple_of(kk * C * R + i * tile, tile), tile)
            v = jnp.dot(xg[kk, pl.ds(i * per, per)].reshape(tile, D), wqkv[...], preferred_element_type=F32)
            raw[r] = v[:, :2 * head]
            cs, sn = cosine[r], sine[r]
            q = v[:, :head]
            q = q * lax.rsqrt(jnp.mean(q * q, axis=-1, keepdims=True) + EPS)
            q_out[r] = rotate(q * qg, cs, sn).astype(BF)
            key = v[:, head:2 * head]
            key = key * lax.rsqrt(jnp.mean(key * key, axis=-1, keepdims=True) + EPS)
            kv[r, 0:head] = rotate(key * kg, cs, sn).astype(BF)
            kv[r, head:2 * head] = v[:, 2 * head:].astype(BF)
            return 0

        lax.fori_loop(0, C * R // tile, project, 0)
    swap = net.remote(kv, kvp, net.slot(), net.over_x())
    swap.start()
    h_mlp.post(1)

    def attend(i, _):
        r = pl.ds(pl.multiple_of(i * tile, tile), tile)
        s = lax.dot_general(q_out[r], kv[:, :head], NT, preferred_element_type=F32) * scale
        s = jnp.where(kp[0:1] <= qp[r, 0:1], s, NEG)
        top = jnp.max(s, axis=-1, keepdims=True)
        e = jnp.exp(s - top)
        m_s[r] = jnp.broadcast_to(top, (tile, 128))
        l_s[r] = jnp.broadcast_to(jnp.sum(e, axis=-1, keepdims=True), (tile, 128))
        acc[r] = jnp.dot(e.astype(BF), kv[:, head:], preferred_element_type=F32)
        return 0

    def attend_more(i, _):
        r = pl.ds(pl.multiple_of(i * tile, tile), tile)
        s = lax.dot_general(q_out[r], kvp[:, :head], NT, preferred_element_type=F32) * scale
        old = m_s[r, 0:1]
        top = jnp.maximum(old, jnp.max(s, axis=-1, keepdims=True))
        e = jnp.exp(s - top)
        shrink = jnp.exp(old - top)
        m_s[r] = jnp.broadcast_to(top, (tile, 128))
        l_s[r] = jnp.broadcast_to(l_s[r, 0:1] * shrink + jnp.sum(e, axis=-1, keepdims=True), (tile, 128))
        acc[r] = acc[r] * shrink + jnp.dot(e.astype(BF), kvp[:, head:], preferred_element_type=F32)
        return 0

    steps = T // tile
    lax.fori_loop(0, steps, attend, 0)
    h_o.relay(every - 1)
    swap.wait()

    @pl.when(x == 1)
    def _():
        lax.fori_loop(0, steps, attend_more, 0)

    o_out[...] = (acc[...] / l_s[...]).astype(BF)
    for i in range(steps):
        r = pl.ds(i * tile, tile)
        lse[:, r] = (m_s[r] + jnp.log(l_s[r])).T[0:8]
    h_o.finish()

    def product(kk, t):
        return jnp.dot(o_out[pl.ds(pl.multiple_of(kk * C * R, C * R), C * R)], wod[:, lanes(t, w)],
                       preferred_element_type=F32)

    reduce = reduce_rows(net, product, red, rs)
    sum_slots = net.used
    next(reduce)
    h_mlp.relay(2)
    for _ in range(tiles // 2):
        steps_of(reduce, 1)
        h_mlp.relay(1)
    cots = gather_rows(net, cot, ct, False)
    next(cots)
    h_mlp.relay(every - 3 - tiles // 2)
    run(reduce)
    half = half_of(x_ref, y, H).astype(F32) + jnp.concatenate([rs[j] for j in range(tiles // 2)], axis=1)
    total = swap_sums(net, jnp.sum(half * half, axis=-1, keepdims=True), stats.at[0], stats.at[1])
    hs = lax.rsqrt(total / D + EPS)
    h_out[...] = half
    hn[...] = times_gain(half * hs, gain_half(gains, y, 1, blocks // 2)).astype(BF)
    rows_h = gather_rows(net, hn, ht, True)
    net.again(row_slots, rows_h)
    run(cots, rows_h)
    h_mlp.finish()

    for kk in range(2):
        def swiglu(i, _, kk=kk):
            rr = pl.ds(pl.multiple_of(i * tile, tile), tile)
            r = pl.ds(pl.multiple_of(kk * C * R + i * tile, tile), tile)
            gu = jnp.dot(ht[kk, pl.ds(i * per, per)].reshape(tile, D), wgu[...], preferred_element_type=F32)
            ga = lax.dot_general(ct[kk, pl.ds(i * per, per)].reshape(tile, D), wdd[...], NT,
                                 preferred_element_type=F32)
            gate, up = gu[:, :unit], gu[:, unit:]
            sigma = jax.nn.sigmoid(gate)
            silu = gate * sigma
            a = (silu * up).astype(BF)
            act[kk, rr] = a
            act_t[:, r] = a.T
            gg = (ga * up * (sigma * (1.0 + gate * (1.0 - sigma)))).astype(BF)
            gu = (ga * silu).astype(BF)
            ggu[kk, rr, 0:unit] = gg
            ggu[kk, rr, unit:2 * unit] = gu
            ggu_t[0:unit, r] = gg.T
            ggu_t[unit:2 * unit, r] = gu.T
            return 0

        lax.fori_loop(0, C * R // tile, swiglu, 0)

    def normed(kk, t):
        return lax.dot_general(ggu[kk], wgu[lanes(t, w), :], NT, preferred_element_type=F32)

    pair = 2 * B

    def weight_grads(block, out):
        t = lanes(block, pair)
        out(0, 2 * unit, jnp.dot(ggu_t[...], ht[:, :, :, t].reshape(T, pair), preferred_element_type=F32))
        out(2 * unit, 3 * unit, jnp.dot(act_t[...], ct[:, :, :, t].reshape(T, pair), preferred_element_type=F32))

    swaps = []

    def to_x(q):
        if q < C - 1:
            return wgu.at[pl.ds(0, 2 * unit), pl.ds(q * pair, pair)], wgu.at[pl.ds(2 * unit, unit), pl.ds(q * pair, pair)]
        return wgu.at[pl.ds(3 * unit, 2 * unit), pl.ds(0, pair)], wgu.at[pl.ds(3 * unit, unit), pl.ds(pair, pair)]

    def send_partial(q):
        def out(a, b, v):
            to_x(q)[a // (2 * unit)][...] = v.astype(BF)

        weight_grads(net.shard(q + 1) * 2 + 1 - x, out)
        pieces = pl.ds(0, 2 * unit), pl.ds(2 * unit, unit)
        swaps.append([net.remote(a, from_x.at[q, r], net.slot(), net.over_x()) for a, r in zip(to_x(q), pieces)])
        for cp in swaps[q]:
            cp.start()

    place = lambda a, b, m: pl.ds(pl.multiple_of((2 * a + b) * m, 128), m)

    def add_partial(q):
        dc = (q + 1) % C
        for cp in swaps[q]:
            cp.wait_recv()

        def out(a, b, v):
            v = v + from_x[q, a:b].astype(F32)
            for kk in range(2):
                part = v[:, kk * B:(kk + 1) * B]
                dk = lax.rem(kk + k, 2)
                if a:
                    zd[2 * dc + dk] = part.astype(BF)
                else:
                    zgu[2 * dc + dk] = part.T.astype(BF)

        weight_grads(net.shard(dc) * 2 + x, out)

    keep.wait()
    hand_out = Deal(net, swiglu_groups(g_out, u_out, d_out, zgu, zd, unit))
    reduce = reduce_rows(net, normed, red, rs)
    net.again(sum_slots, reduce)
    for q in range(C):
        send_partial(q)
        steps_of(reduce, tiles // 2 // C)
    run(reduce)
    g = jnp.concatenate([rs[j] for j in range(tiles // 2)], axis=1)
    hat = half * hs
    col = jnp.sum(g * hat, axis=0, keepdims=True)
    n = vec.shape[2]
    count = H // n
    vec[0] = jnp.zeros(vec.shape[1:], F32)
    for i in range(count):
        vec[0, count + i:count + i + 1] = col[:, i * n:(i + 1) * n]
    m = times_gain(g, gain_half(gains, y, 1, blocks // 2))
    mean = swap_sums(net, jnp.sum(m * hat, axis=-1, keepdims=True), stats.at[2], stats.at[3]) / D
    gh = half_of(cot, y, H).astype(F32) + hs * (m - hat * mean)
    gh_out[...] = gh
    gb[...] = gh.astype(BF)
    rows_g = gather_rows(net, gb, xg, True)
    net.again(row_slots, rows_g)
    add_partial(0)
    steps_of(rows_g, 2)
    add_partial(1)
    steps_of(rows_g, 4)
    add_partial(2)
    run(rows_g)
    hand_out.post(6)

    def rows_of(i):
        return pl.ds(pl.multiple_of(i * tile, tile), tile)

    def grad_o(i, _):
        r = rows_of(i)
        per = tile // R
        g = lax.dot_general(xg[i // (steps // 2), pl.ds((i % (steps // 2)) * per, per)].reshape(tile, D), wod[...], NT,
                            preferred_element_type=F32).astype(BF)
        ggu[i // (steps // 2), pl.ds(pl.multiple_of(i % (steps // 2) * tile, tile), tile), pl.ds(2 * head, head)] = g
        d = jnp.sum(g.astype(F32) * o_out[r].astype(F32), axis=-1, keepdims=True)
        delta[:, r] = jnp.broadcast_to(d, (tile, 128)).T[0:8]
        return 0

    lax.fori_loop(0, steps, grad_o, 0)
    add_partial(C - 1)
    hand_out.post(2)
    keeps = [net.local(zgu.at[0, :, pl.ds(0, unit)], g_out.at[:, place(c, k, unit)]),
             net.local(zgu.at[0, :, pl.ds(unit, unit)], u_out.at[:, place(c, k, unit)]),
             net.local(zd.at[0], d_out.at[place(c, k, unit), :])]
    load_x = net.local(xg_out, ct)
    for cp in keeps + [load_x]:
        cp.start()
    for copies in swaps:
        for cp in copies:
            cp.wait_send()
    acc[...] = jnp.zeros_like(acc)
    own[...] = jnp.zeros_like(own)

    def sweep(keys, grads, masked):
        def step(i, _):
            r = rows_of(i)
            q = q_out[r]
            g = ggu[i // (steps // 2), pl.ds(pl.multiple_of(i % (steps // 2) * tile, tile), tile), pl.ds(2 * head, head)]
            s = lax.dot_general(keys[:, :head], q, NT, preferred_element_type=F32) * scale
            p = jnp.exp(s - lse[0:1, r])
            if masked:
                p = jnp.where(qp[:, 0:1] <= kp[0:1, r], p, 0.0)
            grads[1] += jnp.dot(p.astype(BF), g, preferred_element_type=F32)
            dp = lax.dot_general(keys[:, head:], g, NT, preferred_element_type=F32)
            ds = (p * (dp - delta[0:1, r])).astype(BF)
            grads[0] += jnp.dot(ds, q, preferred_element_type=F32)
            acc[r] += lax.dot_general(ds, keys[:, :head], TN, preferred_element_type=F32)
            return 0

        lax.fori_loop(0, steps, step, 0)

    one = net.remote(peer.at[1 - k], cin.at[0], net.slot(), net.core())
    two = net.remote(l_s, xin, net.slot(), net.over_x())
    three = net.remote(own.at[1 - k], cin.at[1], net.slot(), net.core())

    @pl.when(x == 1)
    def _():
        peer[...] = jnp.zeros_like(peer)
        sweep(kvp, peer, False)
        one.start()
        one.wait()
        l_s[...] = peer[k] + cin[0]
        two.start()

    sweep(kv, own, True)
    three.start()

    def down(kk, t):
        return jnp.dot(act[kk], wdd[:, lanes(t, w)], preferred_element_type=F32)

    reduce_d = reduce_rows(net, down, red, rs)
    net.again(sum_slots, reduce_d)

    def back_norm(grad, value, gain, r):
        rotated = grad * cosine[r] - pltpu.roll(grad, head // 2, 1) * sine[r]
        factor = lax.rsqrt(jnp.mean(value * value, axis=-1, keepdims=True) + EPS)
        hat = value * factor
        m = rotated * gain
        result = factor * (m - hat * jnp.mean(m * hat, axis=-1, keepdims=True))
        return result, jnp.sum(rotated * hat, axis=0, keepdims=True)

    def finish_q(i, total):
        r = rows_of(i)
        g, col = back_norm(acc[r] * scale, raw[r, 0:head], qg, r)
        ggu[i // (steps // 2), pl.ds(pl.multiple_of(i % (steps // 2) * tile, tile), tile), pl.ds(0, head)] = g.astype(BF)
        return total + col

    vec[0, 2 * count:2 * count + 1] = lax.fori_loop(0, steps, finish_q, jnp.zeros((1, head), F32))
    def keep_o(v):
        o_grad[place(c, k, head), :] = v.astype(BF)

    deal_o = Deal(net, [
        (from_x, lambda b: (2, pl.ds(pl.multiple_of(b // 2 * head, head), head), lanes(b % 2, B)), xo, zo,
         [((full, full), lambda a, b: o_grad.at[place(a, b, head), :])], keep_o, False),
    ])
    for i in range(tiles):
        from_x[2, pl.ds(i * head, head), :] = lax.dot_general(
            o_out[...], xg[:, :, :, pl.ds(i * w, w)].reshape(T, w), TN, preferred_element_type=F32).astype(BF)
    three.wait()
    m_s[...] = own[k] + cin[1]

    @pl.when(x == 1)
    def _():
        two.wait_send()

    @pl.when(x == 0)
    def _():
        two.wait_recv()
        m_s[...] = m_s[...] + xin[...]

    def finish_kv(i, total):
        r = rows_of(i)
        v = m_s[r]
        g, col = back_norm(v * scale, raw[r, head:2 * head], kg, r)
        ggu[i // (steps // 2), pl.ds(pl.multiple_of(i % (steps // 2) * tile, tile), tile), pl.ds(head, head)] = jnp.where(k == 0, g, v).astype(BF)
        return total + jnp.where(k == 0, col, 0.0)

    deal_o.start()
    vec[0, 2 * count + 1:2 * count + 2] = lax.fori_loop(0, steps, finish_kv, jnp.zeros((1, head), F32))

    def product(kk, t):
        a = lax.dot_general(ggu[kk, :, 0:head], wqkv[lanes(t, w), 0:head], NT, preferred_element_type=F32)
        return a + lax.dot_general(ggu[kk, :, head:2 * head], wqkv[lanes(t, w), lanes(1 + k, head)], NT,
                                   preferred_element_type=F32)

    def keep_q(v):
        q_grad[:, place(c, k, head)] = v[:, :head].astype(BF)
        kv_grad[k, :, lanes(c, head)] = v[:, head:].astype(BF)

    deal_q = Deal(net, [
        (from_x, lambda b: (b // 8, pl.ds(pl.multiple_of(b // 2 % 4 * (2 * head), 2 * head), 2 * head), lanes(b % 2, B)), xq, zq,
         [((full, pl.ds(0, head)), lambda a, b: q_grad.at[:, place(a, b, head)]),
          ((full, pl.ds(head, head)), lambda a, b: kv_grad.at[b, :, lanes(a, head)])], keep_q, True),
    ])
    steps_of(reduce_d, 1)
    reduce = reduce_rows(net, product, red_x, rs_x)
    load_x.wait()
    next(reduce)
    for i in range(tiles):
        t = pl.ds(i * w, w)
        from_x[i // 4, pl.ds(i % 4 * 2 * head, 2 * head), :] = lax.dot_general(
            ggu[:, :, 0:2 * head].reshape(T, 2 * head), ct[:, :, :, t].reshape(T, w), TN,
            preferred_element_type=F32).astype(BF)
    deal_q.start()
    steps_of(reduce, 1)
    for _ in range(tiles // 2 - 1):
        steps_of(reduce_d, 1)
        steps_of(reduce, 1)
    deal_o.both(2 * C)
    deal_q.both(2 * C)
    run(reduce_d)
    blk[y] = (h_out[...] + jnp.concatenate([rs[j] for j in range(tiles // 2)], axis=1)).astype(BF)
    swap_b = net.remote(blk.at[y], blk.at[y], net.slot(), net.over_y())
    swap_b.start()
    run(reduce)
    value = x_ref[...].astype(F32)
    xscale = lax.rsqrt(jnp.mean(value * value, axis=-1, keepdims=True) + EPS)
    hat = half_of(x_ref, y, H).astype(F32) * xscale
    g = jnp.concatenate([rs_x[j] for j in range(tiles // 2)], axis=1)
    col = jnp.sum(g * hat, axis=0, keepdims=True)
    for i in range(count):
        vec[0, i:i + 1] = col[:, i * n:(i + 1) * n]
    first = net.remote(vec.at[0], vin, net.slot(), net.core())
    first.start()
    m = times_gain(g, gain_half(gains, y, 0, blocks // 2))
    mean = swap_sums(net, jnp.sum(m * hat, axis=-1, keepdims=True), stats.at[4], stats.at[5]) / D
    ig[y] = (gh_out[...] + xscale * (m - hat * mean)).astype(BF)
    swap = net.remote(ig.at[y], ig.at[y], net.slot(), net.over_y())
    swap.start()
    first.wait()
    vec[1] = vec[0] + vin[...]
    second = net.remote(vec.at[1], vx, net.slot(), net.over_x())
    second.start()
    second.wait()
    vz[c] = vec[1] + vx[...]
    third = []
    for dc in range(1, C):
        cp = net.remote(vz.at[c], vz.at[c], net.slot(), net.at(c=net.shard(dc)))
        cp.start()
        third.append(cp)
    for cp in third:
        cp.wait()
    total = vz[0]
    for i in range(1, C):
        total = total + vz[i]
    sums_out[y] = total
    last = net.remote(sums_out.at[y], sums_out.at[y], net.slot(), net.over_y())
    last.start()
    hand_out.finish()
    deal_o.finish()
    deal_q.finish()
    last.wait()
    swap.wait()
    swap_b.wait()
    for cp in keeps:
        cp.wait()


def swiglu_groups(g_out, u_out, d_out, zgu, zd, unit):
    full = slice(None)
    place = lambda a, b: pl.ds(pl.multiple_of((2 * a + b) * unit, 128), unit)
    return [
        (None, None, None, zgu,
         [((full, pl.ds(0, unit)), lambda a, b: g_out.at[:, place(a, b)]),
          ((full, pl.ds(unit, unit)), lambda a, b: u_out.at[:, place(a, b)])], None, False),
        (None, None, None, zd, [((full, full), lambda a, b: d_out.at[place(a, b), :])], None, False),
    ]


class Deal:
    def __init__(self, net, groups):
        self.net, self.groups = net, groups
        self.order = [(dc, dk) for dc in range(1, net.C) for dk in range(2)] + [(0, 1), (0, 0)]
        self.xs, self.zs = {}, []
        self.added = self.posted = 0

    def start(self):
        net = self.net
        for s in self.order:
            b = net.shard(s[0]) * 4 + 2 * (1 - net.x) + (net.k + s[1]) % 2
            for g, (partial, place, from_x, *_) in enumerate(self.groups):
                cp = net.remote(partial.at[place(b)], from_x.at[2 * s[0] + s[1]], net.slot(), net.over_x())
                cp.start()
                self.xs[g, s] = cp

    def add(self, count):
        net = self.net
        for s in self.order[self.added:self.added + count]:
            i = 2 * s[0] + s[1]
            b = net.shard(s[0]) * 4 + 2 * net.x + (net.k + s[1]) % 2
            for g, (partial, place, from_x, sums, puts, keep, flip) in enumerate(self.groups):
                self.xs[g, s].wait_recv()
                total = partial[place(b)].astype(F32) + from_x[i].astype(F32)
                if flip:
                    total = total.T
                if s == (0, 0) and keep is not None:
                    keep(total)
                else:
                    sums[i] = total.astype(BF)
        self.added += count

    def post(self, count):
        net = self.net
        for s in self.order[self.posted:min(self.posted + count, len(self.order) - 1)]:
            i = 2 * s[0] + s[1]
            to = net.at(c=net.shard(s[0]), k=(net.k + s[1]) % 2)
            for partial, place, from_x, sums, puts, keep, flip in self.groups:
                slot = net.slot()
                for take, put in puts:
                    net.remote(sums.at[(i,) + take], put(net.c, net.k), slot, to).start()
                self.zs.append((sums, i, slot))
        self.posted += count

    def both(self, count):
        for _ in range(count):
            self.add(1)
            self.post(1)

    def finish(self):
        for sums, i, slot in self.zs:
            self.net.remote(sums.at[i], sums.at[i], slot, self.net.over_x()).wait()
        for cp in self.xs.values():
            cp.wait_send()


def finish_kernel(few, blk, ig, sums, g, u, d, q, kv, o, block_out, input_grad, a_gain, q_w, k_w, v_w, q_gain, k_gain,
                  o_w, m_gain, g_w, u_w, d_w):
    mine = lax.axis_index(CONTEXT) * 4 + lax.axis_index(FSDP)
    H = blk.shape[2]
    n = H // sums.shape[2]
    for i in range(2):
        block_out[:, i * H:(i + 1) * H] = blk[i]
        input_grad[:, i * H:(i + 1) * H] = ig[i].astype(F32)
    for out, value in ((q_w, q), (o_w, o), (g_w, g), (u_w, u), (d_w, d)):
        out[...] = value[...].astype(F32)
    k_w[...] = kv[0].astype(F32)
    v_w[...] = kv[1].astype(F32)
    half, row = mine // n, mine % n
    a_gain[...] = sums[half, pl.ds(row, 1)]
    m_gain[...] = sums[half, pl.ds(n + row, 1)]
    lanes = sums.shape[2]
    total = sums[0] + sums[1]
    shift = lax.rem(lanes - mine * few, lanes)
    q_gain[...] = pltpu.roll(total[2 * n:2 * n + 8], shift, 1)[0:1, 0:few]
    k_gain[...] = pltpu.roll(total[2 * n:2 * n + 8], shift, 1)[1:2, 0:few]


def call(kernel, name, cid, out_shape, in_specs, out_specs, scratch, *args):
    return pl.pallas_call(
        kernel, name=name, out_shape=out_shape, in_specs=in_specs, out_specs=out_specs,
        scratch_shapes=scratch + [
            pltpu.SemaphoreType.DMA((SLOTS,)), pltpu.SemaphoreType.DMA((SLOTS,)), pltpu.SemaphoreType.DMA((LOCAL_SLOTS,)),
        ],
        compiler_params=pltpu.CompilerParams(
            collective_id=cid, has_side_effects=True, vmem_limit_bytes=67043328
        ),
    )(*args)


def tensor_parallel(layer_input, block_pair, attn_gain, q_weight, key_projection, value_projection, q_gain, k_gain,
                    o_weight, mlp_gain, gate_weight, up_weight, down_weight, cotangent):
    C = lax.axis_size(CONTEXT)
    R, D = layer_input.shape
    B = q_weight.shape[0]
    NB = 4 * C
    T = 2 * C * R
    H = D // 2
    head = HEAD_SIZE
    unit = gate_weight.shape[1] // (2 * C)
    scale = 1.0 / math.sqrt(head)
    S = jax.ShapeDtypeStruct
    k = lax.axis_index(FSDP) % 2
    x = lax.axis_index(FSDP) // 2
    TILES = 8

    red = lambda wire: reduce_scratch(C, R, D, TILES, wire)
    rs = lambda: pltpu.VMEM((TILES // 2, R, D // TILES), F32)
    stat = lambda: pltpu.VMEM((R, 128), F32)
    mine = lax.axis_index(CONTEXT) * 4 + lax.axis_index(FSDP)
    rows_of = lambda v: v.reshape(1, -1)
    freq = np.exp(np.arange(head // 2, dtype=np.float32) * np.float32(-2.0 * math.log(THETA) / head))
    freq = np.broadcast_to(np.concatenate([freq, freq])[None, :], (8, head))
    small = jnp.pad(jnp.stack([q_gain, k_gain]), ((0, 6), (0, head - q_gain.shape[0]))).astype(F32)
    vm = lambda *shape: pltpu.VMEM(shape, BF)
    f32 = lambda *shape: pltpu.VMEM(shape, F32)
    mine_s = [pltpu.VMEM((T, 128), jnp.int32), pltpu.VMEM((8, T), jnp.int32), f32(T, 128), f32(T, 128), vm(D, 3 * head),
              vm(head, D), f32(T, 2 * head), vm(T, head), vm(T, 2 * head), vm(T, 2 * head), vm(T, head), f32(8, T)]
    E = len(mine_s)
    V = (2 * (H // 128) + 8, 128)
    wide = lambda: pltpu.VMEM((2, T, head), F32)
    one = lambda: pltpu.VMEM((T, head), F32)
    narrow = red(BF)
    inner = [narrow[0]] + narrow[4:]

    def layer(*r):
        a = 24 + 6
        b = a + E
        c = b + 9
        d = c + 8
        e = d + 8 + 13
        osend, *rest = r[e:e + 5]
        ht = r[b + 3]
        views = (osend, Columns(ht.at[0], 0, D // TILES), Columns(ht.at[1], 0, D // TILES),
                 Columns(ht.at[1], TILES // 2, D // TILES), *rest)
        return layer_kernel(C, TILES, head, scale, 256, q_gain.shape[0], *r[:a], r[a:b], *r[b:c], r[c:d], *r[d:e], views, *r[e + 5:])

    g_w, u_w, d_w, blk, ig, sums, q_w, kv_w, o_w = call(
        layer, "layer", 1,
        (S((2, C, R, D), BF), S((B, 2 * C * unit), BF), S((B, 2 * C * unit), BF), S((2 * C * unit, B), BF),
         S((2, R, H), BF), S((2, R, H), BF), S((2,) + V, F32), S((B, 2 * C * head), BF), S((2, B, C * head), BF),
         S((2 * C * head, B), BF)),
        [VM] * 6 + [pl.BlockSpec(memory_space=pltpu.SMEM)] + [HBM] * 7, (HBM,) * 4 + (VM,) * 6,
        [vm(16, B), vm(NB, 16, B), f32(R, H), f32(R, H), vm(2 * C, B, 2 * unit), vm(2 * C, unit, B)] + mine_s
        + [vm(2, C * R, unit), vm(unit, D), vm(2, C, R, D), vm(2, C, R, D), vm(2, C, R, D), vm(D, 2 * unit),
           f32(T, 128), f32(T, 128), f32(T, head)] + red(F32)
        + [rs(), vm(R, H), vm(R, H), f32(6, R, 128), vm(2, C * R, 2 * unit), vm(2 * unit, T), vm(unit, T),
           vm(C, 3 * unit, 2 * B)]
        + [f32(8, T), wide(), wide(), wide(), one(), vm(2 * C, 2 * head, B), vm(2 * C, B, 2 * head), vm(2 * C, head, B),
           vm(2 * C, head, B), f32(2, *V), f32(*V), f32(*V), f32(C, *V)]
        + inner + [rs()],
        layer_input, rows_of(attn_gain), rows_of(mlp_gain), small, cotangent, freq, block_pair,
        q_weight, key_projection, value_projection, o_weight, gate_weight, up_weight, down_weight,
    )[1:]
    few = q_gain.shape[0]
    wide_w = lambda v: S(v.shape, F32)
    STEPS = 4
    part = lambda *shape: pl.BlockSpec((shape[0] // STEPS,) + shape[1:], lambda i: (i,) + (0,) * (len(shape) - 1))
    inner_part = lambda n, m, w: pl.BlockSpec((n, m // STEPS, w), lambda i: (0, i, 0))
    same = lambda *shape: pl.BlockSpec(shape, lambda i: (0,) * len(shape))
    kv_part = part(*kv_w.shape[1:])
    out = pl.pallas_call(
        functools.partial(finish_kernel, few), name="finish", grid=(STEPS,),
        out_shape=(S((R, D), BF), S((R, D), F32), S((1, B), F32), wide_w(q_w), S(kv_w.shape[1:], F32),
                   S(kv_w.shape[1:], F32), S((1, few), F32), S((1, few), F32), wide_w(o_w), S((1, B), F32),
                   wide_w(g_w), wide_w(u_w), wide_w(d_w)),
        in_specs=[inner_part(*blk.shape), inner_part(*ig.shape), same(*sums.shape), part(*g_w.shape), part(*u_w.shape),
                  part(*d_w.shape), part(*q_w.shape), inner_part(*kv_w.shape), part(*o_w.shape)],
        out_specs=(part(R, D), part(R, D), same(1, B), part(*q_w.shape), kv_part, kv_part, same(1, few), same(1, few),
                   part(*o_w.shape), same(1, B), part(*g_w.shape), part(*u_w.shape), part(*d_w.shape)),
        compiler_params=pltpu.CompilerParams(vmem_limit_bytes=60 * 1024 * 1024),
    )(blk, ig, sums, g_w, u_w, d_w, q_w, kv_w, o_w)
    return tuple(v.reshape(v.shape[1:]) if i in (2, 6, 7, 9) else v for i, v in enumerate(out))


def fits(mesh_shape, layer_input, q_weight, key_projection, gate_weight):
    C = mesh_shape[CONTEXT]
    return (
        mesh_shape[FSDP] == 4 and mesh_shape[HEADS] == 2
        and key_projection.shape[1] == C * HEAD_SIZE and q_weight.shape[1] == 2 * C * HEAD_SIZE
        and gate_weight.shape[1] % (2 * C * 128) == 0 and 5 * gate_weight.shape[1] <= 2 * C * layer_input.shape[1]
        and gate_weight.shape[1] >= 6 * C * 128 and q_weight.shape[0] == 128
        and C == 4 and layer_input.shape[0] % 128 == 0 and layer_input.shape[1] % (8 * 128) == 0
    )


def solution(mesh):
    def program(*args):
        layer_input, q_weight, key_projection, gate_weight = args[0], args[3], args[4], args[10]
        if fits(dict(mesh.shape), layer_input, q_weight, key_projection, gate_weight):
            return tensor_parallel(*args)
        return per_device(*args)

    return jax.shard_map(
        program,
        mesh=mesh,
        in_specs=(
            P(ROWS, None),
            P(),
            P(ROWS),
            P(ROWS, HEADS),
            P(ROWS, HEADS),
            P(ROWS, HEADS),
            P(ROWS),
            P(ROWS),
            P(HEADS, ROWS),
            P(ROWS),
            P(ROWS, HEADS),
            P(ROWS, HEADS),
            P(HEADS, ROWS),
            P(ROWS, None),
        ),
        out_specs=(
            P(ROWS, None),
            P(ROWS, None),
            P(ROWS),
            P(ROWS, HEADS),
            P(ROWS, HEADS),
            P(ROWS, HEADS),
            P(ROWS),
            P(ROWS),
            P(HEADS, ROWS),
            P(ROWS),
            P(ROWS, HEADS),
            P(ROWS, HEADS),
            P(HEADS, ROWS),
        ),
        check_vma=False,
    )
```
